256 devices in a mesh: row: 32 (over z_lo, y, core), col: 8 (over x, z_hi).
Axes of the slice: x: 4, y: 4, z: 8 (z_hi: 2, z_lo: 4; z = z_hi * 4 + z_lo), core: 2. Of those that a mesh axis runs over, the one named last changes fastest.
Arguments:
- pair_rep: bfloat16 [2048, 2048, 128], P('row', 'col'), may hold values from -6 to 6
- bias_weight: bfloat16 [128, 12], replicated, may hold values from -0.5 to 0.5
- head_weight: float32 [12], replicated, may hold values from -1 to 1
- queries: float32 [192, 2048], P(None, 'row'), may hold values from -48 to 48, as said below
- key_vectors: float32 [192, 2048], P(None, 'col'), may hold values from -48 to 48, as said below
- values: float32 [192, 2048], P(None, 'col'), may hold values from -6 to 6
- query_points: float32 [3, 48, 2048], P(None, None, 'row'), may hold values from -6 to 6
- key_points: float32 [3, 48, 2048], P(None, None, 'col'), may hold values from -6 to 6
- value_points: float32 [3, 96, 2048], P(None, None, 'col'), may hold values from -6 to 6
- rotations: float32 [3, 3, 2048], replicated, may hold values from -1 to 1, as said below
- translations: float32 [3, 2048], replicated, may hold values from -12 to 12
- residue_count: int32 [1], replicated, may hold values from 1024 to 2048
- grad_output: float32 [192, 2048], P(None, 'row'), may hold values from -6 to 6
- grad_points: float32 [3, 96, 2048], P(None, None, 'row'), may hold values from -6 to 6
- grad_pair: bfloat16 [2048, 12, 128], P('row'), may hold values from -2 to 2
Outputs:
- pair_grad: bfloat16 [2048, 2048, 128], P('row', 'col')
- query_grad: float32 [192, 2048], P(None, ('row', 'col'))
- query_point_grad: float32 [3, 48, 2048], P(None, None, ('row', 'col'))
- query_frame_grad: float32 [3, 4, 2048], P(None, None, ('row', 'col'))
- key_grad: float32 [192, 2048], P(None, ('col', 'row'))
- value_grad: float32 [192, 2048], P(None, ('col', 'row'))
- key_point_grad: float32 [3, 48, 2048], P(None, None, ('col', 'row'))
- value_point_grad: float32 [3, 96, 2048], P(None, None, ('col', 'row'))
- key_frame_grad: float32 [3, 4, 2048], P(None, None, ('col', 'row'))
- bias_weight_grad: float32 [128, 12], replicated
- head_weight_grad: float32 [12], replicated
The draws below stay inside these ranges and needn't reach their ends.
Inputs may be any that keep to these rules, and one draw needn't show every extreme that they name: `queries`: entries of order one, except a few residues whose vectors are much larger. `key_vectors`: entries of order one, except a few residues whose vectors are much larger. `rotations`: each residue's 3 x 3 matrix is a rotation: orthonormal with determinant one.
All inputs are finite; a program needn't handle non-finite values.
Results may differ from the reference program's by a relative error of at most 0.0049.
Values sent between devices are 32-bit elements; how exact they have to be, the bound alone decides.
A program may use at most 128 MiB of HBM per device.

```python
import math
import jax
import jax.numpy as jnp
from jax import lax

N = 2048
H = 12
C = 16
PQ = 4
PV = 8
CZ = 128


def drawn_vectors(key):
    base_key = jax.random.fold_in(key, 11)
    first, second = jax.random.split(base_key, 2)
    query_draw = jnp.clip(jax.random.normal(first, (H * C, N), jnp.float32), -4.0, 4.0)
    key_draw = jnp.clip(jax.random.normal(second, (H * C, N), jnp.float32), -4.0, 4.0)
    return (query_draw, key_draw)


def draw_queries(key, part):
    return drawn_vectors(key)[0]


def draw_key_vectors(key, part):
    return drawn_vectors(key)[1]


def draw_rotations(key, part):
    base_key = jax.random.fold_in(key, 23)
    first, second = jax.random.split(base_key)
    scalar = jax.random.uniform(first, (N,), jnp.float32, 0.5, 1.5)
    vector = jax.random.normal(second, (3, N), jnp.float32)
    length = jnp.sqrt(scalar ** 2 + jnp.sum(vector ** 2, axis=0))
    qw = scalar / length
    qx = vector[0] / length
    qy = vector[1] / length
    qz = vector[2] / length
    first_row = jnp.stack([1 - 2 * (qy * qy + qz * qz), 2 * (qx * qy - qw * qz), 2 * (qx * qz + qw * qy)])
    second_row = jnp.stack([2 * (qx * qy + qw * qz), 1 - 2 * (qx * qx + qz * qz), 2 * (qy * qz - qw * qx)])
    third_row = jnp.stack([2 * (qx * qz - qw * qy), 2 * (qy * qz + qw * qx), 1 - 2 * (qx * qx + qy * qy)])
    return jnp.stack([first_row, second_row, third_row])


def levels(stream_key, dims, shards, least, high):
    factor_of, own = 1.0, jax.random.fold_in(stream_key, 6)
    for position, parts in shards:
        heights = jnp.exp(jax.random.uniform(jax.random.fold_in(own, position), (parts,), jnp.float32, least / len(shards), high / len(shards)))
        factor_of = factor_of * jnp.repeat(heights, dims[position] // parts).reshape([-1 if axis == position else 1 for axis in range(len(dims))])
    return factor_of


def gaussian(own_key, shape, deviation, most, pieces=(), kind=jnp.bfloat16):
    loudness = levels(own_key, shape, pieces, -0.22, 0.18) if pieces else 1.0
    drawn = jax.random.normal(own_key, shape, jnp.float32) * deviation * loudness
    return jnp.minimum(jnp.maximum(drawn, -most), most).astype(kind)


def setup_inputs(seed: int = 0) -> dict:
    key_list = jax.random.split(jax.random.key(seed), 16)
    return {
        "pair_rep": gaussian(key_list[0], (N, N, CZ), 1.0, 6.0, ((0, 32), (1, 8))),
        "bias_weight": gaussian(key_list[1], (CZ, H), CZ ** -0.5, 0.5),
        "head_weight": jnp.clip(jax.random.uniform(key_list[2], (H,), jnp.float32, -1.0, 1.0), -1.0, 1.0),
        "queries": draw_queries(jax.random.fold_in(key_list[15], 71), 0),
        "key_vectors": draw_key_vectors(jax.random.fold_in(key_list[15], 71), 0),
        "values": gaussian(key_list[5], (H * C, N), 1.0, 6.0, ((1, 8),), jnp.float32),
        "query_points": gaussian(key_list[6], (3, H * PQ, N), 1.0, 6.0, ((2, 32),), jnp.float32),
        "key_points": gaussian(key_list[7], (3, H * PQ, N), 1.0, 6.0, ((2, 8),), jnp.float32),
        "value_points": gaussian(key_list[8], (3, H * PV, N), 1.0, 6.0, ((2, 8),), jnp.float32),
        "rotations": draw_rotations(jax.random.fold_in(key_list[15], 71), 0),
        "translations": gaussian(key_list[10], (3, N), 2.0, 12.0, (), jnp.float32),
        "residue_count": jax.random.randint(key_list[11], (1,), N // 2, N + 1).astype(jnp.int32),
        "grad_output": gaussian(key_list[12], (H * C, N), 1.0, 6.0, ((1, 32),), jnp.float32),
        "grad_points": gaussian(key_list[13], (3, H * PV, N), 1.0, 6.0, ((2, 32),), jnp.float32),
        "grad_pair": gaussian(key_list[14], (N, H, CZ), 0.3, 2.0, ((0, 32),)),
    }


HIGHEST = lax.Precision.HIGHEST

def globalize(rotation, offset, local):
    return jnp.einsum('xym,ykm->xkm', rotation, local, precision=HIGHEST) + offset[:, None, :]

def rotate_back(rotation, vector):
    return jnp.einsum('xym,xkm->ykm', rotation, vector, precision=HIGHEST)

def frame_terms(grad_global, local):
    rotation_part = jnp.einsum('xkm,ykm->xym', grad_global, local, precision=HIGHEST)
    return jnp.concatenate([rotation_part, lax.optimization_barrier(jnp.sum(grad_global, axis=1))[:, None, :]], axis=1)

def output_frame_terms(point_out, offset, cotan_local, grad_rotated):
    rotation_part = jnp.einsum('xkm,ykm->xym', point_out - offset[:, None, :], cotan_local, precision=HIGHEST)
    return jnp.concatenate([rotation_part, -lax.optimization_barrier(jnp.sum(grad_rotated, axis=1))[:, None, :]], axis=1)

def reference(pair_rep, bias_weight, head_weight, queries, key_vectors, values, query_points, key_points, value_points, rotations, translations, residue_count, grad_output, grad_points, grad_pair):
    logit_scale = math.sqrt(1.0 / 3.0)
    point_scale = math.sqrt(2.0 / (9.0 * PQ))
    inner_scale = 1.0 / math.sqrt(C)
    distance_coef = 0.5 * logit_scale * point_scale * jax.nn.softplus(head_weight)
    query_global = globalize(rotations, translations, query_points).reshape(3, H, PQ, N)
    key_global = globalize(rotations, translations, key_points).reshape(3, H, PQ, N)
    value_global = globalize(rotations, translations, value_points).reshape(3, H, PV, N)
    grad_global = jnp.einsum('xym,ykm->xkm', rotations, grad_points, precision=HIGHEST)
    grad_heads = grad_global.reshape(3, H, PV, N)
    key_heads = key_vectors.reshape(H, C, N)
    value_heads = values.reshape(H, C, N)
    query_heads = queries.reshape(H, C, N)
    out_heads = grad_output.reshape(H, C, N)
    valid = jnp.arange(N) < residue_count[0]
    pair_weight = bias_weight.astype(jnp.float32)
    block = min(128, N)

    def step(carry, start):
        pair_block = lax.dynamic_slice_in_dim(pair_rep, start, block, 0).astype(jnp.float32)
        cotan_pair = lax.dynamic_slice_in_dim(grad_pair, start, block, 0).astype(jnp.float32)
        query_block = lax.dynamic_slice_in_dim(query_heads, start, block, 2)
        out_block = lax.dynamic_slice_in_dim(out_heads, start, block, 2)
        qglobal_block = lax.dynamic_slice_in_dim(query_global, start, block, 3)
        gglobal_block = lax.dynamic_slice_in_dim(grad_heads, start, block, 3)
        inner = jnp.einsum('hci,hcj->hij', query_block, key_heads, precision=HIGHEST)
        cross = jnp.einsum('xhpi,xhpj->hij', qglobal_block, key_global, precision=HIGHEST)
        distance = lax.optimization_barrier(jnp.sum(qglobal_block ** 2, axis=(0, 2)))[:, :, None] + lax.optimization_barrier(jnp.sum(key_global ** 2, axis=(0, 2)))[:, None, :] - 2.0 * cross
        bias = jnp.einsum('ijc,ch->hij', pair_block, pair_weight, precision=HIGHEST)
        logits = logit_scale * (inner_scale * inner + bias) - distance_coef[:, None, None] * distance
        logits = jnp.where(valid[None, None, :], logits, jnp.float32(-1000000000.0))
        row_peak = lax.optimization_barrier(jnp.max(logits, axis=2, keepdims=True))
        exponent = jnp.exp(logits - row_peak)
        attention = exponent / lax.optimization_barrier(jnp.sum(exponent, axis=2, keepdims=True))
        product = jnp.einsum('hci,hcj->hij', out_block, value_heads, precision=HIGHEST) + jnp.einsum('xhvi,xhvj->hij', gglobal_block, value_global, precision=HIGHEST) + jnp.einsum('ijc,ihc->hij', pair_block, cotan_pair, precision=HIGHEST)
        delta = lax.optimization_barrier(jnp.sum(attention * product, axis=2, keepdims=True))
        logit_grad = attention * (product - delta)
        query_grad = logit_scale * inner_scale * jnp.einsum('hij,hcj->hci', logit_grad, key_heads, precision=HIGHEST)
        row_sum = lax.optimization_barrier(jnp.sum(logit_grad, axis=2))
        qpoint_grad = -2.0 * distance_coef[None, :, None, None] * (qglobal_block * row_sum[None, :, None, :] - jnp.einsum('hij,xhpj->xhpi', logit_grad, key_global, precision=HIGHEST))
        qpoint_flat = qpoint_grad.reshape(3, H * PQ, block)
        point_out = jnp.einsum('hij,xhvj->xhvi', attention, value_global, precision=HIGHEST).reshape(3, H * PV, block)
        rot_block = lax.dynamic_slice_in_dim(rotations, start, block, 2)
        shift_block = lax.dynamic_slice_in_dim(translations, start, block, 1)
        local_block = lax.dynamic_slice_in_dim(query_points, start, block, 2)
        cotan_local = lax.dynamic_slice_in_dim(grad_points, start, block, 2)
        gflat_block = gglobal_block.reshape(3, H * PV, block)
        qlocal_grad = rotate_back(rot_block, qpoint_flat)
        qframe = frame_terms(qpoint_flat, local_block) + output_frame_terms(point_out, shift_block, cotan_local, gflat_block)
        key_part = logit_scale * inner_scale * jnp.einsum('hij,hci->hcj', logit_grad, query_block, precision=HIGHEST)
        value_part = jnp.einsum('hij,hci->hcj', attention, out_block, precision=HIGHEST)
        col_sum = lax.optimization_barrier(jnp.sum(logit_grad, axis=1))
        kpoint_part = 2.0 * distance_coef[None, :, None, None] * (jnp.einsum('hij,xhpi->xhpj', logit_grad, qglobal_block, precision=HIGHEST) - key_global * col_sum[None, :, None, :])
        vpoint_part = jnp.einsum('hij,xhvi->xhvj', attention, gglobal_block, precision=HIGHEST)
        grad_rounded = lax.optimization_barrier(logit_grad.astype(jnp.bfloat16)).astype(jnp.float32)
        attn_rounded = lax.optimization_barrier(attention.astype(jnp.bfloat16)).astype(jnp.float32)
        weight_part = logit_scale * jnp.einsum('ijc,hij->ch', pair_block, grad_rounded, precision=HIGHEST)
        distance_part = lax.optimization_barrier(jnp.sum(logit_grad * distance, axis=(1, 2)))
        pair_grad = (logit_scale * jnp.einsum('hij,ch->ijc', grad_rounded, pair_weight, precision=HIGHEST) + jnp.einsum('hij,ihc->ijc', attn_rounded, cotan_pair, precision=HIGHEST)).astype(jnp.bfloat16)
        new_carry = (carry[0] + key_part, carry[1] + value_part, carry[2] + kpoint_part, carry[3] + vpoint_part, carry[4] + weight_part, carry[5] + distance_part)
        return (new_carry, (pair_grad, query_grad.reshape(H * C, block), qlocal_grad, qframe))
    initial = (jnp.zeros((H, C, N), jnp.float32), jnp.zeros((H, C, N), jnp.float32), jnp.zeros((3, H, PQ, N), jnp.float32), jnp.zeros((3, H, PV, N), jnp.float32), jnp.zeros((CZ, H), jnp.float32), jnp.zeros((H,), jnp.float32))
    starts = jnp.arange(N // block, dtype=jnp.int32) * block
    carry, stacked = lax.scan(step, initial, starts)
    pair_grad = stacked[0].reshape(N, N, CZ)
    query_grad = jnp.transpose(stacked[1], (1, 0, 2)).reshape(H * C, N)
    query_point_grad = jnp.transpose(stacked[2], (1, 2, 0, 3)).reshape(3, H * PQ, N)
    query_frame_grad = jnp.transpose(stacked[3], (1, 2, 0, 3)).reshape(3, 4, N)
    kpoint_flat = carry[2].reshape(3, H * PQ, N)
    vpoint_flat = carry[3].reshape(3, H * PV, N)
    key_point_grad = rotate_back(rotations, kpoint_flat)
    value_point_grad = rotate_back(rotations, vpoint_flat)
    key_frame_grad = frame_terms(kpoint_flat, key_points) + frame_terms(vpoint_flat, value_points)
    head_weight_grad = carry[5] * (-0.5 * logit_scale * point_scale) * jax.nn.sigmoid(head_weight)
    return (pair_grad, query_grad, query_point_grad, query_frame_grad, carry[0].reshape(H * C, N), carry[1].reshape(H * C, N), key_point_grad, value_point_grad, key_frame_grad, carry[4], head_weight_grad)
```

```python
import functools
import math

import jax
import jax.numpy as jnp
from jax import lax
from jax.experimental import pallas as pl
from jax.experimental.pallas import tpu as pltpu
from jax.sharding import Mesh
from jax.sharding import PartitionSpec as P

ROW = ("row_0", "row_1", "row_2")
COL = ("col_0", "col_1")
ROW_COL = ROW + COL
COL_ROW = COL + ROW

H, C, PQ, PV, CZ = 12, 16, 4, 8, 128
KF, QF = 896, 768
VAL0, KP0, VP0 = 192, 384, 528
LOGIT = math.sqrt(1.0 / 3.0)
POINT = math.sqrt(2.0 / (9.0 * PQ))
INNER = 1.0 / math.sqrt(C)

F32, BF = jnp.float32, jnp.bfloat16
HIGHEST = lax.Precision.HIGHEST
MESH = pl.DeviceIdType.MESH


def dot(a, b, ca, cb, precision=None):
    return lax.dot_general(
        a, b, (((ca,), (cb,)), ((), ())), precision=precision, preferred_element_type=F32
    )


def split(a):
    hi = a.astype(BF)
    return hi, (a - hi.astype(F32)).astype(BF)


def dot3(a, b, ca, cb):
    (ah, al), (bh, bl) = a, b
    return dot(ah, bh, ca, cb) + dot(ah, bl, ca, cb) + dot(al, bh, ca, cb)


def iota(shape, dim):
    return lax.broadcasted_iota(jnp.int32, shape, dim)


def softplus(x):
    return jnp.maximum(x, 0.0) + jnp.log1p(jnp.exp(-jnp.abs(x)))


def tile_kernel(
    sizes,
    pair_hbm,
    wt_ref,
    hw_ref,
    q_ref,
    k_ref,
    v_ref,
    qp_ref,
    kp_ref,
    vp_ref,
    rot_ref,
    trans_ref,
    count_ref,
    go_ref,
    gp_ref,
    gpair_ref,
    pg_hbm,
    key_out,
    query_out,
    small_out,
    pair_v,
    pg_v,
    s_ref,
    e_ref,
    p_ref,
    d_ref,
    q32,
    k32,
    g48,
    v48,
    vec,
    vec_t,
    stat_own,
    stat_in,
    feat,
    kt,
    k1,
    p1,
    k2,
    p2,
    k3,
    qfeat,
    qt,
    qin,
    w_own,
    w_in,
    w_mid,
    w_in2,
    pair_sem,
    pg_sem,
    stat_send,
    stat_recv,
    k1_send,
    k1_recv,
    k2_send,
    k2_recv,
    k3_send,
    k3_recv,
    q_send,
    q_recv,
    w_send,
    w_recv,
    w2_send,
    w2_recv,
):
    n0, n1, n2, m0, m1 = sizes
    cols_n = m0 * m1
    rows = q_ref.shape[0]
    cols = k_ref.shape[1]
    i0, i1, i2 = (lax.axis_index(a) for a in ROW)
    j0, j1 = (lax.axis_index(a) for a in COL)
    r = (i0 * n1 + i1) * n2 + i2
    c = j0 * m1 + j1

    def col_peer(d):
        p = lax.rem(c + d, cols_n)
        return {"col_0": p // m1, "col_1": lax.rem(p, m1)}

    g1 = cols_n * n2
    g2 = n0 * n1

    def one_peer(d):
        p = lax.rem(c * n2 + i2 + d, g1)
        pc = p // n2
        return {"col_0": pc // m1, "col_1": lax.rem(pc, m1), "row_2": lax.rem(p, n2)}

    def two_peer(d):
        p = lax.rem(i0 * n1 + i1 + d, g2)
        return {"row_0": p // n1, "row_1": lax.rem(p, n1)}

    core_peer = {"row_2": lax.rem(i2 + 1, n2)}

    barrier = pltpu.get_barrier_semaphore()
    for d in range(1, g1):
        pl.semaphore_signal(barrier, inc=1, device_id=one_peer(d), device_id_type=MESH)
    for d in range(1, g2):
        pl.semaphore_signal(barrier, inc=1, device_id=two_peer(d), device_id_type=MESH)

    parts = pair_sem.shape[0]
    step = rows // parts
    loads = [
        pltpu.make_async_copy(
            pair_hbm.at[pl.ds(b * step, step)], pair_v.at[pl.ds(b * step, step)], pair_sem.at[b]
        )
        for b in range(parts)
    ]
    for load in loads:
        load.start()

    col_start = pl.multiple_of(c * cols, 128)
    row_start = r * rows
    row_base = pl.multiple_of((row_start // 128) * 128, 128)
    row_half = lax.rem(row_start, 128)

    def row_window(w):
        return jnp.where(row_half == 0, w[:, :rows], w[:, 128 - rows :])

    def row_rot(x, y):
        return row_window(rot_ref[x, pl.ds(y, 1), pl.ds(row_base, 128)])

    def col_rot(x, y):
        return rot_ref[x, pl.ds(y, 1), pl.ds(col_start, cols)]

    coef = 0.5 * LOGIT * POINT * softplus(hw_ref[...])

    zero_q = jnp.zeros((2, rows), F32)
    zero_k = jnp.zeros((2, cols), F32)
    q_t = q_ref[...].T * (LOGIT * INNER)
    k_all = k_ref[...]
    rr = [[row_rot(x, y) for y in range(3)] for x in range(3)]
    cr = [[col_rot(x, y) for y in range(3)] for x in range(3)]
    for x in range(3):
        t_row = row_window(trans_ref[pl.ds(x, 1), pl.ds(row_base, 128)])
        t_col = trans_ref[pl.ds(x, 1), pl.ds(col_start, cols)]
        qg = sum(rr[x][y] * qp_ref[y] for y in range(3)) + t_row
        kg = sum(cr[x][y] * kp_ref[y] for y in range(3)) + t_col
        vg = sum(cr[x][y] * vp_ref[y] for y in range(3)) + t_col
        for h in range(H):
            q32[32 * h + 16 + 4 * x : 32 * h + 20 + 4 * x, :] = qg[4 * h : 4 * h + 4]
            k32[32 * h + 16 + 4 * x : 32 * h + 20 + 4 * x, :] = kg[4 * h : 4 * h + 4]
            v48[48 * h + 16 + 8 * x : 48 * h + 24 + 8 * x, :] = vg[8 * h : 8 * h + 8]
    gp_t = [gp_ref[y].T for y in range(3)]
    for x in range(3):
        gg = sum(rr[x][y] * gp_t[y] for y in range(3))
        for h in range(H):
            g48[48 * h + 16 + 8 * x : 48 * h + 24 + 8 * x, :] = gg[8 * h : 8 * h + 8]
    go_t = go_ref[...].T
    for h in range(H):
        q32[32 * h : 32 * h + 16, :] = q_t[16 * h : 16 * h + 16]
        k32[32 * h : 32 * h + 16, :] = k_all[16 * h : 16 * h + 16]
        g48[48 * h : 48 * h + 16, :] = go_t[16 * h : 16 * h + 16]
        v48[48 * h : 48 * h + 16, :] = v_ref[16 * h : 16 * h + 16, :]
        g48[48 * h + 40 : 48 * h + 48, :] = jnp.zeros((8, rows), F32)
        v48[48 * h + 40 : 48 * h + 48, :] = jnp.zeros((8, cols), F32)
        qh = q32[32 * h + 16 : 32 * h + 28, :]
        kh = k32[32 * h + 16 : 32 * h + 28, :]
        q32[32 * h + 28 : 32 * h + 32, :] = jnp.concatenate(
            [jnp.sum(qh * qh, axis=0, keepdims=True), jnp.ones((1, rows), F32), zero_q], axis=0
        )
        k32[32 * h + 28 : 32 * h + 32, :] = jnp.concatenate(
            [jnp.ones((1, cols), F32), jnp.sum(kh * kh, axis=0, keepdims=True), zero_k], axis=0
        )

    def pair_row(at):
        return jnp.concatenate(
            [s_ref[a, pl.ds(at, rows, stride=32), :] for a in range(cols // 128)], axis=1
        )

    def put_pair_row(at, value):
        for a in range(cols // 128):
            s_ref[a, pl.ds(at, rows, stride=32), :] = value[:, 128 * a : 128 * a + 128]

    def pair_block(at, count):
        return jnp.concatenate(
            [s_ref[a, at : at + count, :] for a in range(cols // 128)], axis=1
        )

    w16 = jnp.concatenate([wt_ref[...].astype(F32), jnp.zeros((4, CZ), F32)], axis=0)
    w16b = w16.astype(BF)

    def stack(i):
        gpad = jnp.concatenate(
            [gpair_ref[:, i, :].astype(F32), jnp.zeros((4, CZ), F32)], axis=0
        ).astype(BF)
        return gpad

    for b in range(parts):
        loads[b].wait()
        for ii in range(step):
            i = b * step + ii
            both = jnp.concatenate([w16b, stack(i)], axis=0)
            proj = dot(both, pair_v[i], 1, 1)
            for a in range(cols // 128):
                s_ref[a, 32 * i : 32 * i + 32, :] = proj[:, 128 * a : 128 * a + 128]

    point_row = iota((16, 1), 0) < 12
    valid = col_start + iota((1, cols), 1) < count_ref[0]
    lane = iota((rows, 128), 1)
    for h in range(H):
        qa = q32[32 * h : 32 * h + 16, :]
        qb = q32[32 * h + 16 : 32 * h + 32, :]
        kb = k32[32 * h + 16 : 32 * h + 32, :]
        inner = dot(qa, k32[32 * h : 32 * h + 16, :], 0, 0, HIGHEST)
        dist = dot(qb, jnp.where(point_row, -2.0 * kb, kb), 0, 0, HIGHEST)
        prod = dot3(
            split(g48[48 * h : 48 * h + 48, :]), split(v48[48 * h : 48 * h + 48, :]), 0, 0
        )
        prod = prod + pair_row(16 + h)
        logits = inner + LOGIT * pair_row(h) - coef[:, h : h + 1] * dist
        logits = jnp.where(valid, logits, -1000000000.0)
        peak = jnp.max(logits, axis=1, keepdims=True)
        e = jnp.exp(logits - peak)
        total = jnp.sum(e, axis=1, keepdims=True)
        upper = jnp.sum(e * prod, axis=1, keepdims=True)
        e_ref[h * rows : (h + 1) * rows, :] = e
        p_ref[h * rows : (h + 1) * rows, :] = prod
        d_ref[h * rows : (h + 1) * rows, :] = dist
        vec[h * rows : (h + 1) * rows, :] = jnp.where(
            lane == 0, peak, jnp.where(lane == 1, total, upper)
        )
    for b in range(H * rows // 128):
        stat_own[:, 128 * b : 128 * b + 128] = vec[128 * b : 128 * b + 128, :].T[0:8]

    pl.semaphore_wait(barrier, g1 - 1 + g2 - 1)

    stat_copies = []
    for d in range(1, cols_n):
        copy = pltpu.make_async_remote_copy(
            src_ref=stat_own,
            dst_ref=stat_in.at[d - 1],
            send_sem=stat_send.at[d - 1],
            recv_sem=stat_recv.at[d - 1],
            device_id=col_peer(d),
            device_id_type=MESH,
        )
        copy.start()
        stat_copies.append(copy)
    for copy in stat_copies:
        copy.wait()

    stats = [stat_own[...]] + [stat_in[d] for d in range(cols_n - 1)]
    peak = functools.reduce(jnp.maximum, [s[0:1] for s in stats])
    weights = [jnp.exp(s[0:1] - peak) for s in stats]
    total = sum(w * s[1:2] for w, s in zip(weights, stats))
    upper = sum(w * s[2:3] for w, s in zip(weights, stats))
    delta = upper / total
    scale = weights[0] / total
    eight = iota((8, 128), 0)
    for b in range(H * rows // 128):
        cut = slice(128 * b, 128 * b + 128)
        both = jnp.where(eight == 0, scale[:, cut], delta[:, cut])
        vec_t[cut, 0:8] = both.T

    kind = iota((32, 1), 0)
    is_vec = kind < 16
    is_point = (kind >= 16) & (kind < 28)
    head_sum = jnp.zeros((1, 128), F32)
    lane1 = iota((1, 128), 1)
    feat[816:KF, :] = jnp.zeros((KF - 816, cols), F32)
    for h in range(H):
        own = slice(h * rows, (h + 1) * rows)
        attn = e_ref[own, :] * vec_t[own, 0:1]
        dlog = attn * (p_ref[own, :] - vec_t[own, 1:2])
        moment = jnp.sum(jnp.sum(dlog * d_ref[own, :], axis=0, keepdims=True), axis=1, keepdims=True)
        head_sum = jnp.where(lane1 == h, moment, head_sum)
        put_pair_row(h, dlog)
        put_pair_row(16 + h, attn)
        e_ref[own, :] = attn
        p_ref[own, :] = dlog
        two = 2.0 * coef[:, h : h + 1]
        kd = dot3(split(q32[32 * h : 32 * h + 32, :]), split(dlog), 1, 0)
        col_sum = kd[29:30]
        kd = jnp.where(is_vec, kd, two * (kd - k32[32 * h : 32 * h + 32, :] * col_sum))
        ka = dot3(split(g48[48 * h : 48 * h + 48, :]), split(attn), 1, 0)
        feat[16 * h : 16 * h + 16, :] = kd[0:16]
        feat[VAL0 + 16 * h : VAL0 + 16 * h + 16, :] = ka[0:16]
        for x in range(3):
            at = KP0 + 48 * x + 4 * h
            feat[at : at + 4, :] = kd[16 + 4 * x : 20 + 4 * x]
            at = VP0 + 96 * x + 8 * h
            feat[at : at + 8, :] = ka[16 + 8 * x : 24 + 8 * x]
    share = kt.shape[2]
    for a in range(KF // 128):
        for b in range(cols // 128):
            block = feat[128 * a : 128 * a + 128, 128 * b : 128 * b + 128].T
            per = 128 // (share * n2)
            kt[b * per : (b + 1) * per, :, :, 128 * a : 128 * a + 128] = block.reshape(
                per, n2, share, 128
            )

    copy1 = pltpu.make_async_remote_copy(
        src_ref=kt.at[:, core_peer["row_2"]],
        dst_ref=k1,
        send_sem=k1_send,
        recv_sem=k1_recv,
        device_id=core_peer,
        device_id_type=MESH,
    )
    copy1.start()

    acc = jnp.zeros((16, CZ), F32)
    for i in range(rows):
        acc = acc + dot(pair_block(32 * i, 16).astype(BF), pair_v[i], 1, 0)
    w_own[...] = jnp.where(iota((16, 1), 0) == 12, head_sum, LOGIT * acc)
    w_copies = []
    for d in range(1, g1):
        copy = pltpu.make_async_remote_copy(
            src_ref=w_own,
            dst_ref=w_in.at[d - 1],
            send_sem=w_send.at[d - 1],
            recv_sem=w_recv.at[d - 1],
            device_id=one_peer(d),
            device_id_type=MESH,
        )
        copy.start()
        w_copies.append(copy)

    copy1.wait()
    p1[...] = (kt[:, i2] + k1[...]).reshape(p1.shape)
    copies2 = []
    for d in range(1, n1):
        y = lax.rem(i1 + d, n1)
        copy = pltpu.make_async_remote_copy(
            src_ref=p1.at[:, y],
            dst_ref=k2.at[d - 1],
            send_sem=k2_send.at[d - 1],
            recv_sem=k2_recv.at[d - 1],
            device_id={"row_1": y},
            device_id_type=MESH,
        )
        copy.start()
        copies2.append(copy)

    for h in range(H):
        own = slice(h * rows, (h + 1) * rows)
        two = 2.0 * coef[:, h : h + 1]
        qd = dot3(split(k32[32 * h : 32 * h + 32, :]), split(p_ref[own, :]), 1, 1)
        row_sum = qd[28:29]
        qd = jnp.where(is_vec, LOGIT * INNER * qd, two * (qd - q32[32 * h : 32 * h + 32, :] * row_sum))
        qa = dot3(split(v48[48 * h : 48 * h + 48, :]), split(e_ref[own, :]), 1, 1)
        qfeat[16 * h : 16 * h + 16, :] = qd[0:16]
        for x in range(3):
            at = 192 + 48 * x + 4 * h
            qfeat[at : at + 4, :] = qd[16 + 4 * x : 20 + 4 * x]
            at = 336 + 96 * x + 8 * h
            qfeat[at : at + 8, :] = qa[16 + 8 * x : 24 + 8 * x]
    qfeat[624:QF, :] = jnp.zeros((QF - 624, rows), F32)
    for a in range(QF // 128):
        qt[:, :, 128 * a : 128 * a + 128] = qfeat[128 * a : 128 * a + 128, :].T.reshape(
            qt.shape[0], qt.shape[1], 128
        )
    q_copies = []
    for d in range(1, cols_n):
        copy = pltpu.make_async_remote_copy(
            src_ref=qt.at[lax.rem(c + d, cols_n)],
            dst_ref=qin.at[d - 1],
            send_sem=q_send.at[d - 1],
            recv_sem=q_recv.at[d - 1],
            device_id=col_peer(d),
            device_id_type=MESH,
        )
        copy.start()
        q_copies.append(copy)

    w16s = (LOGIT * w16).astype(BF)
    zero32 = jnp.zeros((32, CZ), BF)
    stores = []
    for b in range(rows // 4):
        turned = pair_block(128 * b, 128).T.astype(BF)
        for half in range(2):
            first, second = 4 * b + 2 * half, 4 * b + 2 * half + 1
            wa = jnp.concatenate([w16s, stack(first)], axis=0)
            wb = jnp.concatenate([w16s, stack(second)], axis=0)
            left = [zero32] * 4
            right = [zero32] * 4
            left[2 * half], right[2 * half + 1] = wa, wb
            block = jnp.concatenate(
                [jnp.concatenate(left, axis=0), jnp.concatenate(right, axis=0)], axis=1
            )
            out = dot(turned, block, 1, 0)
            pg_v[first] = out[:, :CZ].astype(BF)
            pg_v[second] = out[:, CZ:].astype(BF)
        if (b + 1) % (rows // 4 // parts) == 0:
            p = (b + 1) // (rows // 4 // parts) - 1
            store = pltpu.make_async_copy(
                pg_v.at[pl.ds(p * step, step)], pg_hbm.at[pl.ds(p * step, step)], pg_sem.at[p]
            )
            store.start()
            stores.append(store)

    for copy in copies2:
        copy.wait()
    p2[...] = p1[:, i1] + functools.reduce(jnp.add, [k2[d] for d in range(n1 - 1)])
    copies3 = []
    for d in range(1, n0):
        z = lax.rem(i0 + d, n0)
        copy = pltpu.make_async_remote_copy(
            src_ref=p2.at[z],
            dst_ref=k3.at[d - 1],
            send_sem=k3_send.at[d - 1],
            recv_sem=k3_recv.at[d - 1],
            device_id={"row_0": z},
            device_id_type=MESH,
        )
        copy.start()
        copies3.append(copy)

    for copy in w_copies:
        copy.wait()
    w_mid[...] = w_own[...] + functools.reduce(jnp.add, [w_in[d] for d in range(g1 - 1)])
    w2_copies = []
    for d in range(1, g2):
        copy = pltpu.make_async_remote_copy(
            src_ref=w_mid,
            dst_ref=w_in2.at[d - 1],
            send_sem=w2_send.at[d - 1],
            recv_sem=w2_recv.at[d - 1],
            device_id=two_peer(d),
            device_id_type=MESH,
        )
        copy.start()
        w2_copies.append(copy)

    for copy in q_copies:
        copy.wait()
    query_out[...] = qt[c] + functools.reduce(jnp.add, [qin[d] for d in range(cols_n - 1)])
    for copy in copies3:
        copy.wait()
    key_out[...] = p2[i0] + functools.reduce(jnp.add, [k3[d] for d in range(n0 - 1)])
    for copy in w2_copies:
        copy.wait()
    small_out[...] = w_mid[...] + functools.reduce(jnp.add, [w_in2[d] for d in range(g2 - 1)])
    for store in stores:
        store.wait()


def finish_kernel(
    sizes,
    key_ref,
    query_ref,
    small_ref,
    hw_ref,
    qp_ref,
    kp_ref,
    vp_ref,
    rot_ref,
    trans_ref,
    gp_ref,
    qg_out,
    qpg_out,
    qfg_out,
    kg_out,
    vg_out,
    kpg_out,
    vpg_out,
    kfg_out,
    bw_out,
    hw_out,
):
    n0, n1, n2, m0, m1 = sizes
    share, qshare = key_ref.shape[0], query_ref.shape[0]
    rows, cols = gp_ref.shape[1], kp_ref.shape[2]
    i0, i1, i2 = (lax.axis_index(a) for a in ROW)
    j0, j1 = (lax.axis_index(a) for a in COL)
    r = (i0 * n1 + i1) * n2 + i2
    c = j0 * m1 + j1

    def pick(count, width, at):
        return (iota((count, width), 1) == iota((count, width), 0) + at).astype(F32)

    def take(sel, array):
        return dot(sel, array, 1, 1, HIGHEST)

    def frames(start, count):
        base = pl.multiple_of((start // 128) * 128, 128)
        sel = pick(count, 128, start - base)
        rot = [take(sel, rot_ref[x, :, pl.ds(base, 128)]) for x in range(3)]
        return rot, take(sel, trans_ref[:, pl.ds(base, 128)])

    def column(a, y):
        return a[:, y : y + 1]

    def total(a):
        return jnp.sum(a, axis=1, keepdims=True)

    def put_frame(out, parts):
        count = parts[0][0].shape[0]
        for x in range(3):
            lane = iota((count, 128), 1)
            wide = jnp.zeros((count, 128), F32)
            for y in range(4):
                wide = jnp.where(lane == y, parts[x][y], wide)
            if count % 8:
                wide = jnp.concatenate([wide, jnp.zeros((8 - count % 8, 128), F32)], axis=0)
            out[x] = wide.T[0:4, :count]

    rot, anchor = frames(r * rows + c * qshare, qshare)
    local_sel = pick(qshare, rows, c * qshare)
    summed = query_ref[...]
    qg_out[...] = summed[:, 0:192]
    dqg = [summed[:, 192 + 48 * x : 240 + 48 * x] for x in range(3)]
    opt = [summed[:, 336 + 96 * x : 432 + 96 * x] for x in range(3)]
    local = [take(local_sel, qp_ref[y]) for y in range(3)]
    cotan = [gp_ref[y, pl.ds(c * qshare, qshare), :] for y in range(3)]
    for y in range(3):
        qpg_out[y] = sum(column(rot[x], y) * dqg[x] for x in range(3))
    parts = []
    for x in range(3):
        shifted = opt[x] - column(anchor, x)
        turned = sum(column(rot[x], y) * cotan[y] for y in range(3))
        parts.append(
            [total(dqg[x] * local[y]) + total(shifted * cotan[y]) for y in range(3)]
            + [total(dqg[x]) - total(turned)]
        )
    put_frame(qfg_out, parts)

    rot, anchor = frames(c * cols + r * share, share)
    local_sel = pick(share, cols, r * share)
    summed = key_ref[...]
    kg_out[...] = summed[:, 0:192]
    vg_out[...] = summed[:, VAL0 : VAL0 + 192]
    dkg = [summed[:, KP0 + 48 * x : KP0 + 48 + 48 * x] for x in range(3)]
    dvg = [summed[:, VP0 + 96 * x : VP0 + 96 + 96 * x] for x in range(3)]
    klocal = [take(local_sel, kp_ref[y]) for y in range(3)]
    vlocal = [take(local_sel, vp_ref[y]) for y in range(3)]
    for y in range(3):
        kpg_out[y] = sum(column(rot[x], y) * dkg[x] for x in range(3))
        vpg_out[y] = sum(column(rot[x], y) * dvg[x] for x in range(3))
    parts = []
    for x in range(3):
        parts.append(
            [total(dkg[x] * klocal[y]) + total(dvg[x] * vlocal[y]) for y in range(3)]
            + [total(dkg[x]) + total(dvg[x])]
        )
    put_frame(kfg_out, parts)

    bw_out[...] = small_ref[0:H, :]
    raw = hw_ref[...]
    hw_out[...] = small_ref[12:13, 0:H] * (-0.5 * LOGIT * POINT) / (1.0 + jnp.exp(-raw))


def per_device(
    sizes,
    pair_rep,
    bias_weight,
    head_weight,
    queries,
    key_vectors,
    values,
    query_points,
    key_points,
    value_points,
    rotations,
    translations,
    residue_count,
    grad_output,
    grad_points,
    grad_pair,
):
    n0, n1, n2, m0, m1 = sizes
    cols_n, g1, g2 = m0 * m1, m0 * m1 * n2, n0 * n1
    rows, cols = pair_rep.shape[:2]
    share, qshare = cols // (n0 * n1 * n2), rows // cols_n
    head_row = head_weight.reshape(1, H)
    grad_points_t = jnp.transpose(grad_points, (0, 2, 1))
    vmem = pl.BlockSpec(memory_space=pltpu.VMEM)
    hbm = pl.BlockSpec(memory_space=pl.ANY)
    smem = pl.BlockSpec(memory_space=pltpu.SMEM)
    parts = 4

    def buf(*shape, dtype=F32):
        return pltpu.VMEM(shape, dtype)

    dma = pltpu.SemaphoreType.DMA
    pair_grad, key_sum, query_sum, small_sum = pl.pallas_call(
        functools.partial(tile_kernel, sizes),
        name="tile",
        out_shape=(
            jax.ShapeDtypeStruct(pair_rep.shape, BF),
            jax.ShapeDtypeStruct((share, KF), F32),
            jax.ShapeDtypeStruct((qshare, QF), F32),
            jax.ShapeDtypeStruct((16, CZ), F32),
        ),
        in_specs=[hbm] + [vmem] * 10 + [smem] + [vmem] * 3,
        out_specs=(hbm, vmem, vmem, vmem),
        scratch_shapes=[
            buf(rows, cols, CZ, dtype=BF),
            buf(rows, cols, CZ, dtype=BF),
            buf(cols // 128, rows * 32, 128),
            buf(H * rows, cols),
            buf(H * rows, cols),
            buf(H * rows, cols),
            buf(H * 32, rows),
            buf(H * 32, cols),
            buf(H * 48, rows),
            buf(H * 48, cols),
            buf(H * rows, 128),
            buf(H * rows, 128),
            buf(8, H * rows),
            buf(cols_n - 1, 8, H * rows),
            buf(KF, cols),
            buf(n0 * n1, n2, share, KF),
            buf(n0 * n1, share, KF),
            buf(n0, n1, share, KF),
            buf(n1 - 1, n0, share, KF),
            buf(n0, share, KF),
            buf(n0 - 1, share, KF),
            buf(QF, rows),
            buf(cols_n, qshare, QF),
            buf(cols_n - 1, qshare, QF),
            buf(16, CZ),
            buf(g1 - 1, 16, CZ),
            buf(16, CZ),
            buf(g2 - 1, 16, CZ),
            dma((parts,)),
            dma((parts,)),
            dma((cols_n - 1,)),
            dma((cols_n - 1,)),
            dma,
            dma,
            dma((n1 - 1,)),
            dma((n1 - 1,)),
            dma((n0 - 1,)),
            dma((n0 - 1,)),
            dma((cols_n - 1,)),
            dma((cols_n - 1,)),
            dma((g1 - 1,)),
            dma((g1 - 1,)),
            dma((g2 - 1,)),
            dma((g2 - 1,)),
        ],
        compiler_params=pltpu.CompilerParams(
            collective_id=0, has_side_effects=True, vmem_limit_bytes=48 * 1024 * 1024
        ),
    )(
        pair_rep,
        bias_weight.T,
        head_row,
        queries.T,
        key_vectors,
        values,
        query_points,
        key_points,
        value_points,
        rotations,
        translations,
        residue_count,
        grad_output.T,
        grad_points_t,
        jnp.transpose(grad_pair, (1, 0, 2)),
    )
    qg, qpg, qfg, kg, vg, kpg, vpg, kfg, bw, hw = pl.pallas_call(
        functools.partial(finish_kernel, sizes),
        name="finish",
        out_shape=(
            jax.ShapeDtypeStruct((qshare, 192), F32),
            jax.ShapeDtypeStruct((3, qshare, 48), F32),
            jax.ShapeDtypeStruct((3, 4, qshare), F32),
            jax.ShapeDtypeStruct((share, 192), F32),
            jax.ShapeDtypeStruct((share, 192), F32),
            jax.ShapeDtypeStruct((3, share, 48), F32),
            jax.ShapeDtypeStruct((3, share, 96), F32),
            jax.ShapeDtypeStruct((3, 4, share), F32),
            jax.ShapeDtypeStruct((H, CZ), F32),
            jax.ShapeDtypeStruct((1, H), F32),
        ),
        in_specs=[vmem] * 10,
        out_specs=(vmem,) * 10,
    )(
        key_sum,
        query_sum,
        small_sum,
        head_row,
        query_points,
        key_points,
        value_points,
        rotations,
        translations,
        grad_points_t,
    )

    def swap(a):
        return jnp.transpose(a, (0, 2, 1))

    return (
        pair_grad,
        qg.T,
        swap(qpg),
        qfg,
        kg.T,
        vg.T,
        swap(kpg),
        swap(vpg),
        kfg,
        bw.T,
        hw.reshape(H),
    )


def solution(mesh, sizes=(4, 4, 2, 4, 2)):
    finer = Mesh(mesh.devices.reshape(sizes), ROW_COL)
    in_specs = (
        P(ROW, COL, None),
        P(),
        P(),
        P(None, ROW),
        P(None, COL),
        P(None, COL),
        P(None, None, ROW),
        P(None, None, COL),
        P(None, None, COL),
        P(),
        P(),
        P(),
        P(None, ROW),
        P(None, None, ROW),
        P(ROW, None, None),
    )
    out_specs = (
        P(ROW, COL, None),
        P(None, ROW_COL),
        P(None, None, ROW_COL),
        P(None, None, ROW_COL),
        P(None, COL_ROW),
        P(None, COL_ROW),
        P(None, None, COL_ROW),
        P(None, None, COL_ROW),
        P(None, None, COL_ROW),
        P(),
        P(),
    )
    return jax.shard_map(
        functools.partial(per_device, sizes),
        mesh=finer,
        in_specs=in_specs,
        out_specs=out_specs,
        check_vma=False,
    )
```

```python
import functools
import math

import jax
import jax.numpy as jnp
from jax import lax
from jax.experimental import pallas as pl
from jax.experimental.pallas import tpu as pltpu
from jax.sharding import Mesh
from jax.sharding import PartitionSpec as P

ROW = ("row_0", "row_1", "row_2")
COL = ("col_0", "col_1")
ROW_COL = ROW + COL
COL_ROW = COL + ROW

H, C, PQ, PV, CZ = 12, 16, 4, 8, 128
KD, KV, QF = 384, 512, 640
LOGIT = math.sqrt(1.0 / 3.0)
POINT = math.sqrt(2.0 / (9.0 * PQ))
INNER = 1.0 / math.sqrt(C)

F32, BF = jnp.float32, jnp.bfloat16
HIGHEST = lax.Precision.HIGHEST
MESH = pl.DeviceIdType.MESH
VMEM_BYTES = 67043328


def dot(a, b, ca, cb, precision=None):
    return lax.dot_general(
        a, b, (((ca,), (cb,)), ((), ())), precision=precision, preferred_element_type=F32
    )


def split(a):
    hi = a.astype(BF)
    return hi, (a - hi.astype(F32)).astype(BF)


def dot3(a, b, ca, cb):
    (ah, al), (bh, bl) = a, b
    return dot(ah, bh, ca, cb) + dot(ah, bl, ca, cb) + dot(al, bh, ca, cb)


def split3(a):
    first = a.astype(BF)
    rest = a - first.astype(F32)
    second = rest.astype(BF)
    return first, second, (rest - second.astype(F32)).astype(BF)


def dot6(a, b):
    (a1, a2, a3), (b1, b2, b3) = split3(a), split3(b)
    left = jnp.concatenate([a1, a1, a1, a2, a2, a3], axis=0)
    return dot(left, jnp.concatenate([b1, b2, b3, b1, b2, b1], axis=0), 0, 0)


def three(a, axis):
    hi, lo = split(a)
    return jnp.concatenate([hi, hi, lo], axis=axis)


def three_rhs(b):
    hi, lo = split(b)
    return jnp.concatenate([hi, lo, hi], axis=0)


def iota(shape, dim):
    return lax.broadcasted_iota(jnp.int32, shape, dim)


def softplus(x):
    return jnp.maximum(x, 0.0) + jnp.log1p(jnp.exp(-jnp.abs(x)))


def tile_kernel(
    sizes,
    pair_hbm,
    *refs,
):
    inputs, refs = refs[:14], refs[14:]
    sums, refs = refs[:5], refs[5:]
    copies_in, refs = refs[:14], refs[14:]
    tile_body(sizes, pair_hbm, inputs, copies_in, *sums, *copies_in, *refs)


def tile_body(
    sizes,
    pair_hbm,
    inputs,
    copies_in,
    turn_hbm,
    kd_hbm,
    kv_hbm,
    query_hbm,
    small_hbm,
    wt_ref,
    hw_ref,
    q_ref,
    k_ref,
    v_ref,
    qp_ref,
    kp_ref,
    vp_ref,
    rot_ref,
    trans_ref,
    count_ref,
    go_ref,
    gp_ref,
    gpair_ref,
    pair_v,
    turn_v,
    kd_out,
    kv_out,
    query_out,
    small_out,
    s_ref,
    e_ref,
    p_ref,
    d_ref,
    q32,
    k32,
    g48,
    v48,
    vec,
    own_peak,
    stat_own,
    stat_in,
    q_pack,
    g_pack,
    qa,
    qb,
    qv,
    qfeat,
    qt,
    qx,
    qy,
    qz,
    kd_refs,
    kv_refs,
    w_refs,
    in_sem,
    pair_sem,
    out_sem,
    stat_sems,
    qx_sems,
    qz_sems,
    kd_sems,
    kv_sems,
    w_sems,
):
    n0, n1, n2, m0, m1 = sizes
    cols_n = m0 * m1
    rows = q_ref.shape[0]
    cols = k_ref.shape[1]
    i0, i1, i2 = (lax.axis_index(a) for a in ROW)
    j0, j1 = (lax.axis_index(a) for a in COL)
    r = (i0 * n1 + i1) * n2 + i2
    c = j0 * m1 + j1

    def col_peer(d):
        p = lax.rem(c + d, cols_n)
        return {"col_0": p // m1, "col_1": lax.rem(p, m1)}

    groups = {
        "z": (m1 * n0, j1 * n0 + i0, lambda p: {"col_1": p // n0, "row_0": lax.rem(p, n0)}),
        "x": (m0 * n2, j0 * n2 + i2, lambda p: {"col_0": p // n2, "row_2": lax.rem(p, n2)}),
        "y": (n1, i1, lambda p: {"row_1": p}),
    }

    def group_peer(name, d):
        count, here, place = groups[name]
        return place(lax.rem(here + d, count))

    def send(src, dst, sems, n, device):
        copy = pltpu.make_async_remote_copy(
            src_ref=src,
            dst_ref=dst,
            send_sem=sems[0].at[n],
            recv_sem=sems[1].at[n],
            device_id=device,
            device_id_type=MESH,
        )
        copy.start()
        return copy

    parts = pair_sem.shape[0]
    step = rows // parts
    loads = [
        pltpu.make_async_copy(
            pair_hbm.at[pl.ds(b * step, step)], pair_v.at[pl.ds(b * step, step)], pair_sem.at[b]
        )
        for b in range(parts)
    ]
    smalls = [
        pltpu.make_async_copy(src, dst, in_sem.at[n])
        for n, (src, dst) in enumerate(zip(inputs, copies_in))
    ]
    for load in smalls:
        load.start()

    barrier = pltpu.get_barrier_semaphore()
    expected = 0
    for d in range(1, cols_n):
        pl.semaphore_signal(barrier, inc=1, device_id=col_peer(d), device_id_type=MESH)
        expected += 1
    for name in groups:
        for d in range(1, groups[name][0]):
            pl.semaphore_signal(
                barrier, inc=1, device_id=group_peer(name, d), device_id_type=MESH
            )
            expected += 1

    for load in loads:
        load.start()
    for load in smalls:
        load.wait()

    col_start = pl.multiple_of(c * cols, 128)
    row_start = r * rows
    row_base = pl.multiple_of((row_start // 128) * 128, 128)
    row_half = lax.rem(row_start, 128)

    def row_window(w):
        return jnp.where(row_half == 0, w[:, :rows], w[:, 128 - rows :])

    def row_rot(x, y):
        return row_window(rot_ref[x, pl.ds(y, 1), pl.ds(row_base, 128)])

    def col_rot(x, y):
        return rot_ref[x, pl.ds(y, 1), pl.ds(col_start, cols)]

    coef = 0.5 * LOGIT * POINT * softplus(hw_ref[...])

    zero_q = jnp.zeros((2, rows), F32)
    zero_k = jnp.zeros((2, cols), F32)
    q_t = q_ref[...].T * (LOGIT * INNER)
    k_all = k_ref[...]
    rr = [[row_rot(x, y) for y in range(3)] for x in range(3)]
    cr = [[col_rot(x, y) for y in range(3)] for x in range(3)]
    for x in range(3):
        t_row = row_window(trans_ref[pl.ds(x, 1), pl.ds(row_base, 128)])
        t_col = trans_ref[pl.ds(x, 1), pl.ds(col_start, cols)]
        qg = sum(rr[x][y] * qp_ref[y] for y in range(3)) + t_row
        kg = sum(cr[x][y] * kp_ref[y] for y in range(3)) + t_col
        vg = sum(cr[x][y] * vp_ref[y] for y in range(3)) + t_col
        for h in range(H):
            q32[32 * h + 16 + 4 * x : 32 * h + 20 + 4 * x, :] = qg[4 * h : 4 * h + 4]
            k32[32 * h + 16 + 4 * x : 32 * h + 20 + 4 * x, :] = kg[4 * h : 4 * h + 4]
            v48[48 * h + 16 + 8 * x : 48 * h + 24 + 8 * x, :] = vg[8 * h : 8 * h + 8]
    gp_t = [gp_ref[y].T for y in range(3)]
    for x in range(3):
        gg = sum(rr[x][y] * gp_t[y] for y in range(3))
        for h in range(H):
            g48[48 * h + 16 + 8 * x : 48 * h + 24 + 8 * x, :] = gg[8 * h : 8 * h + 8]
    go_t = go_ref[...].T
    for h in range(H):
        q32[32 * h : 32 * h + 16, :] = q_t[16 * h : 16 * h + 16]
        k32[32 * h : 32 * h + 16, :] = k_all[16 * h : 16 * h + 16]
        g48[48 * h : 48 * h + 16, :] = go_t[16 * h : 16 * h + 16]
        v48[48 * h : 48 * h + 16, :] = v_ref[16 * h : 16 * h + 16, :]
        g48[48 * h + 40 : 48 * h + 48, :] = jnp.zeros((8, rows), F32)
        v48[48 * h + 40 : 48 * h + 48, :] = jnp.zeros((8, cols), F32)
        qh = q32[32 * h + 16 : 32 * h + 28, :]
        kh = k32[32 * h + 16 : 32 * h + 28, :]
        q32[32 * h + 28 : 32 * h + 32, :] = jnp.concatenate(
            [jnp.sum(qh * qh, axis=0, keepdims=True), jnp.ones((1, rows), F32), zero_q], axis=0
        )
        k32[32 * h + 28 : 32 * h + 32, :] = jnp.concatenate(
            [jnp.ones((1, cols), F32), jnp.sum(kh * kh, axis=0, keepdims=True), zero_k], axis=0
        )

    def pair_row(at):
        return jnp.concatenate(
            [s_ref[a, pl.ds(at, rows, stride=32), :] for a in range(cols // 128)], axis=1
        )

    def put_pair_row(at, value):
        for a in range(cols // 128):
            s_ref[a, pl.ds(at, rows, stride=32), :] = value[:, 128 * a : 128 * a + 128]

    def pair_block(at, count):
        return jnp.concatenate(
            [s_ref[a, at : at + count, :] for a in range(cols // 128)], axis=1
        )

    w16 = jnp.concatenate([wt_ref[...].astype(F32), jnp.zeros((4, CZ), F32)], axis=0)
    w16b = w16.astype(BF)

    def stack(i):
        gpad = jnp.concatenate(
            [gpair_ref[:, i, :].astype(F32), jnp.zeros((4, CZ), F32)], axis=0
        ).astype(BF)
        return gpad

    point_row = iota((16, 1), 0) < 12
    for h in range(H):
        own = slice(h * rows, (h + 1) * rows)
        kb = k32[32 * h + 16 : 32 * h + 32, :]
        inner = dot6(q32[32 * h : 32 * h + 16, :], k32[32 * h : 32 * h + 16, :])
        dist = dot6(q32[32 * h + 16 : 32 * h + 32, :], jnp.where(point_row, -2.0 * kb, kb))
        d_ref[own, :] = dist
        e_ref[own, :] = inner - coef[:, h : h + 1] * dist
        p_ref[own, :] = dot(
            three(g48[48 * h : 48 * h + 48, :], 0), three_rhs(v48[48 * h : 48 * h + 48, :]), 0, 0
        )

    for b in range(parts):
        loads[b].wait()
        for ii in range(step):
            i = b * step + ii
            both = jnp.concatenate([w16b, stack(i)], axis=0)
            proj = dot(both, pair_v[i], 1, 1)
            for a in range(cols // 128):
                s_ref[a, 32 * i : 32 * i + 32, :] = proj[:, 128 * a : 128 * a + 128]

    valid = col_start + iota((1, cols), 1) < count_ref[0]
    lane = iota((rows, 128), 1)
    for h in range(H):
        own = slice(h * rows, (h + 1) * rows)
        prod = p_ref[own, :] + pair_row(16 + h)
        logits = e_ref[own, :] + LOGIT * pair_row(h)
        logits = jnp.where(valid, logits, -1000000000.0)
        peak = jnp.max(logits, axis=1, keepdims=True)
        e = jnp.exp(logits - peak)
        total = jnp.sum(e, axis=1, keepdims=True)
        upper = jnp.sum(e * prod, axis=1, keepdims=True)
        e_ref[own, :] = e
        p_ref[own, :] = prod
        vec[h * rows : (h + 1) * rows, :] = jnp.where(
            lane == 0, peak + jnp.log(total), jnp.where(lane == 1, upper / total, peak)
        )
    blocks = H * rows // 128
    stat_own[...] = jnp.zeros_like(stat_own)
    own_peak[...] = jnp.zeros_like(own_peak)
    for b in range(blocks):
        turned = vec[128 * b : 128 * b + 128, :].T
        stat_own[b : b + 1, :] = turned[0:1]
        stat_own[8 + b : 9 + b, :] = turned[1:2]
        own_peak[b : b + 1, :] = turned[2:3]

    pl.semaphore_wait(barrier, expected)

    stat_copies = [
        send(stat_own, stat_in.at[d - 1], stat_sems, d - 1, col_peer(d)) for d in range(1, cols_n)
    ]

    for h in range(H):
        own = slice(h * rows, (h + 1) * rows)
        e = e_ref[own, :]
        es = split(e)
        ks = split(k32[32 * h : 32 * h + 32, :])
        qa[32 * h : 32 * h + 32, :] = dot3(ks, split(e * (p_ref[own, :] - vec[own, 1:2])), 1, 1)
        qb[32 * h : 32 * h + 32, :] = dot3(ks, es, 1, 1)
        qv[24 * h : 24 * h + 24, :] = dot3(split(v48[48 * h : 48 * h + 48, :]), es, 1, 1)[16:40]

    for h in range(H):
        q_pack[32 * h : 32 * h + 32, :] = three(q32[32 * h : 32 * h + 32, :], 1)
        g_pack[48 * h : 48 * h + 48, :] = three(g48[48 * h : 48 * h + 48, :], 1)

    for copy in stat_copies:
        copy.wait()

    stats = [stat_own[...]] + [stat_in[d] for d in range(cols_n - 1)]
    peak = functools.reduce(jnp.maximum, [s[0:8] for s in stats])
    weights = [jnp.exp(s[0:8] - peak) for s in stats]
    total = functools.reduce(jnp.add, weights)
    delta = functools.reduce(jnp.add, [w * s[8:16] for w, s in zip(weights, stats)]) / total
    scale = jnp.exp(own_peak[...] - peak) / total
    shift = delta - stats[0][8:16]
    scale_t, delta_t = scale.T, delta.T

    kind = iota((32, 1), 0)
    is_vec = kind < 16

    class Staged:
        def __init__(self, refs, sems, out):
            self.feat, self.kt, self.k1, self.p1, self.k2, self.p2, self.k3 = refs
            self.sems = (sems[0:2], sems[2:4], sems[4:6])
            self.out = out

        def turn(self):
            share = self.kt.shape[2]
            per = 128 // (share * n2)
            for a in range(self.feat.shape[0] // 128):
                for b in range(cols // 128):
                    block = self.feat[128 * a : 128 * a + 128, 128 * b : 128 * b + 128].T
                    self.kt[b * per : (b + 1) * per, :, :, 128 * a : 128 * a + 128] = block.reshape(
                        per, n2, share, 128
                    )

        def send1(self):
            other = lax.rem(i2 + 1, n2)
            self.copies = [send(self.kt.at[:, other], self.k1, self.sems[0], 0, {"row_2": other})]

        def wait(self):
            for copy in self.copies:
                copy.wait()

        def send2(self):
            self.wait()
            self.p1[...] = (self.kt[:, i2] + self.k1[...]).reshape(self.p1.shape)
            self.copies = []
            for d in range(1, n1):
                to = lax.rem(i1 + d, n1)
                self.copies.append(
                    send(self.p1.at[:, to], self.k2.at[d - 1], self.sems[1], d - 1, {"row_1": to})
                )

        def send3(self):
            self.wait()
            self.p2[...] = self.p1[:, i1] + functools.reduce(
                jnp.add, [self.k2[d] for d in range(n1 - 1)]
            )
            self.copies = []
            for d in range(1, n0):
                to = lax.rem(i0 + d, n0)
                self.copies.append(
                    send(self.p2.at[to], self.k3.at[d - 1], self.sems[2], d - 1, {"row_0": to})
                )

        def finish(self):
            self.wait()
            self.out[...] = self.p2[i0] + functools.reduce(
                jnp.add, [self.k3[d] for d in range(n0 - 1)]
            )

    side_d = Staged(kd_refs, kd_sems, kd_out)
    side_v = Staged(kv_refs, kv_sems, kv_out)

    head_sum = jnp.zeros((1, 128), F32)
    lane1 = iota((1, 128), 1)
    side_d.feat[336:KD, :] = jnp.zeros((KD - 336, cols), F32)
    side_v.feat[480:KV, :] = jnp.zeros((KV - 480, cols), F32)
    for h in range(H):
        own = slice(h * rows, (h + 1) * rows)
        at = (slice(rows * (h % 2), rows * (h % 2) + rows), slice(h // 2, h // 2 + 1))
        attn = e_ref[own, :] * scale_t[at]
        dlog = attn * (p_ref[own, :] - delta_t[at])
        moment = jnp.sum(jnp.sum(dlog * d_ref[own, :], axis=0, keepdims=True), axis=1, keepdims=True)
        head_sum = jnp.where(lane1 == h, moment, head_sum)
        put_pair_row(h, dlog)
        put_pair_row(16 + h, attn)
        e_ref[own, :] = attn
        two = 2.0 * coef[:, h : h + 1]
        kd = dot(q_pack[32 * h : 32 * h + 32, :], three_rhs(dlog), 1, 0)
        col_sum = kd[29:30]
        kd = jnp.where(is_vec, kd, two * (kd - k32[32 * h : 32 * h + 32, :] * col_sum))
        side_d.feat[16 * h : 16 * h + 16, :] = kd[0:16]
        for x in range(3):
            to = 192 + 48 * x + 4 * h
            side_d.feat[to : to + 4, :] = kd[16 + 4 * x : 20 + 4 * x]
    side_d.turn()
    side_d.send1()

    for h in range(H):
        own = slice(h * rows, (h + 1) * rows)
        ka = dot(g_pack[48 * h : 48 * h + 48, :], three_rhs(e_ref[own, :]), 1, 0)
        side_v.feat[16 * h : 16 * h + 16, :] = ka[0:16]
        for x in range(3):
            to = 192 + 96 * x + 8 * h
            side_v.feat[to : to + 8, :] = ka[16 + 8 * x : 24 + 8 * x]
    side_v.turn()
    side_v.send1()

    acc = jnp.zeros((16, CZ), F32)
    for i in range(rows):
        acc = acc + dot(pair_block(32 * i, 16).astype(BF), pair_v[i], 1, 0)

    class Small:
        def __init__(self, value):
            w_refs[0][...] = value
            self.level = 0

        def send(self, name):
            at = self.level
            self.copies = [
                send(
                    w_refs[2 * at],
                    w_refs[2 * at + 1].at[d - 1],
                    w_sems[2 * at : 2 * at + 2],
                    d - 1,
                    group_peer(name, d),
                )
                for d in range(1, groups[name][0])
            ]

        def add(self):
            for copy in self.copies:
                copy.wait()
            here, came = w_refs[2 * self.level], w_refs[2 * self.level + 1]
            total = here[...] + functools.reduce(
                jnp.add, [came[d] for d in range(came.shape[0])]
            )
            self.level += 1
            if self.level < 3:
                w_refs[2 * self.level][...] = total
            return total

    small = Small(jnp.where(iota((16, 1), 0) == 12, head_sum, LOGIT * acc))
    small.send("z")

    side_d.send2()

    for h in range(H):
        at = (slice(h // 2, h // 2 + 1), slice(rows * (h % 2), rows * (h % 2) + rows))
        two = 2.0 * coef[:, h : h + 1]
        head = slice(32 * h, 32 * h + 32)
        qd = scale[at] * (qa[head, :] - shift[at] * qb[head, :])
        row_sum = qd[28:29]
        qd = jnp.where(is_vec, LOGIT * INNER * qd, two * (qd - q32[head, :] * row_sum))
        opt = scale[at] * qv[24 * h : 24 * h + 24, :]
        qfeat[16 * h : 16 * h + 16, :] = qd[0:16]
        for x in range(3):
            to = 192 + 48 * x + 4 * h
            qfeat[to : to + 4, :] = qd[16 + 4 * x : 20 + 4 * x]
            to = 336 + 96 * x + 8 * h
            qfeat[to : to + 8, :] = opt[8 * x : 8 * x + 8]
    qfeat[624:QF, :] = jnp.zeros((QF - 624, rows), F32)
    for a in range(QF // 128):
        qt[:, :, 128 * a : 128 * a + 128] = qfeat[128 * a : 128 * a + 128, :].T.reshape(
            qt.shape[0], qt.shape[1], 128
        )
    qx_copies = []
    for d in range(1, m0):
        to = lax.rem(j0 + d, m0)
        qx_copies.append(
            send(qt.at[pl.ds(to * m1, m1)], qx.at[d - 1], qx_sems, d - 1, {"col_0": to})
        )

    side_v.send2()

    for b in range(rows // 4):
        turn_v[b] = pair_block(128 * b, 128).T.astype(BF)
    turn_copy = pltpu.make_async_copy(turn_v, turn_hbm, out_sem.at[0])
    turn_copy.start()

    small.add()
    small.send("x")
    side_d.send3()
    for copy in qx_copies:
        copy.wait()
    qy[...] = qt[pl.ds(j0 * m1, m1)] + functools.reduce(jnp.add, [qx[d] for d in range(m0 - 1)])
    qz_copies = []
    for d in range(1, m1):
        to = lax.rem(j1 + d, m1)
        qz_copies.append(send(qy.at[to], qz.at[d - 1], qz_sems, d - 1, {"col_1": to}))
    side_v.send3()
    small.add()
    small.send("y")
    side_d.finish()
    side_v.finish()
    for copy in qz_copies:
        copy.wait()
    query_out[...] = functools.reduce(jnp.add, [qz[d] for d in range(m1 - 1)], qy[j1])
    small_out[...] = small.add()
    outs = [
        pltpu.make_async_copy(query_out, query_hbm, out_sem.at[1]),
        pltpu.make_async_copy(kd_out, kd_hbm, out_sem.at[2]),
        pltpu.make_async_copy(kv_out, kv_hbm, out_sem.at[3]),
        pltpu.make_async_copy(small_out, small_hbm, out_sem.at[4]),
    ]
    for copy in outs:
        copy.start()
    for copy in outs + [turn_copy]:
        copy.wait()


def finish_kernel(sizes, *refs):
    inputs, refs = refs[:14], refs[14:]
    outs, refs = refs[:11], refs[11:]
    copies_in, refs = refs[:14], refs[14:]
    results, (pg_v, in_sem, pg_sem, out_sem) = refs[:10], refs[10:]
    turn_ref, wt_ref, gpair_ref = copies_in[:3]
    loads = [
        pltpu.make_async_copy(src, dst, in_sem.at[n])
        for n, (src, dst) in enumerate(zip(inputs, copies_in))
    ]
    for load in loads:
        load.start()
    for load in loads[:3]:
        load.wait()

    rows = pg_v.shape[0]
    zero4 = jnp.zeros((4, CZ), F32)
    w16s = jnp.concatenate([LOGIT * wt_ref[...].astype(F32), zero4], axis=0).astype(BF)
    zero32 = jnp.zeros((32, CZ), BF)

    def weights(i):
        gpad = jnp.concatenate([gpair_ref[:, i, :].astype(F32), zero4], axis=0).astype(BF)
        return jnp.concatenate([w16s, gpad], axis=0)

    stores = []
    parts = pg_sem.shape[0]
    step = rows // parts
    for b in range(rows // 4):
        for half in range(2):
            first, second = 4 * b + 2 * half, 4 * b + 2 * half + 1
            left = [zero32] * 4
            right = [zero32] * 4
            left[2 * half], right[2 * half + 1] = weights(first), weights(second)
            block = jnp.concatenate(
                [jnp.concatenate(left, axis=0), jnp.concatenate(right, axis=0)], axis=1
            )
            out = dot(turn_ref[b], block, 1, 0)
            pg_v[first] = out[:, :CZ].astype(BF)
            pg_v[second] = out[:, CZ:].astype(BF)
        if 4 * (b + 1) % step == 0:
            p = 4 * (b + 1) // step - 1
            store = pltpu.make_async_copy(
                pg_v.at[pl.ds(p * step, step)], outs[0].at[pl.ds(p * step, step)], pg_sem.at[p]
            )
            store.start()
            stores.append(store)

    for load in loads[3:]:
        load.wait()
    finish_body(sizes, *copies_in[3:], *results)
    for n, (src, dst) in enumerate(zip(results, outs[1:])):
        store = pltpu.make_async_copy(src, dst, out_sem.at[n])
        store.start()
        stores.append(store)
    for store in stores:
        store.wait()


def finish_body(
    sizes,
    kd_ref,
    kv_ref,
    query_ref,
    small_ref,
    hw_ref,
    qp_ref,
    kp_ref,
    vp_ref,
    rot_ref,
    trans_ref,
    gp_ref,
    qg_out,
    qpg_out,
    qfg_out,
    kg_out,
    vg_out,
    kpg_out,
    vpg_out,
    kfg_out,
    bw_out,
    hw_out,
):
    n0, n1, n2, m0, m1 = sizes
    share, qshare = kd_ref.shape[0], query_ref.shape[0]
    rows, cols = gp_ref.shape[1], kp_ref.shape[2]
    i0, i1, i2 = (lax.axis_index(a) for a in ROW)
    j0, j1 = (lax.axis_index(a) for a in COL)
    r = (i0 * n1 + i1) * n2 + i2
    c = j0 * m1 + j1

    def pick(count, width, at):
        return (iota((count, width), 1) == iota((count, width), 0) + at).astype(F32)

    def take(sel, array):
        return dot(sel, array, 1, 1, HIGHEST)

    def frames(start, count):
        base = pl.multiple_of((start // 128) * 128, 128)
        sel = pick(count, 128, start - base)
        rot = [take(sel, rot_ref[x, :, pl.ds(base, 128)]) for x in range(3)]
        return rot, take(sel, trans_ref[:, pl.ds(base, 128)])

    def column(a, y):
        return a[:, y : y + 1]

    def total(a):
        return jnp.sum(a, axis=1, keepdims=True)

    def put_frame(out, parts):
        count = parts[0][0].shape[0]
        for x in range(3):
            lane = iota((count, 128), 1)
            wide = jnp.zeros((count, 128), F32)
            for y in range(4):
                wide = jnp.where(lane == y, parts[x][y], wide)
            if count % 8:
                wide = jnp.concatenate([wide, jnp.zeros((8 - count % 8, 128), F32)], axis=0)
            out[x] = wide.T[0:4, :count]

    rot, anchor = frames(r * rows + c * qshare, qshare)
    local_sel = pick(qshare, rows, c * qshare)
    summed = query_ref[...]
    qg_out[...] = summed[:, 0:192]
    dqg = [summed[:, 192 + 48 * x : 240 + 48 * x] for x in range(3)]
    opt = [summed[:, 336 + 96 * x : 432 + 96 * x] for x in range(3)]
    local = [take(local_sel, qp_ref[y]) for y in range(3)]
    cotan = [gp_ref[y, pl.ds(c * qshare, qshare), :] for y in range(3)]
    for y in range(3):
        qpg_out[y] = sum(column(rot[x], y) * dqg[x] for x in range(3))
    parts = []
    for x in range(3):
        shifted = opt[x] - column(anchor, x)
        turned = sum(column(rot[x], y) * cotan[y] for y in range(3))
        parts.append(
            [total(dqg[x] * local[y]) + total(shifted * cotan[y]) for y in range(3)]
            + [total(dqg[x]) - total(turned)]
        )
    put_frame(qfg_out, parts)

    rot, anchor = frames(c * cols + r * share, share)
    local_sel = pick(share, cols, r * share)
    summed = kd_ref[...]
    kg_out[...] = summed[:, 0:192]
    dkg = [summed[:, 192 + 48 * x : 240 + 48 * x] for x in range(3)]
    summed = kv_ref[...]
    vg_out[...] = summed[:, 0:192]
    dvg = [summed[:, 192 + 96 * x : 288 + 96 * x] for x in range(3)]
    klocal = [take(local_sel, kp_ref[y]) for y in range(3)]
    vlocal = [take(local_sel, vp_ref[y]) for y in range(3)]
    for y in range(3):
        kpg_out[y] = sum(column(rot[x], y) * dkg[x] for x in range(3))
        vpg_out[y] = sum(column(rot[x], y) * dvg[x] for x in range(3))
    parts = []
    for x in range(3):
        parts.append(
            [total(dkg[x] * klocal[y]) + total(dvg[x] * vlocal[y]) for y in range(3)]
            + [total(dkg[x]) + total(dvg[x])]
        )
    put_frame(kfg_out, parts)

    bw_out[...] = small_ref[0:H, :]
    raw = hw_ref[...]
    hw_out[...] = small_ref[12:13, 0:H] * (-0.5 * LOGIT * POINT) / (1.0 + jnp.exp(-raw))


def per_device(
    sizes,
    pair_rep,
    bias_weight,
    head_weight,
    queries,
    key_vectors,
    values,
    query_points,
    key_points,
    value_points,
    rotations,
    translations,
    residue_count,
    grad_output,
    grad_points,
    grad_pair,
):
    n0, n1, n2, m0, m1 = sizes
    cols_n = m0 * m1
    rows, cols = pair_rep.shape[:2]
    share, qshare = cols // (n0 * n1 * n2), rows // cols_n
    head_row = head_weight.reshape(1, H)
    grad_points_t = jnp.transpose(grad_points, (0, 2, 1))
    hbm = pl.BlockSpec(memory_space=pl.ANY)
    dma = pltpu.SemaphoreType.DMA
    params = dict(vmem_limit_bytes=VMEM_BYTES)

    def buf(*shape, dtype=F32):
        return pltpu.VMEM(shape, dtype)

    def like(array):
        space = pltpu.VMEM if array.size > 1 else pltpu.SMEM
        return space(array.shape, array.dtype)

    weight_t = bias_weight.T
    grad_pair_t = jnp.transpose(grad_pair, (1, 0, 2))
    operands = (
        weight_t,
        head_row,
        queries.T,
        key_vectors,
        values,
        query_points,
        key_points,
        value_points,
        rotations,
        translations,
        residue_count,
        grad_output.T,
        grad_points_t,
        grad_pair_t,
    )
    sums = (
        jax.ShapeDtypeStruct((rows // 4, cols, 128), BF),
        jax.ShapeDtypeStruct((share, KD), F32),
        jax.ShapeDtypeStruct((share, KV), F32),
        jax.ShapeDtypeStruct((qshare, QF), F32),
        jax.ShapeDtypeStruct((16, CZ), F32),
    )

    def staged(width):
        return (
            buf(width, cols),
            buf(n0 * n1, n2, share, width),
            buf(n0 * n1, share, width),
            buf(n0, n1, share, width),
            buf(n1 - 1, n0, share, width),
            buf(n0, share, width),
            buf(n0 - 1, share, width),
        )

    def pairs(*counts):
        return tuple(dma((n,)) for n in counts for _ in range(2))

    levels = (m1 * n0, m0 * n2, n1)
    turned, kd_sum, kv_sum, query_sum, small_sum = pl.pallas_call(
        functools.partial(tile_kernel, sizes),
        name="tile",
        out_shape=sums,
        in_specs=[hbm] * (1 + len(operands)),
        out_specs=(hbm,) * 5,
        scratch_shapes=[
            *[like(a) for a in operands],
            like(pair_rep),
            *[like(a) for a in sums],
            buf(cols // 128, rows * 32, 128),
            buf(H * rows, cols),
            buf(H * rows, cols),
            buf(H * rows, cols),
            buf(H * 32, rows),
            buf(H * 32, cols),
            buf(H * 48, rows),
            buf(H * 48, cols),
            buf(H * rows, 128),
            buf(8, 128),
            buf(16, 128),
            buf(cols_n - 1, 16, 128),
            buf(H * 32, 3 * rows, dtype=BF),
            buf(H * 48, 3 * rows, dtype=BF),
            buf(H * 32, rows),
            buf(H * 32, rows),
            buf(H * 24, rows),
            buf(QF, rows),
            buf(cols_n, qshare, QF),
            buf(m0 - 1, m1, qshare, QF),
            buf(m1, qshare, QF),
            buf(max(m1 - 1, 1), qshare, QF),
            staged(KD),
            staged(KV),
            tuple(b for n in levels for b in (buf(16, CZ), buf(n - 1, 16, CZ))),
            dma((len(operands),)),
            dma((4,)),
            dma((len(sums),)),
            pairs(cols_n - 1),
            pairs(m0 - 1),
            pairs(max(m1 - 1, 1)),
            pairs(1, n1 - 1, n0 - 1),
            pairs(1, n1 - 1, n0 - 1),
            pairs(*[n - 1 for n in levels]),
        ],
        compiler_params=pltpu.CompilerParams(collective_id=0, has_side_effects=True, **params),
    )(pair_rep, *operands)
    operands = (
        turned,
        weight_t,
        grad_pair_t,
        kd_sum,
        kv_sum,
        query_sum,
        small_sum,
        head_row,
        query_points,
        key_points,
        value_points,
        rotations,
        translations,
        grad_points_t,
    )
    results = (
        jax.ShapeDtypeStruct((qshare, 192), F32),
        jax.ShapeDtypeStruct((3, qshare, 48), F32),
        jax.ShapeDtypeStruct((3, 4, qshare), F32),
        jax.ShapeDtypeStruct((share, 192), F32),
        jax.ShapeDtypeStruct((share, 192), F32),
        jax.ShapeDtypeStruct((3, share, 48), F32),
        jax.ShapeDtypeStruct((3, share, 96), F32),
        jax.ShapeDtypeStruct((3, 4, share), F32),
        jax.ShapeDtypeStruct((H, CZ), F32),
        jax.ShapeDtypeStruct((1, H), F32),
    )
    pair_grad, qg, qpg, qfg, kg, vg, kpg, vpg, kfg, bw, hw = pl.pallas_call(
        functools.partial(finish_kernel, sizes),
        name="finish",
        out_shape=(jax.ShapeDtypeStruct(pair_rep.shape, BF), *results),
        in_specs=[hbm] * len(operands),
        out_specs=(hbm,) * 11,
        scratch_shapes=[
            *[like(a) for a in operands],
            *[like(a) for a in results],
            like(pair_rep),
            dma((len(operands),)),
            dma((4,)),
            dma((len(results),)),
        ],
        compiler_params=pltpu.CompilerParams(**params),
    )(*operands)

    def swap(a):
        return jnp.transpose(a, (0, 2, 1))

    return (
        pair_grad,
        qg.T,
        swap(qpg),
        qfg,
        kg.T,
        vg.T,
        swap(kpg),
        swap(vpg),
        kfg,
        bw.T,
        hw.reshape(H),
    )


def solution(mesh, sizes=(4, 4, 2, 4, 2)):
    finer = Mesh(mesh.devices.reshape(sizes), ROW_COL)
    in_specs = (
        P(ROW, COL, None),
        P(),
        P(),
        P(None, ROW),
        P(None, COL),
        P(None, COL),
        P(None, None, ROW),
        P(None, None, COL),
        P(None, None, COL),
        P(),
        P(),
        P(),
        P(None, ROW),
        P(None, None, ROW),
        P(ROW, None, None),
    )
    out_specs = (
        P(ROW, COL, None),
        P(None, ROW_COL),
        P(None, None, ROW_COL),
        P(None, None, ROW_COL),
        P(None, COL_ROW),
        P(None, COL_ROW),
        P(None, None, COL_ROW),
        P(None, None, COL_ROW),
        P(None, None, COL_ROW),
        P(),
        P(),
    )
    return jax.shard_map(
        functools.partial(per_device, sizes),
        mesh=finer,
        in_specs=in_specs,
        out_specs=out_specs,
        check_vma=False,
    )
```

```python
import functools
import math

import jax
import jax.numpy as jnp
from jax import lax
from jax.experimental import pallas as pl
from jax.experimental.pallas import tpu as pltpu
from jax.sharding import Mesh
from jax.sharding import PartitionSpec as P

ROW = ("row_0", "row_1", "row_2")
COL = ("col_0", "col_1")
ROW_COL = ROW + COL
COL_ROW = COL + ROW

H, C, PQ, PV, CZ = 12, 16, 4, 8, 128
KD, KV, QF = 384, 512, 640
ROT_Q, ROT_K, SEL_Q, SEL_D, SEL_V, SEL_C = 0, 9, 18, 30, 36, 45


def frame_lines(values, count):
    diagonal = iota((count, 128), 0) == iota((count, 128), 1)
    return [
        jnp.sum(jnp.where(diagonal, v, 0.0), axis=0, keepdims=True)[:, :count] for v in values
    ]
LOGIT = math.sqrt(1.0 / 3.0)
POINT = math.sqrt(2.0 / (9.0 * PQ))
INNER = 1.0 / math.sqrt(C)

F32, BF = jnp.float32, jnp.bfloat16
HIGHEST = lax.Precision.HIGHEST
MESH = pl.DeviceIdType.MESH
VMEM_BYTES = 67043328


def dot(a, b, ca, cb, precision=None):
    return lax.dot_general(
        a, b, (((ca,), (cb,)), ((), ())), precision=precision, preferred_element_type=F32
    )


def split(a):
    hi = a.astype(BF)
    return hi, (a - hi.astype(F32)).astype(BF)


def dot3(a, b, ca, cb):
    (ah, al), (bh, bl) = a, b
    return dot(ah, bh, ca, cb) + dot(ah, bl, ca, cb) + dot(al, bh, ca, cb)


def split3(a):
    first = a.astype(BF)
    rest = a - first.astype(F32)
    second = rest.astype(BF)
    return first, second, (rest - second.astype(F32)).astype(BF)


def dot6(a, b):
    (a1, a2, a3), (b1, b2, b3) = split3(a), split3(b)
    left = jnp.concatenate([a1, a1, a1, a2, a2, a3], axis=0)
    return dot(left, jnp.concatenate([b1, b2, b3, b1, b2, b1], axis=0), 0, 0)


def three(a, axis):
    hi, lo = split(a)
    return jnp.concatenate([hi, hi, lo], axis=axis)


def three_rhs(b):
    hi, lo = split(b)
    return jnp.concatenate([hi, lo, hi], axis=0)


def iota(shape, dim):
    return lax.broadcasted_iota(jnp.int32, shape, dim)


def softplus(x):
    return jnp.maximum(x, 0.0) + jnp.log1p(jnp.exp(-jnp.abs(x)))


def tile_kernel(
    sizes,
    pair_hbm,
    *refs,
):
    inputs, refs = refs[:14], refs[14:]
    sums, refs = refs[:6], refs[6:]
    copies_in, refs = refs[:14], refs[14:]
    tile_body(sizes, pair_hbm, inputs, copies_in, *sums, *copies_in, *refs)


def tile_body(
    sizes,
    pair_hbm,
    inputs,
    copies_in,
    turn_hbm,
    kd_hbm,
    kv_hbm,
    query_hbm,
    small_hbm,
    sel_hbm,
    wt_ref,
    hw_ref,
    q_ref,
    k_ref,
    v_ref,
    qp_ref,
    kp_ref,
    vp_ref,
    rot_ref,
    trans_ref,
    count_ref,
    go_ref,
    gp_ref,
    gpair_ref,
    pair_v,
    turn_v,
    kd_out,
    kv_out,
    query_out,
    small_out,
    sel_out,
    turn_buf,
    wide_d,
    wide_v,
    s_ref,
    pair_t,
    ub_ref,
    x_ref,
    e_ref,
    p_ref,
    d_ref,
    q32,
    k32,
    g48,
    v48,
    vec,
    own_peak,
    own_dist,
    stat_own,
    stat_in,
    q_pack,
    g_pack,
    qa,
    qb,
    qv,
    qfeat,
    qt,
    qx,
    qy,
    qz,
    kd_refs,
    kv_refs,
    w_refs,
    in_sem,
    pair_sem,
    out_sem,
    stat_sems,
    qx_sems,
    qz_sems,
    kd_sems,
    kv_sems,
    w_sems,
):
    n0, n1, n2, m0, m1 = sizes
    cols_n = m0 * m1
    rows = q_ref.shape[0]
    cols = k_ref.shape[1]
    i0, i1, i2 = (lax.axis_index(a) for a in ROW)
    j0, j1 = (lax.axis_index(a) for a in COL)
    r = (i0 * n1 + i1) * n2 + i2
    c = j0 * m1 + j1

    def col_peer(d):
        p = lax.rem(c + d, cols_n)
        return {"col_0": p // m1, "col_1": lax.rem(p, m1)}

    groups = {
        "z": (m1 * n0, j1 * n0 + i0, lambda p: {"col_1": p // n0, "row_0": lax.rem(p, n0)}),
        "x": (m0 * n2, j0 * n2 + i2, lambda p: {"col_0": p // n2, "row_2": lax.rem(p, n2)}),
        "y": (n1, i1, lambda p: {"row_1": p}),
    }

    def group_peer(name, d):
        count, here, place = groups[name]
        return place(lax.rem(here + d, count))

    def send(src, dst, sems, n, device):
        copy = pltpu.make_async_remote_copy(
            src_ref=src,
            dst_ref=dst,
            send_sem=sems[0].at[n],
            recv_sem=sems[1].at[n],
            device_id=device,
            device_id_type=MESH,
        )
        copy.start()
        return copy

    parts = pair_sem.shape[0]
    step = rows // parts
    loads = [
        pltpu.make_async_copy(
            pair_hbm.at[pl.ds(b * step, step)], pair_v.at[pl.ds(b * step, step)], pair_sem.at[b]
        )
        for b in range(parts)
    ]
    smalls = [
        pltpu.make_async_copy(src, dst, in_sem.at[n])
        for n, (src, dst) in enumerate(zip(inputs, copies_in))
    ]
    for load in smalls + loads[:2]:
        load.start()

    barrier = pltpu.get_barrier_semaphore()
    expected = 0
    for d in range(1, cols_n):
        pl.semaphore_signal(barrier, inc=1, device_id=col_peer(d), device_id_type=MESH)
        expected += 1
    for name in groups:
        for d in range(1, groups[name][0]):
            pl.semaphore_signal(
                barrier, inc=1, device_id=group_peer(name, d), device_id_type=MESH
            )
            expected += 1

    for load in loads[2:]:
        load.start()
    for load in smalls:
        load.wait()

    col_start = pl.multiple_of(c * cols, 128)
    row_start = r * rows
    row_base = pl.multiple_of((row_start // 128) * 128, 128)
    row_half = lax.rem(row_start, 128)

    def row_window(w):
        return jnp.where(row_half == 0, w[:, :rows], w[:, 128 - rows :])

    def row_rot(x, y):
        return row_window(rot_ref[x, pl.ds(y, 1), pl.ds(row_base, 128)])

    def col_rot(x, y):
        return rot_ref[x, pl.ds(y, 1), pl.ds(col_start, cols)]

    coef = 0.5 * LOGIT * POINT * softplus(hw_ref[...])

    zero_q = jnp.zeros((2, rows), F32)
    zero_k = jnp.zeros((2, cols), F32)
    q_t = q_ref[...].T * (LOGIT * INNER)
    k_all = k_ref[...]
    rr = [[row_rot(x, y) for y in range(3)] for x in range(3)]
    cr = [[col_rot(x, y) for y in range(3)] for x in range(3)]
    for x in range(3):
        t_row = row_window(trans_ref[pl.ds(x, 1), pl.ds(row_base, 128)])
        t_col = trans_ref[pl.ds(x, 1), pl.ds(col_start, cols)]
        qg = sum(rr[x][y] * qp_ref[y] for y in range(3)) + t_row
        kg = sum(cr[x][y] * kp_ref[y] for y in range(3)) + t_col
        vg = sum(cr[x][y] * vp_ref[y] for y in range(3)) + t_col
        for h in range(H):
            q32[32 * h + 16 + 4 * x : 32 * h + 20 + 4 * x, :] = qg[4 * h : 4 * h + 4]
            k32[32 * h + 16 + 4 * x : 32 * h + 20 + 4 * x, :] = kg[4 * h : 4 * h + 4]
            v48[48 * h + 16 + 8 * x : 48 * h + 24 + 8 * x, :] = vg[8 * h : 8 * h + 8]
    gp_t = [gp_ref[y].T for y in range(3)]
    for x in range(3):
        gg = sum(rr[x][y] * gp_t[y] for y in range(3))
        for h in range(H):
            g48[48 * h + 16 + 8 * x : 48 * h + 24 + 8 * x, :] = gg[8 * h : 8 * h + 8]
    go_t = go_ref[...].T
    for h in range(H):
        q32[32 * h : 32 * h + 16, :] = q_t[16 * h : 16 * h + 16]
        k32[32 * h : 32 * h + 16, :] = k_all[16 * h : 16 * h + 16]
        g48[48 * h : 48 * h + 16, :] = go_t[16 * h : 16 * h + 16]
        v48[48 * h : 48 * h + 16, :] = v_ref[16 * h : 16 * h + 16, :]
        g48[48 * h + 40 : 48 * h + 48, :] = jnp.zeros((8, rows), F32)
        v48[48 * h + 40 : 48 * h + 48, :] = jnp.zeros((8, cols), F32)
        qh = q32[32 * h + 16 : 32 * h + 28, :]
        kh = k32[32 * h + 16 : 32 * h + 28, :]
        q32[32 * h + 28 : 32 * h + 32, :] = jnp.concatenate(
            [jnp.sum(qh * qh, axis=0, keepdims=True), jnp.ones((1, rows), F32), zero_q], axis=0
        )
        k32[32 * h + 28 : 32 * h + 32, :] = jnp.concatenate(
            [jnp.ones((1, cols), F32), jnp.sum(kh * kh, axis=0, keepdims=True), zero_k], axis=0
        )

    w16 = jnp.concatenate([wt_ref[...].astype(F32), jnp.zeros((4, CZ), F32)], axis=0)
    w16b = w16.astype(BF)

    def stack(i):
        gpad = jnp.concatenate(
            [gpair_ref[:, i, :].astype(F32), jnp.zeros((4, CZ), F32)], axis=0
        ).astype(BF)
        return gpad

    e_ref[H:16] = jnp.zeros((16 - H, rows, cols), F32)
    p_ref[H:16] = jnp.zeros((16 - H, rows, cols), F32)
    point_row = iota((16, 1), 0) < 12
    for h in range(H):
        kb = k32[32 * h + 16 : 32 * h + 32, :]
        inner = dot6(q32[32 * h : 32 * h + 16, :], k32[32 * h : 32 * h + 16, :])
        dist = dot6(q32[32 * h + 16 : 32 * h + 32, :], jnp.where(point_row, -2.0 * kb, kb))
        d_ref[h] = dist
        e_ref[h] = inner - coef[:, h : h + 1] * dist
        p_ref[h] = dot(
            three(g48[48 * h : 48 * h + 48, :], 0), three_rhs(v48[48 * h : 48 * h + 48, :]), 0, 0
        )

    for b in range(parts):
        loads[b].wait()
        for ib in range(b * step // 8, (b + 1) * step // 8):
            proj = []
            for i in range(8 * ib, 8 * ib + 8):
                both = jnp.concatenate([w16b, stack(i)], axis=0)
                if i % 4 == 3:
                    proj.append(dot(both, pair_v[i], 1, 1))
                else:
                    pair_t[i] = pair_v[i].T
                    proj.append(dot(both, pair_t[i], 1, 0))
            s_ref[:, 8 * ib : 8 * ib + 8, :] = jnp.transpose(jnp.stack(proj), (1, 0, 2))

    valid = col_start + iota((1, cols), 1) < count_ref[0]
    lane = iota((rows, 128), 1)
    for h in range(H):
        prod = p_ref[h] + s_ref[16 + h]
        logits = e_ref[h] + LOGIT * s_ref[h]
        logits = jnp.where(valid, logits, -1000000000.0)
        peak = jnp.max(logits, axis=1, keepdims=True)
        e = jnp.exp(logits - peak)
        total = jnp.sum(e, axis=1, keepdims=True)
        upper = jnp.sum(e * prod, axis=1, keepdims=True)
        e_ref[h] = e
        p_ref[h] = prod
        vec[h * rows : (h + 1) * rows, :] = jnp.where(
            lane == 0, peak + jnp.log(total), jnp.where(lane == 1, upper / total, peak)
        )
    blocks = H * rows // 128
    stat_own[...] = jnp.zeros_like(stat_own)
    own_peak[...] = jnp.zeros_like(own_peak)
    own_dist[...] = jnp.zeros_like(own_dist)
    for b in range(blocks):
        turned = vec[128 * b : 128 * b + 128, :].T
        stat_own[b : b + 1, :] = turned[0:1]
        stat_own[8 + b : 9 + b, :] = turned[1:2]
        own_peak[b : b + 1, :] = turned[2:3]

    pl.semaphore_wait(barrier, expected)

    stat_copies = [
        send(stat_own, stat_in.at[d - 1], stat_sems, d - 1, col_peer(d)) for d in range(1, cols_n)
    ]

    for a in (6, 14, 22, 30):
        s_ref[a : a + 2] = jnp.zeros((2, rows, cols), F32)
    for h in range(H):
        own = slice(h * rows, (h + 1) * rows)
        e = e_ref[h]
        es = split(e)
        ep = e * (p_ref[h] - vec[own, 1:2])
        ks = split(k32[32 * h : 32 * h + 32, :])
        qa[32 * h : 32 * h + 32, :] = dot3(ks, split(ep), 1, 1)
        qb[32 * h : 32 * h + 32, :] = dot3(ks, es, 1, 1)
        qv[24 * h : 24 * h + 24, :] = dot3(split(v48[48 * h : 48 * h + 48, :]), es, 1, 1)[16:40]
        s_ref[8 * (h % 2) + h // 2] = ep
        s_ref[16 + 8 * (h % 2) + h // 2] = e
        dist = d_ref[h]
        vec[own, :] = jnp.where(
            lane == 0,
            jnp.sum(ep * dist, axis=1, keepdims=True),
            jnp.sum(e * dist, axis=1, keepdims=True),
        )
    for b in range(blocks):
        turned = vec[128 * b : 128 * b + 128, :].T
        own_dist[b : b + 1, :] = turned[0:1]
        own_dist[8 + b : 9 + b, :] = turned[1:2]
    for ib in range(rows // 8):
        by_query = jnp.transpose(s_ref[:, 8 * ib : 8 * ib + 8, :], (1, 0, 2))
        for ii in range(8):
            both = dot(jnp.concatenate(split(by_query[ii]), axis=0), pair_v[8 * ib + ii], 1, 0)
            ub_ref[8 * ib + ii] = both[0:32] + both[32:64]
    for h in range(H):
        q_pack[32 * h : 32 * h + 32, :] = three(q32[32 * h : 32 * h + 32, :], 1)
        g_pack[48 * h : 48 * h + 48, :] = three(g48[48 * h : 48 * h + 48, :], 1)

    for copy in stat_copies:
        copy.wait()

    stats = [stat_own[...]] + [stat_in[d] for d in range(cols_n - 1)]
    peak = functools.reduce(jnp.maximum, [s[0:8] for s in stats])
    weights = [jnp.exp(s[0:8] - peak) for s in stats]
    total = functools.reduce(jnp.add, weights)
    delta = functools.reduce(jnp.add, [w * s[8:16] for w, s in zip(weights, stats)]) / total
    scale = jnp.exp(own_peak[...] - peak) / total
    shift = delta - stats[0][8:16]
    scale_t, delta_t = scale.T, delta.T

    class Small:
        def __init__(self, value):
            w_refs[0][...] = value
            self.level = 0

        def send(self, name):
            at = self.level
            self.copies = [
                send(
                    w_refs[2 * at],
                    w_refs[2 * at + 1].at[d - 1],
                    w_sems[2 * at : 2 * at + 2],
                    d - 1,
                    group_peer(name, d),
                )
                for d in range(1, groups[name][0])
            ]

        def add(self):
            for copy in self.copies:
                copy.wait()
            here, came = w_refs[2 * self.level], w_refs[2 * self.level + 1]
            total = here[...] + functools.reduce(
                jnp.add, [came[d] for d in range(came.shape[0])]
            )
            self.level += 1
            if self.level < 3:
                w_refs[2 * self.level][...] = total
            return total

    half = rows
    scale_h = jnp.concatenate([scale[:, :half], scale[:, half:]], axis=0)
    shift_h = jnp.concatenate([shift[:, :half], shift[:, half:]], axis=0)
    acc = jnp.zeros((16, CZ), F32)
    for i in range(rows):
        acc = acc + scale_h[:, i : i + 1] * (
            ub_ref[i, 0:16] - shift_h[:, i : i + 1] * ub_ref[i, 16:32]
        )
    moment = scale * (own_dist[0:8, :] - shift * own_dist[8:16, :])
    lane8, row8 = iota((8, 128), 1), iota((8, 128), 0)
    even = jnp.sum(jnp.where(lane8 < half, moment, 0.0), axis=1, keepdims=True)
    odd = jnp.sum(jnp.where(lane8 < half, 0.0, moment), axis=1, keepdims=True)
    spread = jnp.where(lane8 == 2 * row8, even, jnp.where(lane8 == 2 * row8 + 1, odd, 0.0))
    head_sum = jnp.sum(spread, axis=0, keepdims=True)
    small = Small(jnp.where(iota((16, 1), 0) == 6, head_sum, LOGIT * acc))
    small.send("z")

    kind = iota((32, 1), 0)
    is_vec = kind < 16

    class Staged:
        def __init__(self, refs, sems, out):
            self.feat, self.kt, self.k1, self.p1, self.k2, self.p2, self.k3 = refs
            self.sems = (sems[0:2], sems[2:4], sems[4:6])
            self.out = out

        def turn(self):
            share = self.kt.shape[2]
            per = 128 // (share * n2)
            for a in range(self.feat.shape[0] // 128):
                for b in range(cols // 128):
                    block = self.feat[128 * a : 128 * a + 128, 128 * b : 128 * b + 128].T
                    self.kt[b * per : (b + 1) * per, :, :, 128 * a : 128 * a + 128] = block.reshape(
                        per, n2, share, 128
                    )

        def send1(self):
            other = lax.rem(i2 + 1, n2)
            self.copies = [send(self.kt.at[:, other], self.k1, self.sems[0], 0, {"row_2": other})]

        def wait(self):
            for copy in self.copies:
                copy.wait()

        def send2(self):
            self.wait()
            self.p1[...] = (self.kt[:, i2] + self.k1[...]).reshape(self.p1.shape)
            self.copies = []
            for d in range(1, n1):
                to = lax.rem(i1 + d, n1)
                self.copies.append(
                    send(self.p1.at[:, to], self.k2.at[d - 1], self.sems[1], d - 1, {"row_1": to})
                )

        def send3(self):
            self.wait()
            self.p2[...] = self.p1[:, i1] + functools.reduce(
                jnp.add, [self.k2[d] for d in range(n1 - 1)]
            )
            self.copies = []
            for d in range(1, n0):
                to = lax.rem(i0 + d, n0)
                self.copies.append(
                    send(self.p2.at[to], self.k3.at[d - 1], self.sems[2], d - 1, {"row_0": to})
                )

        def finish(self):
            self.wait()
            self.out[...] = self.p2[i0] + functools.reduce(
                jnp.add, [self.k3[d] for d in range(n0 - 1)]
            )

    side_d = Staged(kd_refs, kd_sems, kd_out)
    side_v = Staged(kv_refs, kv_sems, kv_out)

    side_d.feat[336:KD, :] = jnp.zeros((KD - 336, cols), F32)
    side_v.feat[480:KV, :] = jnp.zeros((KV - 480, cols), F32)
    for h in range(H):
        own = slice(h * rows, (h + 1) * rows)
        at = (slice(rows * (h % 2), rows * (h % 2) + rows), slice(h // 2, h // 2 + 1))
        attn = e_ref[h] * scale_t[at]
        dlog = attn * (p_ref[h] - delta_t[at])
        p_ref[h] = dlog
        e_ref[h] = attn
        two = 2.0 * coef[:, h : h + 1]
        kd = dot(q_pack[32 * h : 32 * h + 32, :], three_rhs(dlog), 1, 0)
        col_sum = kd[29:30]
        kd = jnp.where(is_vec, kd, two * (kd - k32[32 * h : 32 * h + 32, :] * col_sum))
        side_d.feat[16 * h : 16 * h + 16, :] = kd[0:16]
        for x in range(3):
            to = 192 + 48 * x + 4 * h
            side_d.feat[to : to + 4, :] = kd[16 + 4 * x : 20 + 4 * x]
    side_d.turn()
    side_d.send1()

    for h in range(H):
        own = slice(h * rows, (h + 1) * rows)
        ka = dot(g_pack[48 * h : 48 * h + 48, :], three_rhs(e_ref[h]), 1, 0)
        side_v.feat[16 * h : 16 * h + 16, :] = ka[0:16]
        for x in range(3):
            to = 192 + 96 * x + 8 * h
            side_v.feat[to : to + 8, :] = ka[16 + 8 * x : 24 + 8 * x]
    side_v.turn()
    side_v.send1()

    side_d.send2()

    for h in range(H):
        at = (slice(h // 2, h // 2 + 1), slice(rows * (h % 2), rows * (h % 2) + rows))
        two = 2.0 * coef[:, h : h + 1]
        head = slice(32 * h, 32 * h + 32)
        qd = scale[at] * (qa[head, :] - shift[at] * qb[head, :])
        row_sum = qd[28:29]
        qd = jnp.where(is_vec, LOGIT * INNER * qd, two * (qd - q32[head, :] * row_sum))
        opt = scale[at] * qv[24 * h : 24 * h + 24, :]
        qfeat[16 * h : 16 * h + 16, :] = qd[0:16]
        for x in range(3):
            to = 192 + 48 * x + 4 * h
            qfeat[to : to + 4, :] = qd[16 + 4 * x : 20 + 4 * x]
            to = 336 + 96 * x + 8 * h
            qfeat[to : to + 8, :] = opt[8 * x : 8 * x + 8]
    qfeat[624:QF, :] = jnp.zeros((QF - 624, rows), F32)
    for a in range(QF // 128):
        qt[:, :, 128 * a : 128 * a + 128] = qfeat[128 * a : 128 * a + 128, :].T.reshape(
            qt.shape[0], qt.shape[1], 128
        )
    qx_copies = []
    for d in range(1, m0):
        to = lax.rem(j0 + d, m0)
        qx_copies.append(
            send(qt.at[pl.ds(to * m1, m1)], qx.at[d - 1], qx_sems, d - 1, {"col_0": to})
        )

    side_v.send2()

    for ib in range(rows // 8):
        some = slice(8 * ib, 8 * ib + 8)
        x_ref[some, 0:16, :] = jnp.transpose(p_ref[:, some, :], (1, 0, 2)).astype(BF)
        x_ref[some, 16:32, :] = jnp.transpose(e_ref[:, some, :], (1, 0, 2)).astype(BF)
    for b in range(rows // 4):
        turn_v[b] = x_ref[4 * b : 4 * b + 4].reshape(128, cols).T
    turn_copy = pltpu.make_async_copy(turn_v, turn_hbm, out_sem.at[0])
    turn_copy.start()

    share = kd_out.shape[0]

    def frames(start):
        base = pl.multiple_of((start // 128) * 128, 128)
        sel = iota((share, 128), 1) == iota((share, 128), 0) + (start - base)

        def every_lane(row):
            one = jnp.sum(jnp.where(sel, row, 0.0), axis=1, keepdims=True)
            return jnp.broadcast_to(one, (share, 128))

        rot = [
            [every_lane(rot_ref[x, pl.ds(y, 1), pl.ds(base, 128)]) for y in range(3)]
            for x in range(3)
        ]
        return rot, [every_lane(trans_ref[pl.ds(x, 1), pl.ds(base, 128)]) for x in range(3)]

    rot, anchor = frames(r * rows + c * share)
    key_rot, _ = frames(c * cols + r * share)
    key_base = pl.multiple_of((r * share // 128) * 128, 128)
    key_at = pl.multiple_of(lax.rem(r * share, 128), 8)
    query_at = pl.multiple_of(c * share, 8)

    def hand_over(to, blocks, wide, at):
        for begin, block in blocks:
            wide[begin : begin + block.shape[0], :] = block
        for n in range(1, wide.shape[0] // 128):
            turn_buf[0 : wide.shape[1], :] = wide[128 * n : 128 * n + 128, :].T
            sel_out[to + n - 1] = turn_buf[pl.ds(at, share), :]

    constants = []
    for x in range(3):
        for y in range(3):
            sel_out[ROT_Q + 3 * x + y] = rot[x][y]
            sel_out[ROT_K + 3 * x + y] = key_rot[x][y]
    cotan = [gp_ref[y, pl.ds(query_at, share), :] for y in range(3)]
    sums = [jnp.sum(a, axis=1, keepdims=True) for a in cotan]
    for x in range(3):
        constants += [-anchor[x][:, 0:1] * sums[y] for y in range(3)]
        constants.append(-sum(rot[x][y][:, 0:1] * sums[y] for y in range(3)))
    for n, line in enumerate(frame_lines(constants, share)):
        sel_out[SEL_C + n // share, n % share : n % share + 1, 0:share] = line
    qfeat[...] = jnp.zeros_like(qfeat)
    wide_d[...] = jnp.zeros_like(wide_d)
    wide_v[...] = jnp.zeros_like(wide_v)
    for y in range(3):
        local, cotan_y = qp_ref[y], gp_ref[y].T
        blocks = [(192 + 48 * x, local) for x in range(3)]
        blocks += [(336 + 96 * x, cotan_y) for x in range(3)]
        hand_over(SEL_Q + 4 * y, blocks, qfeat, query_at)
        local = kp_ref[y, :, pl.ds(key_base, 128)]
        hand_over(SEL_D + 2 * y, [(192 + 48 * x, local) for x in range(3)], wide_d, key_at)
        local = vp_ref[y, :, pl.ds(key_base, 128)]
        hand_over(SEL_V + 3 * y, [(192 + 96 * x, local) for x in range(3)], wide_v, key_at)
    sel_copy = pltpu.make_async_copy(sel_out, sel_hbm, out_sem.at[5])
    sel_copy.start()

    small.add()
    small.send("x")
    side_d.send3()
    for copy in qx_copies:
        copy.wait()
    qy[...] = qt[pl.ds(j0 * m1, m1)] + functools.reduce(jnp.add, [qx[d] for d in range(m0 - 1)])
    qz_copies = []
    for d in range(1, m1):
        to = lax.rem(j1 + d, m1)
        qz_copies.append(send(qy.at[to], qz.at[d - 1], qz_sems, d - 1, {"col_1": to}))
    side_v.send3()
    small.add()
    small.send("y")
    side_d.finish()
    side_v.finish()
    for copy in qz_copies:
        copy.wait()
    query_out[...] = functools.reduce(jnp.add, [qz[d] for d in range(m1 - 1)], qy[j1])
    small_out[...] = small.add()
    outs = [
        pltpu.make_async_copy(query_out, query_hbm, out_sem.at[1]),
        pltpu.make_async_copy(kd_out, kd_hbm, out_sem.at[2]),
        pltpu.make_async_copy(kv_out, kv_hbm, out_sem.at[3]),
        pltpu.make_async_copy(small_out, small_hbm, out_sem.at[4]),
    ]
    for copy in outs:
        copy.start()
    for copy in outs + [turn_copy, sel_copy]:
        copy.wait()


def finish_kernel(*refs):
    inputs, refs = refs[:9], refs[9:]
    outs, refs = refs[:11], refs[11:]
    copies_in, refs = refs[:9], refs[9:]
    results, (pg_v, in_sem, pg_sem, out_sem) = refs[:10], refs[10:]
    turn_ref, wt_ref, gpair_ref = copies_in[:3]
    loads = [
        pltpu.make_async_copy(src, dst, in_sem.at[n])
        for n, (src, dst) in enumerate(zip(inputs, copies_in))
    ]
    for load in loads[3:] + loads[:3]:
        load.start()
    for load in loads[3:]:
        load.wait()
    finish_body(*copies_in[3:], *results)
    stores = []
    for n, (src, dst) in enumerate(zip(results, outs[1:])):
        store = pltpu.make_async_copy(src, dst, out_sem.at[n])
        store.start()
        stores.append(store)
    for load in loads[:3]:
        load.wait()

    rows = pg_v.shape[0]
    zero4 = jnp.zeros((4, CZ), F32)
    w16s = jnp.concatenate([LOGIT * wt_ref[...].astype(F32), zero4], axis=0).astype(BF)
    zero32 = jnp.zeros((32, CZ), BF)

    def weights(i):
        gpad = jnp.concatenate([gpair_ref[:, i, :].astype(F32), zero4], axis=0).astype(BF)
        return jnp.concatenate([w16s, gpad], axis=0)

    parts = pg_sem.shape[0]
    step = rows // parts
    for b in range(rows // 4):
        for half in range(2):
            first, second = 4 * b + 2 * half, 4 * b + 2 * half + 1
            left = [zero32] * 4
            right = [zero32] * 4
            left[2 * half], right[2 * half + 1] = weights(first), weights(second)
            block = jnp.concatenate(
                [jnp.concatenate(left, axis=0), jnp.concatenate(right, axis=0)], axis=1
            )
            out = dot(turn_ref[b], block, 1, 0)
            pg_v[first] = out[:, :CZ].astype(BF)
            pg_v[second] = out[:, CZ:].astype(BF)
        if 4 * (b + 1) % step == 0:
            p = 4 * (b + 1) // step - 1
            store = pltpu.make_async_copy(
                pg_v.at[pl.ds(p * step, step)], outs[0].at[pl.ds(p * step, step)], pg_sem.at[p]
            )
            store.start()
            stores.append(store)

    for store in stores:
        store.wait()


def finish_body(
    kd_ref,
    kv_ref,
    query_ref,
    small_ref,
    sel_ref,
    hw_ref,
    qg_out,
    qpg_out,
    qfg_out,
    kg_out,
    vg_out,
    kpg_out,
    vpg_out,
    kfg_out,
    bw_out,
    hw_out,
):
    share = kd_ref.shape[0]

    def lanes(width, x, *segments):
        lane = iota((share, width), 1) + 128
        return functools.reduce(
            jnp.logical_or,
            [(lane >= b + w * x) & (lane < b + w * x + w) for b, w in segments],
        )

    def segment_sum(values, mask):
        kept = jnp.where(mask, values, 0.0)
        parts = [kept[:, 128 * n : 128 * n + 128] for n in range(kept.shape[1] // 128)]
        return functools.reduce(jnp.add, parts)

    def handed(at, count):
        return jnp.concatenate([sel_ref[at + n] for n in range(count)], axis=1)

    def put(out, lines):
        for n, line in enumerate(lines):
            out[n // 4, n % 4 : n % 4 + 1, :] = line

    query, key_d, key_v = query_ref[...], kd_ref[...], kv_ref[...]
    qg_out[...] = query[:, 0:192]
    kg_out[...] = key_d[:, 0:192]
    vg_out[...] = key_v[:, 0:192]
    turned = [
        (qpg_out, ROT_Q, [query[:, 192 + 48 * x : 240 + 48 * x] for x in range(3)]),
        (kpg_out, ROT_K, [key_d[:, 192 + 48 * x : 240 + 48 * x] for x in range(3)]),
        (vpg_out, ROT_K, [key_v[:, 192 + 96 * x : 288 + 96 * x] for x in range(3)]),
    ]

    query, key_d, key_v = query[:, 128:], key_d[:, 128:], key_v[:, 128:]
    frame, key_frame = [], []
    for x in range(3):
        both = lanes(512, x, (192, 48), (336, 96))
        mask_d, mask_v = lanes(256, x, (192, 48)), lanes(384, x, (192, 96))
        for y in range(4):
            if y < 3:
                one = segment_sum(query * handed(SEL_Q + 4 * y, 4), both)
                two = segment_sum(key_d * handed(SEL_D + 2 * y, 2), mask_d)
                three_ = segment_sum(key_v * handed(SEL_V + 3 * y, 3), mask_v)
            else:
                one = segment_sum(query, lanes(512, x, (192, 48)))
                two, three_ = segment_sum(key_d, mask_d), segment_sum(key_v, mask_v)
            frame.append(jnp.sum(one, axis=1, keepdims=True))
            key_frame.append(jnp.sum(two + three_, axis=1, keepdims=True))
    lines = frame_lines(frame, share)
    put(
        qfg_out,
        [
            line + sel_ref[SEL_C + n // share, n % share : n % share + 1, 0:share]
            for n, line in enumerate(lines)
        ],
    )
    put(kfg_out, frame_lines(key_frame, share))
    for out, at, parts in turned:
        width = parts[0].shape[1]
        for y in range(3):
            out[y] = sum(sel_ref[at + 3 * x + y, :, 0:width] * parts[x] for x in range(3))

    for h in range(H):
        bw_out[h : h + 1, :] = small_ref[8 * (h % 2) + h // 2 : 8 * (h % 2) + h // 2 + 1, :]
    raw = hw_ref[...]
    hw_out[...] = small_ref[6:7, 0:H] * (-0.5 * LOGIT * POINT) / (1.0 + jnp.exp(-raw))


def per_device(
    sizes,
    pair_rep,
    bias_weight,
    head_weight,
    queries,
    key_vectors,
    values,
    query_points,
    key_points,
    value_points,
    rotations,
    translations,
    residue_count,
    grad_output,
    grad_points,
    grad_pair,
):
    n0, n1, n2, m0, m1 = sizes
    cols_n = m0 * m1
    rows, cols = pair_rep.shape[:2]
    share, qshare = cols // (n0 * n1 * n2), rows // cols_n
    head_row = head_weight.reshape(1, H)
    grad_points_t = jnp.transpose(grad_points, (0, 2, 1))
    hbm = pl.BlockSpec(memory_space=pl.ANY)
    dma = pltpu.SemaphoreType.DMA
    params = dict(vmem_limit_bytes=VMEM_BYTES)

    def buf(*shape, dtype=F32):
        return pltpu.VMEM(shape, dtype)

    def like(array):
        space = pltpu.VMEM if array.size > 1 else pltpu.SMEM
        return space(array.shape, array.dtype)

    weight_t = bias_weight.T
    grad_pair_t = jnp.transpose(grad_pair, (1, 0, 2))
    operands = (
        weight_t,
        head_row,
        queries.T,
        key_vectors,
        values,
        query_points,
        key_points,
        value_points,
        rotations,
        translations,
        residue_count,
        grad_output.T,
        grad_points_t,
        grad_pair_t,
    )
    sums = (
        jax.ShapeDtypeStruct((rows // 4, cols, 128), BF),
        jax.ShapeDtypeStruct((share, KD), F32),
        jax.ShapeDtypeStruct((share, KV), F32),
        jax.ShapeDtypeStruct((qshare, QF), F32),
        jax.ShapeDtypeStruct((16, CZ), F32),
        jax.ShapeDtypeStruct((SEL_C + 2, share, 128), F32),
    )

    def staged(width):
        return (
            buf(width, cols),
            buf(n0 * n1, n2, share, width),
            buf(n0 * n1, share, width),
            buf(n0, n1, share, width),
            buf(n1 - 1, n0, share, width),
            buf(n0, share, width),
            buf(n0 - 1, share, width),
        )

    def pairs(*counts):
        return tuple(dma((n,)) for n in counts for _ in range(2))

    levels = (m1 * n0, m0 * n2, n1)
    turned, kd_sum, kv_sum, query_sum, small_sum, own_parts = pl.pallas_call(
        functools.partial(tile_kernel, sizes),
        name="tile",
        out_shape=sums,
        in_specs=[hbm] * (1 + len(operands)),
        out_specs=(hbm,) * 6,
        scratch_shapes=[
            *[like(a) for a in operands],
            like(pair_rep),
            *[like(a) for a in sums],
            buf(128, 128),
            buf(KD, 128),
            buf(KV, 128),
            buf(32, rows, cols),
            buf(rows, CZ, cols, dtype=BF),
            buf(rows, 32, CZ),
            buf(rows, 32, cols, dtype=BF),
            buf(16, rows, cols),
            buf(16, rows, cols),
            buf(H, rows, cols),
            buf(H * 32, rows),
            buf(H * 32, cols),
            buf(H * 48, rows),
            buf(H * 48, cols),
            buf(H * rows, 128),
            buf(8, 128),
            buf(16, 128),
            buf(16, 128),
            buf(cols_n - 1, 16, 128),
            buf(H * 32, 3 * rows, dtype=BF),
            buf(H * 48, 3 * rows, dtype=BF),
            buf(H * 32, rows),
            buf(H * 32, rows),
            buf(H * 24, rows),
            buf(QF, rows),
            buf(cols_n, qshare, QF),
            buf(m0 - 1, m1, qshare, QF),
            buf(m1, qshare, QF),
            buf(max(m1 - 1, 1), qshare, QF),
            staged(KD),
            staged(KV),
            tuple(b for n in levels for b in (buf(16, CZ), buf(n - 1, 16, CZ))),
            dma((len(operands),)),
            dma((4,)),
            dma((len(sums),)),
            pairs(cols_n - 1),
            pairs(m0 - 1),
            pairs(max(m1 - 1, 1)),
            pairs(1, n1 - 1, n0 - 1),
            pairs(1, n1 - 1, n0 - 1),
            pairs(*[n - 1 for n in levels]),
        ],
        compiler_params=pltpu.CompilerParams(collective_id=0, has_side_effects=True, **params),
    )(pair_rep, *operands)
    operands = (
        turned,
        weight_t,
        grad_pair_t,
        kd_sum,
        kv_sum,
        query_sum,
        small_sum,
        own_parts,
        head_row,
    )
    results = (
        jax.ShapeDtypeStruct((qshare, 192), F32),
        jax.ShapeDtypeStruct((3, qshare, 48), F32),
        jax.ShapeDtypeStruct((3, 4, qshare), F32),
        jax.ShapeDtypeStruct((share, 192), F32),
        jax.ShapeDtypeStruct((share, 192), F32),
        jax.ShapeDtypeStruct((3, share, 48), F32),
        jax.ShapeDtypeStruct((3, share, 96), F32),
        jax.ShapeDtypeStruct((3, 4, share), F32),
        jax.ShapeDtypeStruct((H, CZ), F32),
        jax.ShapeDtypeStruct((1, H), F32),
    )
    pair_grad, qg, qpg, qfg, kg, vg, kpg, vpg, kfg, bw, hw = pl.pallas_call(
        finish_kernel,
        name="finish",
        out_shape=(jax.ShapeDtypeStruct(pair_rep.shape, BF), *results),
        in_specs=[hbm] * len(operands),
        out_specs=(hbm,) * 11,
        scratch_shapes=[
            *[like(a) for a in operands],
            *[like(a) for a in results],
            like(pair_rep),
            dma((len(operands),)),
            dma((8,)),
            dma((len(results),)),
        ],
        compiler_params=pltpu.CompilerParams(**params),
    )(*operands)

    def swap(a):
        return jnp.transpose(a, (0, 2, 1))

    return (
        pair_grad,
        qg.T,
        swap(qpg),
        qfg,
        kg.T,
        vg.T,
        swap(kpg),
        swap(vpg),
        kfg,
        bw.T,
        hw.reshape(H),
    )


def solution(mesh, sizes=(4, 4, 2, 4, 2)):
    finer = Mesh(mesh.devices.reshape(sizes), ROW_COL)
    in_specs = (
        P(ROW, COL, None),
        P(),
        P(),
        P(None, ROW),
        P(None, COL),
        P(None, COL),
        P(None, None, ROW),
        P(None, None, COL),
        P(None, None, COL),
        P(),
        P(),
        P(),
        P(None, ROW),
        P(None, None, ROW),
        P(ROW, None, None),
    )
    out_specs = (
        P(ROW, COL, None),
        P(None, ROW_COL),
        P(None, None, ROW_COL),
        P(None, None, ROW_COL),
        P(None, COL_ROW),
        P(None, COL_ROW),
        P(None, None, COL_ROW),
        P(None, None, COL_ROW),
        P(None, None, COL_ROW),
        P(),
        P(),
    )
    return jax.shard_map(
        functools.partial(per_device, sizes),
        mesh=finer,
        in_specs=in_specs,
        out_specs=out_specs,
        check_vma=False,
    )
```

```python
import functools
import math

import jax
import jax.numpy as jnp
from jax import lax
from jax.experimental import pallas as pl
from jax.experimental.pallas import tpu as pltpu
from jax.sharding import Mesh
from jax.sharding import PartitionSpec as P

ROW = ("row_0", "row_1", "row_2")
COL = ("col_0", "col_1")
ROW_COL = ROW + COL
COL_ROW = COL + ROW

H, C, PQ, PV, CZ = 12, 16, 4, 8, 128
KD, KV, QF = 384, 512, 640
ROT_Q, ROT_K, SEL_Q, SEL_D, SEL_V, SEL_C = 0, 9, 18, 30, 36, 45


def frame_lines(values, count):
    diagonal = iota((count, 128), 0) == iota((count, 128), 1)
    return [
        jnp.sum(jnp.where(diagonal, v, 0.0), axis=0, keepdims=True)[:, :count] for v in values
    ]
LOGIT = math.sqrt(1.0 / 3.0)
POINT = math.sqrt(2.0 / (9.0 * PQ))
INNER = 1.0 / math.sqrt(C)

F32, BF = jnp.float32, jnp.bfloat16
HIGHEST = lax.Precision.HIGHEST
MESH = pl.DeviceIdType.MESH
VMEM_BYTES = 67043328


def dot(a, b, ca, cb, precision=None):
    return lax.dot_general(
        a, b, (((ca,), (cb,)), ((), ())), precision=precision, preferred_element_type=F32
    )


def split(a):
    hi = a.astype(BF)
    return hi, (a - hi.astype(F32)).astype(BF)


def dot3(a, b, ca, cb):
    (ah, al), (bh, bl) = a, b
    return dot(ah, bh, ca, cb) + dot(ah, bl, ca, cb) + dot(al, bh, ca, cb)


def split3(a):
    first = a.astype(BF)
    rest = a - first.astype(F32)
    second = rest.astype(BF)
    return first, second, (rest - second.astype(F32)).astype(BF)


def dot6(a, b):
    (a1, a2, a3), (b1, b2, b3) = split3(a), split3(b)
    left = jnp.concatenate([a1, a1, a1, a2, a2, a3], axis=0)
    return dot(left, jnp.concatenate([b1, b2, b3, b1, b2, b1], axis=0), 0, 0)


def three(a, axis):
    hi, lo = split(a)
    return jnp.concatenate([hi, hi, lo], axis=axis)


def three_rhs(b):
    hi, lo = split(b)
    return jnp.concatenate([hi, lo, hi], axis=0)


def iota(shape, dim):
    return lax.broadcasted_iota(jnp.int32, shape, dim)


def softplus(x):
    return jnp.maximum(x, 0.0) + jnp.log1p(jnp.exp(-jnp.abs(x)))


def tile_kernel(
    sizes,
    pair_hbm,
    *refs,
):
    inputs, refs = refs[:14], refs[14:]
    sums, refs = refs[:6], refs[6:]
    copies_in, refs = refs[:14], refs[14:]
    tile_body(sizes, pair_hbm, inputs, copies_in, *sums, *copies_in, *refs)


def tile_body(
    sizes,
    pair_hbm,
    inputs,
    copies_in,
    turn_hbm,
    kd_hbm,
    kv_hbm,
    query_hbm,
    small_hbm,
    sel_hbm,
    wt_ref,
    hw_ref,
    q_ref,
    k_ref,
    v_ref,
    qp_ref,
    kp_ref,
    vp_ref,
    rot_ref,
    trans_ref,
    count_ref,
    go_ref,
    gp_ref,
    gpair_ref,
    pair_v,
    turn_v,
    kd_out,
    kv_out,
    query_out,
    small_out,
    sel_out,
    turn_buf,
    wide_d,
    wide_v,
    s_ref,
    pair_t,
    ub_ref,
    x_ref,
    e_ref,
    p_ref,
    d_ref,
    q32,
    k32,
    g48,
    v48,
    vec,
    own_peak,
    own_dist,
    stat_own,
    stat_in,
    q_pack,
    g_pack,
    qa,
    qb,
    qv,
    qfeat,
    qt,
    qx,
    qy,
    qz,
    kd_refs,
    kv_refs,
    w_refs,
    in_sem,
    pair_sem,
    out_sem,
    stat_sems,
    qx_sems,
    qz_sems,
    kd_sems,
    kv_sems,
    w_sems,
):
    n0, n1, n2, m0, m1 = sizes
    cols_n = m0 * m1
    rows = q_ref.shape[0]
    cols = k_ref.shape[1]
    i0, i1, i2 = (lax.axis_index(a) for a in ROW)
    j0, j1 = (lax.axis_index(a) for a in COL)
    r = (i0 * n1 + i1) * n2 + i2
    c = j0 * m1 + j1

    def col_peer(d):
        p = lax.rem(c + d, cols_n)
        return {"col_0": p // m1, "col_1": lax.rem(p, m1)}

    groups = {
        "x": (m0 * n2, j0 * n2 + i2, lambda p: {"col_0": p // n2, "row_2": lax.rem(p, n2)}),
        "z": (m1 * n0, j1 * n0 + i0, lambda p: {"col_1": p // n0, "row_0": lax.rem(p, n0)}),
        "y": (n1, i1, lambda p: {"row_1": p}),
    }

    def group_peer(name, d):
        count, here, place = groups[name]
        return place(lax.rem(here + d, count))

    def send(src, dst, sems, n, device):
        copy = pltpu.make_async_remote_copy(
            src_ref=src,
            dst_ref=dst,
            send_sem=sems[0].at[n],
            recv_sem=sems[1].at[n],
            device_id=device,
            device_id_type=MESH,
        )
        copy.start()
        return copy

    parts = pair_sem.shape[0]
    step = rows // parts
    loads = [
        pltpu.make_async_copy(
            pair_hbm.at[pl.ds(b * step, step)], pair_v.at[pl.ds(b * step, step)], pair_sem.at[b]
        )
        for b in range(parts)
    ]
    smalls = [
        pltpu.make_async_copy(src, dst, in_sem.at[n])
        for n, (src, dst) in enumerate(zip(inputs, copies_in))
    ]
    for load in smalls:
        load.start()

    barrier = pltpu.get_barrier_semaphore()
    expected = 0
    for d in range(1, cols_n):
        pl.semaphore_signal(barrier, inc=1, device_id=col_peer(d), device_id_type=MESH)
        expected += 1
    for name in groups:
        for d in range(1, groups[name][0]):
            pl.semaphore_signal(
                barrier, inc=1, device_id=group_peer(name, d), device_id_type=MESH
            )
            expected += 1

    for load in loads:
        load.start()
    for load in smalls:
        load.wait()

    col_start = pl.multiple_of(c * cols, 128)
    row_start = r * rows
    row_base = pl.multiple_of((row_start // 128) * 128, 128)
    row_half = lax.rem(row_start, 128)

    def row_window(w):
        return jnp.where(row_half == 0, w[:, :rows], w[:, 128 - rows :])

    def row_rot(x, y):
        return row_window(rot_ref[x, pl.ds(y, 1), pl.ds(row_base, 128)])

    def col_rot(x, y):
        return rot_ref[x, pl.ds(y, 1), pl.ds(col_start, cols)]

    coef = 0.5 * LOGIT * POINT * softplus(hw_ref[...])

    zero_q = jnp.zeros((2, rows), F32)
    zero_k = jnp.zeros((2, cols), F32)
    q_t = q_ref[...].T * (LOGIT * INNER)
    k_all = k_ref[...]
    rr = [[row_rot(x, y) for y in range(3)] for x in range(3)]
    cr = [[col_rot(x, y) for y in range(3)] for x in range(3)]
    for x in range(3):
        t_row = row_window(trans_ref[pl.ds(x, 1), pl.ds(row_base, 128)])
        t_col = trans_ref[pl.ds(x, 1), pl.ds(col_start, cols)]
        qg = sum(rr[x][y] * qp_ref[y] for y in range(3)) + t_row
        kg = sum(cr[x][y] * kp_ref[y] for y in range(3)) + t_col
        vg = sum(cr[x][y] * vp_ref[y] for y in range(3)) + t_col
        for h in range(H):
            q32[32 * h + 16 + 4 * x : 32 * h + 20 + 4 * x, :] = qg[4 * h : 4 * h + 4]
            k32[32 * h + 16 + 4 * x : 32 * h + 20 + 4 * x, :] = kg[4 * h : 4 * h + 4]
            v48[48 * h + 16 + 8 * x : 48 * h + 24 + 8 * x, :] = vg[8 * h : 8 * h + 8]
    gp_t = [gp_ref[y].T for y in range(3)]
    for x in range(3):
        gg = sum(rr[x][y] * gp_t[y] for y in range(3))
        for h in range(H):
            g48[48 * h + 16 + 8 * x : 48 * h + 24 + 8 * x, :] = gg[8 * h : 8 * h + 8]
    go_t = go_ref[...].T
    for h in range(H):
        q32[32 * h : 32 * h + 16, :] = q_t[16 * h : 16 * h + 16]
        k32[32 * h : 32 * h + 16, :] = k_all[16 * h : 16 * h + 16]
        g48[48 * h : 48 * h + 16, :] = go_t[16 * h : 16 * h + 16]
        v48[48 * h : 48 * h + 16, :] = v_ref[16 * h : 16 * h + 16, :]
        g48[48 * h + 40 : 48 * h + 48, :] = jnp.zeros((8, rows), F32)
        v48[48 * h + 40 : 48 * h + 48, :] = jnp.zeros((8, cols), F32)
        qh = q32[32 * h + 16 : 32 * h + 28, :]
        kh = k32[32 * h + 16 : 32 * h + 28, :]
        q32[32 * h + 28 : 32 * h + 32, :] = jnp.concatenate(
            [jnp.sum(qh * qh, axis=0, keepdims=True), jnp.ones((1, rows), F32), zero_q], axis=0
        )
        k32[32 * h + 28 : 32 * h + 32, :] = jnp.concatenate(
            [jnp.ones((1, cols), F32), jnp.sum(kh * kh, axis=0, keepdims=True), zero_k], axis=0
        )

    w16 = jnp.concatenate([wt_ref[...].astype(F32), jnp.zeros((4, CZ), F32)], axis=0)
    w16b = w16.astype(BF)

    def stack(i):
        gpad = jnp.concatenate(
            [gpair_ref[:, i, :].astype(F32), jnp.zeros((4, CZ), F32)], axis=0
        ).astype(BF)
        return gpad

    e_ref[H:16] = jnp.zeros((16 - H, rows, cols), F32)
    p_ref[H:16] = jnp.zeros((16 - H, rows, cols), F32)
    point_row = iota((16, 1), 0) < 12
    for h in range(H):
        kb = k32[32 * h + 16 : 32 * h + 32, :]
        inner = dot6(q32[32 * h : 32 * h + 16, :], k32[32 * h : 32 * h + 16, :])
        dist = dot6(q32[32 * h + 16 : 32 * h + 32, :], jnp.where(point_row, -2.0 * kb, kb))
        d_ref[h] = dist
        e_ref[h] = inner - coef[:, h : h + 1] * dist
        p_ref[h] = dot(
            three(g48[48 * h : 48 * h + 48, :], 0), three_rhs(v48[48 * h : 48 * h + 48, :]), 0, 0
        )

    for b in range(parts):
        loads[b].wait()
        for ib in range(b * step // 8, (b + 1) * step // 8):
            proj = []
            for i in range(8 * ib, 8 * ib + 8):
                both = jnp.concatenate([w16b, stack(i)], axis=0)
                if i % 4 == 3:
                    proj.append(dot(both, pair_v[i], 1, 1))
                else:
                    pair_t[i] = pair_v[i].T
                    proj.append(dot(both, pair_t[i], 1, 0))
            s_ref[:, 8 * ib : 8 * ib + 8, :] = jnp.transpose(jnp.stack(proj), (1, 0, 2))

    valid = col_start + iota((1, cols), 1) < count_ref[0]
    lane = iota((rows, 128), 1)
    for h in range(H):
        prod = p_ref[h] + s_ref[16 + h]
        logits = e_ref[h] + LOGIT * s_ref[h]
        logits = jnp.where(valid, logits, -1000000000.0)
        peak = jnp.max(logits, axis=1, keepdims=True)
        e = jnp.exp(logits - peak)
        total = jnp.sum(e, axis=1, keepdims=True)
        upper = jnp.sum(e * prod, axis=1, keepdims=True)
        e_ref[h] = e
        p_ref[h] = prod
        vec[h * rows : (h + 1) * rows, :] = jnp.where(
            lane == 0, peak + jnp.log(total), jnp.where(lane == 1, upper / total, peak)
        )
    blocks = H * rows // 128
    own_peak[...] = jnp.zeros_like(own_peak)
    own_dist[...] = jnp.zeros_like(own_dist)
    for b in range(blocks):
        turned = vec[128 * b : 128 * b + 128, :].T
        stat_own[b : b + 1, :] = turned[0:1]
        stat_own[blocks + b : blocks + b + 1, :] = turned[1:2]
        own_peak[b : b + 1, :] = turned[2:3]

    pl.semaphore_wait(barrier, expected)

    stat_copies = [
        send(stat_own, stat_in.at[d - 1], stat_sems, d - 1, col_peer(d))
        for d in sorted(range(1, cols_n), key=lambda d: d % m1 == 0)
    ]

    for a in (6, 14, 22, 30):
        s_ref[a : a + 2] = jnp.zeros((2, rows, cols), F32)
    for h in range(H):
        own = slice(h * rows, (h + 1) * rows)
        e = e_ref[h]
        es = split(e)
        ep = e * (p_ref[h] - vec[own, 1:2])
        ks = split(k32[32 * h : 32 * h + 32, :])
        qa[32 * h : 32 * h + 32, :] = dot3(ks, split(ep), 1, 1)
        qb[32 * h : 32 * h + 32, :] = dot3(ks, es, 1, 1)
        qv[24 * h : 24 * h + 24, :] = dot3(split(v48[48 * h : 48 * h + 48, :]), es, 1, 1)[16:40]
        s_ref[8 * (h % 2) + h // 2] = ep
        s_ref[16 + 8 * (h % 2) + h // 2] = e
        dist = d_ref[h]
        vec[own, :] = jnp.where(
            lane == 0,
            jnp.sum(ep * dist, axis=1, keepdims=True),
            jnp.sum(e * dist, axis=1, keepdims=True),
        )
    for b in range(blocks):
        turned = vec[128 * b : 128 * b + 128, :].T
        own_dist[b : b + 1, :] = turned[0:1]
        own_dist[8 + b : 9 + b, :] = turned[1:2]
    for ib in range(rows // 8):
        by_query = jnp.transpose(s_ref[:, 8 * ib : 8 * ib + 8, :], (1, 0, 2))
        for ii in range(8):
            both = dot(jnp.concatenate(split(by_query[ii]), axis=0), pair_v[8 * ib + ii], 1, 0)
            ub_ref[8 * ib + ii] = both[0:32] + both[32:64]
    for h in range(H):
        q_pack[32 * h : 32 * h + 32, :] = three(q32[32 * h : 32 * h + 32, :], 1)
        g_pack[48 * h : 48 * h + 48, :] = three(g48[48 * h : 48 * h + 48, :], 1)

    for copy in stat_copies:
        copy.wait()

    def padded(ref, part):
        rows_here = ref[part * blocks : part * blocks + blocks, :]
        return jnp.concatenate([rows_here, jnp.zeros((8 - blocks, 128), F32)], axis=0)

    stats = [
        (padded(ref, 0), padded(ref, 1))
        for ref in [stat_own] + [stat_in.at[d] for d in range(cols_n - 1)]
    ]
    peak = functools.reduce(jnp.maximum, [s[0] for s in stats])
    weights = [jnp.exp(s[0] - peak) for s in stats]
    total = functools.reduce(jnp.add, weights)
    delta = functools.reduce(jnp.add, [w * s[1] for w, s in zip(weights, stats)]) / total
    scale = jnp.exp(own_peak[...] - peak) / total
    shift = delta - stats[0][1]
    scale_t, delta_t = scale.T, delta.T

    class Small:
        def __init__(self, value):
            w_refs[0][...] = value
            self.level = 0

        def send(self, name):
            at = self.level
            self.copies = [
                send(
                    w_refs[2 * at],
                    w_refs[2 * at + 1].at[d - 1],
                    w_sems[2 * at : 2 * at + 2],
                    d - 1,
                    group_peer(name, d),
                )
                for d in range(1, groups[name][0])
            ]

        def add(self):
            for copy in self.copies:
                copy.wait()
            here, came = w_refs[2 * self.level], w_refs[2 * self.level + 1]
            total = here[...] + functools.reduce(
                jnp.add, [came[d] for d in range(came.shape[0])]
            )
            self.level += 1
            if self.level < 3:
                w_refs[2 * self.level][...] = total
            return total

    half = rows
    scale_h = jnp.concatenate([scale[:, :half], scale[:, half:]], axis=0)
    shift_h = jnp.concatenate([shift[:, :half], shift[:, half:]], axis=0)
    acc = jnp.zeros((16, CZ), F32)
    for i in range(rows):
        acc = acc + scale_h[:, i : i + 1] * (
            ub_ref[i, 0:16] - shift_h[:, i : i + 1] * ub_ref[i, 16:32]
        )
    moment = scale * (own_dist[0:8, :] - shift * own_dist[8:16, :])
    lane8, row8 = iota((8, 128), 1), iota((8, 128), 0)
    even = jnp.sum(jnp.where(lane8 < half, moment, 0.0), axis=1, keepdims=True)
    odd = jnp.sum(jnp.where(lane8 < half, 0.0, moment), axis=1, keepdims=True)
    spread = jnp.where(lane8 == 2 * row8, even, jnp.where(lane8 == 2 * row8 + 1, odd, 0.0))
    head_sum = jnp.sum(spread, axis=0, keepdims=True)
    small = Small(jnp.where(iota((16, 1), 0) == 6, head_sum, LOGIT * acc))
    small.send("x")

    kind = iota((32, 1), 0)
    is_vec = kind < 16

    class Staged:
        def __init__(self, refs, sems, out):
            self.feat, self.kt, self.k1, self.p1, self.k2, self.p2, self.k3 = refs
            self.sems = (sems[0:2], sems[2:4], sems[4:6])
            self.out = out

        def turn(self):
            share = self.kt.shape[2]
            per = 128 // (share * n2)
            for a in range(self.feat.shape[0] // 128):
                for b in range(cols // 128):
                    block = self.feat[128 * a : 128 * a + 128, 128 * b : 128 * b + 128].T
                    block = block.reshape(per, n2, share, 128)
                    for n in range(n2):
                        self.kt[n, b * per : (b + 1) * per, :, 128 * a : 128 * a + 128] = block[:, n]

        def send1(self):
            other = lax.rem(i2 + 1, n2)
            self.copies = [send(self.kt.at[other], self.k1, self.sems[0], 0, {"row_2": other})]

        def wait(self):
            for copy in self.copies:
                copy.wait()

        def send2(self):
            self.wait()
            for y in range(n1):
                for z in range(n0):
                    self.p1[y, z] = self.kt[i2, z * n1 + y] + self.k1[z * n1 + y]
            self.copies = []
            for d in range(1, n1):
                to = lax.rem(i1 + d, n1)
                self.copies.append(
                    send(self.p1.at[to], self.k2.at[d - 1], self.sems[1], d - 1, {"row_1": to})
                )

        def send3(self):
            self.wait()
            self.p2[...] = self.p1[i1] + functools.reduce(
                jnp.add, [self.k2[d] for d in range(n1 - 1)]
            )
            self.copies = []
            for d in range(1, n0):
                to = lax.rem(i0 + d, n0)
                self.copies.append(
                    send(self.p2.at[to], self.k3.at[d - 1], self.sems[2], d - 1, {"row_0": to})
                )

        def finish(self):
            self.wait()
            self.out[...] = self.p2[i0] + functools.reduce(
                jnp.add, [self.k3[d] for d in range(n0 - 1)]
            )

    side_d = Staged(kd_refs, kd_sems, kd_out)
    side_v = Staged(kv_refs, kv_sems, kv_out)

    side_d.feat[336:KD, :] = jnp.zeros((KD - 336, cols), F32)
    side_v.feat[480:KV, :] = jnp.zeros((KV - 480, cols), F32)
    for h in range(H):
        own = slice(h * rows, (h + 1) * rows)
        at = (slice(rows * (h % 2), rows * (h % 2) + rows), slice(h // 2, h // 2 + 1))
        attn = e_ref[h] * scale_t[at]
        dlog = attn * (p_ref[h] - delta_t[at])
        p_ref[h] = dlog
        e_ref[h] = attn
        two = 2.0 * coef[:, h : h + 1]
        kd = dot(q_pack[32 * h : 32 * h + 32, :], three_rhs(dlog), 1, 0)
        col_sum = kd[29:30]
        kd = jnp.where(is_vec, kd, two * (kd - k32[32 * h : 32 * h + 32, :] * col_sum))
        side_d.feat[16 * h : 16 * h + 16, :] = kd[0:16]
        for x in range(3):
            to = 192 + 48 * x + 4 * h
            side_d.feat[to : to + 4, :] = kd[16 + 4 * x : 20 + 4 * x]
    side_d.turn()
    side_d.send1()

    for h in range(H):
        own = slice(h * rows, (h + 1) * rows)
        ka = dot(g_pack[48 * h : 48 * h + 48, :], three_rhs(e_ref[h]), 1, 0)
        side_v.feat[16 * h : 16 * h + 16, :] = ka[0:16]
        for x in range(3):
            to = 192 + 96 * x + 8 * h
            side_v.feat[to : to + 8, :] = ka[16 + 8 * x : 24 + 8 * x]
    side_v.turn()
    side_v.send1()

    for h in range(H):
        at = (slice(h // 2, h // 2 + 1), slice(rows * (h % 2), rows * (h % 2) + rows))
        two = 2.0 * coef[:, h : h + 1]
        head = slice(32 * h, 32 * h + 32)
        qd = scale[at] * (qa[head, :] - shift[at] * qb[head, :])
        row_sum = qd[28:29]
        qd = jnp.where(is_vec, LOGIT * INNER * qd, two * (qd - q32[head, :] * row_sum))
        opt = scale[at] * qv[24 * h : 24 * h + 24, :]
        qfeat[16 * h : 16 * h + 16, :] = qd[0:16]
        for x in range(3):
            to = 192 + 48 * x + 4 * h
            qfeat[to : to + 4, :] = qd[16 + 4 * x : 20 + 4 * x]
            to = 336 + 96 * x + 8 * h
            qfeat[to : to + 8, :] = opt[8 * x : 8 * x + 8]
    qfeat[624:QF, :] = jnp.zeros((QF - 624, rows), F32)
    for a in range(QF // 128):
        qt[:, :, 128 * a : 128 * a + 128] = qfeat[128 * a : 128 * a + 128, :].T.reshape(
            qt.shape[0], qt.shape[1], 128
        )
    qx_copies = []
    for d in range(1, m0):
        to = lax.rem(j0 + d, m0)
        qx_copies.append(
            send(qt.at[pl.ds(to * m1, m1)], qx.at[d - 1], qx_sems, d - 1, {"col_0": to})
        )

    side_d.send2()

    side_v.send2()
    small.add()
    small.send("z")

    for ib in range(rows // 8):
        some = slice(8 * ib, 8 * ib + 8)
        x_ref[some, 0:16, :] = jnp.transpose(p_ref[:, some, :], (1, 0, 2)).astype(BF)
        x_ref[some, 16:32, :] = jnp.transpose(e_ref[:, some, :], (1, 0, 2)).astype(BF)
    for b in range(rows // 4):
        turn_v[b] = x_ref[4 * b : 4 * b + 4].reshape(128, cols).T
    turn_copy = pltpu.make_async_copy(turn_v, turn_hbm, out_sem.at[0])
    turn_copy.start()

    share = kd_out.shape[0]

    def frames(start):
        base = pl.multiple_of((start // 128) * 128, 128)
        sel = iota((share, 128), 1) == iota((share, 128), 0) + (start - base)

        def every_lane(row):
            one = jnp.sum(jnp.where(sel, row, 0.0), axis=1, keepdims=True)
            return jnp.broadcast_to(one, (share, 128))

        rot = [
            [every_lane(rot_ref[x, pl.ds(y, 1), pl.ds(base, 128)]) for y in range(3)]
            for x in range(3)
        ]
        return rot, [every_lane(trans_ref[pl.ds(x, 1), pl.ds(base, 128)]) for x in range(3)]

    rot, anchor = frames(r * rows + c * share)
    key_rot, _ = frames(c * cols + r * share)
    key_base = pl.multiple_of((r * share // 128) * 128, 128)
    key_at = pl.multiple_of(lax.rem(r * share, 128), 8)
    query_at = pl.multiple_of(c * share, 8)

    def hand_over(to, blocks, wide, at):
        for begin, block in blocks:
            wide[begin : begin + block.shape[0], :] = block
        for n in range(1, wide.shape[0] // 128):
            turn_buf[0 : wide.shape[1], :] = wide[128 * n : 128 * n + 128, :].T
            sel_out[to + n - 1] = turn_buf[pl.ds(at, share), :]

    constants = []
    for x in range(3):
        for y in range(3):
            sel_out[ROT_Q + 3 * x + y] = rot[x][y]
            sel_out[ROT_K + 3 * x + y] = key_rot[x][y]
    cotan = [gp_ref[y, pl.ds(query_at, share), :] for y in range(3)]
    sums = [jnp.sum(a, axis=1, keepdims=True) for a in cotan]
    for x in range(3):
        constants += [-anchor[x][:, 0:1] * sums[y] for y in range(3)]
        constants.append(-sum(rot[x][y][:, 0:1] * sums[y] for y in range(3)))
    for n, line in enumerate(frame_lines(constants, share)):
        sel_out[SEL_C + n // share, n % share : n % share + 1, 0:share] = line
    qfeat[...] = jnp.zeros_like(qfeat)
    wide_d[...] = jnp.zeros_like(wide_d)
    wide_v[...] = jnp.zeros_like(wide_v)
    for y in range(3):
        local, cotan_y = qp_ref[y], gp_ref[y].T
        blocks = [(192 + 48 * x, local) for x in range(3)]
        blocks += [(336 + 96 * x, cotan_y) for x in range(3)]
        hand_over(SEL_Q + 4 * y, blocks, qfeat, query_at)
        local = kp_ref[y, :, pl.ds(key_base, 128)]
        hand_over(SEL_D + 2 * y, [(192 + 48 * x, local) for x in range(3)], wide_d, key_at)
        local = vp_ref[y, :, pl.ds(key_base, 128)]
        hand_over(SEL_V + 3 * y, [(192 + 96 * x, local) for x in range(3)], wide_v, key_at)
    sel_copy = pltpu.make_async_copy(sel_out, sel_hbm, out_sem.at[5])
    sel_copy.start()

    for copy in qx_copies:
        copy.wait()
    qy[...] = qt[pl.ds(j0 * m1, m1)] + functools.reduce(jnp.add, [qx[d] for d in range(m0 - 1)])
    qz_copies = []
    for d in range(1, m1):
        to = lax.rem(j1 + d, m1)
        qz_copies.append(send(qy.at[to], qz.at[d - 1], qz_sems, d - 1, {"col_1": to}))
    side_d.send3()
    side_v.send3()
    small.add()
    small.send("y")
    side_d.finish()
    side_v.finish()
    for copy in qz_copies:
        copy.wait()
    query_out[...] = functools.reduce(jnp.add, [qz[d] for d in range(m1 - 1)], qy[j1])
    small_out[...] = small.add()
    outs = [
        pltpu.make_async_copy(query_out, query_hbm, out_sem.at[1]),
        pltpu.make_async_copy(kd_out, kd_hbm, out_sem.at[2]),
        pltpu.make_async_copy(kv_out, kv_hbm, out_sem.at[3]),
        pltpu.make_async_copy(small_out, small_hbm, out_sem.at[4]),
    ]
    for copy in outs:
        copy.start()
    for copy in outs + [turn_copy, sel_copy]:
        copy.wait()


def finish_kernel(*refs):
    inputs, refs = refs[:9], refs[9:]
    outs, refs = refs[:11], refs[11:]
    copies_in, refs = refs[:9], refs[9:]
    results, (pg_v, in_sem, pg_sem, out_sem) = refs[:10], refs[10:]
    turn_ref, wt_ref, gpair_ref = copies_in[:3]
    loads = [
        pltpu.make_async_copy(src, dst, in_sem.at[n])
        for n, (src, dst) in enumerate(zip(inputs, copies_in))
    ]
    for load in loads:
        load.start()
    for load in loads[:3]:
        load.wait()
    stores = []

    rows = pg_v.shape[0]
    zero4 = jnp.zeros((4, CZ), F32)
    w16s = jnp.concatenate([LOGIT * wt_ref[...].astype(F32), zero4], axis=0).astype(BF)
    zero32 = jnp.zeros((32, CZ), BF)

    def weights(i):
        gpad = jnp.concatenate([gpair_ref[:, i, :].astype(F32), zero4], axis=0).astype(BF)
        return jnp.concatenate([w16s, gpad], axis=0)

    parts = pg_sem.shape[0]
    step = rows // parts
    for b in range(rows // 4):
        for half in range(2):
            first, second = 4 * b + 2 * half, 4 * b + 2 * half + 1
            left = [zero32] * 4
            right = [zero32] * 4
            left[2 * half], right[2 * half + 1] = weights(first), weights(second)
            block = jnp.concatenate(
                [jnp.concatenate(left, axis=0), jnp.concatenate(right, axis=0)], axis=1
            )
            out = dot(turn_ref[b], block, 1, 0)
            pg_v[first] = out[:, :CZ].astype(BF)
            pg_v[second] = out[:, CZ:].astype(BF)
        if 4 * (b + 1) % step == 0:
            p = 4 * (b + 1) // step - 1
            store = pltpu.make_async_copy(
                pg_v.at[pl.ds(p * step, step)], outs[0].at[pl.ds(p * step, step)], pg_sem.at[p]
            )
            store.start()
            stores.append(store)

    for load in loads[3:]:
        load.wait()
    finish_body(*copies_in[3:], *results)
    for n, (src, dst) in enumerate(zip(results, outs[1:])):
        store = pltpu.make_async_copy(src, dst, out_sem.at[n])
        store.start()
        stores.append(store)
    for store in stores:
        store.wait()


def finish_body(
    kd_ref,
    kv_ref,
    query_ref,
    small_ref,
    sel_ref,
    hw_ref,
    qg_out,
    qpg_out,
    qfg_out,
    kg_out,
    vg_out,
    kpg_out,
    vpg_out,
    kfg_out,
    bw_out,
    hw_out,
):
    share = kd_ref.shape[0]

    def lanes(width, x, *segments):
        lane = iota((share, width), 1) + 128
        return functools.reduce(
            jnp.logical_or,
            [(lane >= b + w * x) & (lane < b + w * x + w) for b, w in segments],
        )

    def segment_sum(values, mask):
        kept = jnp.where(mask, values, 0.0)
        parts = [kept[:, 128 * n : 128 * n + 128] for n in range(kept.shape[1] // 128)]
        return functools.reduce(jnp.add, parts)

    def handed(at, count):
        return jnp.concatenate([sel_ref[at + n] for n in range(count)], axis=1)

    def put(out, lines):
        for n, line in enumerate(lines):
            out[n // 4, n % 4 : n % 4 + 1, :] = line

    query, key_d, key_v = query_ref[...], kd_ref[...], kv_ref[...]
    qg_out[...] = query[:, 0:192]
    kg_out[...] = key_d[:, 0:192]
    vg_out[...] = key_v[:, 0:192]
    turned = [
        (qpg_out, ROT_Q, [query[:, 192 + 48 * x : 240 + 48 * x] for x in range(3)]),
        (kpg_out, ROT_K, [key_d[:, 192 + 48 * x : 240 + 48 * x] for x in range(3)]),
        (vpg_out, ROT_K, [key_v[:, 192 + 96 * x : 288 + 96 * x] for x in range(3)]),
    ]

    query, key_d, key_v = query[:, 128:], key_d[:, 128:], key_v[:, 128:]
    frame, key_frame = [], []
    for x in range(3):
        both = lanes(512, x, (192, 48), (336, 96))
        mask_d, mask_v = lanes(256, x, (192, 48)), lanes(384, x, (192, 96))
        for y in range(4):
            if y < 3:
                one = segment_sum(query * handed(SEL_Q + 4 * y, 4), both)
                two = segment_sum(key_d * handed(SEL_D + 2 * y, 2), mask_d)
                three_ = segment_sum(key_v * handed(SEL_V + 3 * y, 3), mask_v)
            else:
                one = segment_sum(query, lanes(512, x, (192, 48)))
                two, three_ = segment_sum(key_d, mask_d), segment_sum(key_v, mask_v)
            frame.append(jnp.sum(one, axis=1, keepdims=True))
            key_frame.append(jnp.sum(two + three_, axis=1, keepdims=True))
    lines = frame_lines(frame, share)
    put(
        qfg_out,
        [
            line + sel_ref[SEL_C + n // share, n % share : n % share + 1, 0:share]
            for n, line in enumerate(lines)
        ],
    )
    put(kfg_out, frame_lines(key_frame, share))
    for out, at, parts in turned:
        width = parts[0].shape[1]
        for y in range(3):
            out[y] = sum(sel_ref[at + 3 * x + y, :, 0:width] * parts[x] for x in range(3))

    for h in range(H):
        bw_out[h : h + 1, :] = small_ref[8 * (h % 2) + h // 2 : 8 * (h % 2) + h // 2 + 1, :]
    raw = hw_ref[...]
    hw_out[...] = small_ref[6:7, 0:H] * (-0.5 * LOGIT * POINT) / (1.0 + jnp.exp(-raw))


def per_device(
    sizes,
    pair_rep,
    bias_weight,
    head_weight,
    queries,
    key_vectors,
    values,
    query_points,
    key_points,
    value_points,
    rotations,
    translations,
    residue_count,
    grad_output,
    grad_points,
    grad_pair,
):
    n0, n1, n2, m0, m1 = sizes
    cols_n = m0 * m1
    rows, cols = pair_rep.shape[:2]
    share, qshare = cols // (n0 * n1 * n2), rows // cols_n
    head_row = head_weight.reshape(1, H)
    grad_points_t = jnp.transpose(grad_points, (0, 2, 1))
    hbm = pl.BlockSpec(memory_space=pl.ANY)
    dma = pltpu.SemaphoreType.DMA
    params = dict(vmem_limit_bytes=VMEM_BYTES)

    def buf(*shape, dtype=F32):
        return pltpu.VMEM(shape, dtype)

    def like(array):
        space = pltpu.VMEM if array.size > 1 else pltpu.SMEM
        return space(array.shape, array.dtype)

    weight_t = bias_weight.T
    grad_pair_t = jnp.transpose(grad_pair, (1, 0, 2))
    operands = (
        weight_t,
        head_row,
        queries.T,
        key_vectors,
        values,
        query_points,
        key_points,
        value_points,
        rotations,
        translations,
        residue_count,
        grad_output.T,
        grad_points_t,
        grad_pair_t,
    )
    sums = (
        jax.ShapeDtypeStruct((rows // 4, cols, 128), BF),
        jax.ShapeDtypeStruct((share, KD), F32),
        jax.ShapeDtypeStruct((share, KV), F32),
        jax.ShapeDtypeStruct((qshare, QF), F32),
        jax.ShapeDtypeStruct((16, CZ), F32),
        jax.ShapeDtypeStruct((SEL_C + 2, share, 128), F32),
    )

    def staged(width):
        return (
            buf(width, cols),
            buf(n2, n0 * n1, share, width),
            buf(n0 * n1, share, width),
            buf(n1, n0, share, width),
            buf(n1 - 1, n0, share, width),
            buf(n0, share, width),
            buf(n0 - 1, share, width),
        )

    def pairs(*counts):
        return tuple(dma((n,)) for n in counts for _ in range(2))

    levels = (m0 * n2, m1 * n0, n1)
    turned, kd_sum, kv_sum, query_sum, small_sum, own_parts = pl.pallas_call(
        functools.partial(tile_kernel, sizes),
        name="tile",
        out_shape=sums,
        in_specs=[hbm] * (1 + len(operands)),
        out_specs=(hbm,) * 6,
        scratch_shapes=[
            *[like(a) for a in operands],
            like(pair_rep),
            *[like(a) for a in sums],
            buf(128, 128),
            buf(KD, 128),
            buf(KV, 128),
            buf(32, rows, cols),
            buf(rows, CZ, cols, dtype=BF),
            buf(rows, 32, CZ),
            buf(rows, 32, cols, dtype=BF),
            buf(16, rows, cols),
            buf(16, rows, cols),
            buf(H, rows, cols),
            buf(H * 32, rows),
            buf(H * 32, cols),
            buf(H * 48, rows),
            buf(H * 48, cols),
            buf(H * rows, 128),
            buf(8, 128),
            buf(16, 128),
            buf(2 * H * rows // 128, 128),
            buf(cols_n - 1, 2 * H * rows // 128, 128),
            buf(H * 32, 3 * rows, dtype=BF),
            buf(H * 48, 3 * rows, dtype=BF),
            buf(H * 32, rows),
            buf(H * 32, rows),
            buf(H * 24, rows),
            buf(QF, rows),
            buf(cols_n, qshare, QF),
            buf(m0 - 1, m1, qshare, QF),
            buf(m1, qshare, QF),
            buf(max(m1 - 1, 1), qshare, QF),
            staged(KD),
            staged(KV),
            tuple(b for n in levels for b in (buf(16, CZ), buf(n - 1, 16, CZ))),
            dma((len(operands),)),
            dma((2,)),
            dma((len(sums),)),
            pairs(cols_n - 1),
            pairs(m0 - 1),
            pairs(max(m1 - 1, 1)),
            pairs(1, n1 - 1, n0 - 1),
            pairs(1, n1 - 1, n0 - 1),
            pairs(*[n - 1 for n in levels]),
        ],
        compiler_params=pltpu.CompilerParams(collective_id=0, has_side_effects=True, **params),
    )(pair_rep, *operands)
    operands = (
        turned,
        weight_t,
        grad_pair_t,
        kd_sum,
        kv_sum,
        query_sum,
        small_sum,
        own_parts,
        head_row,
    )
    results = (
        jax.ShapeDtypeStruct((qshare, 192), F32),
        jax.ShapeDtypeStruct((3, qshare, 48), F32),
        jax.ShapeDtypeStruct((3, 4, qshare), F32),
        jax.ShapeDtypeStruct((share, 192), F32),
        jax.ShapeDtypeStruct((share, 192), F32),
        jax.ShapeDtypeStruct((3, share, 48), F32),
        jax.ShapeDtypeStruct((3, share, 96), F32),
        jax.ShapeDtypeStruct((3, 4, share), F32),
        jax.ShapeDtypeStruct((H, CZ), F32),
        jax.ShapeDtypeStruct((1, H), F32),
    )
    pair_grad, qg, qpg, qfg, kg, vg, kpg, vpg, kfg, bw, hw = pl.pallas_call(
        finish_kernel,
        name="finish",
        out_shape=(jax.ShapeDtypeStruct(pair_rep.shape, BF), *results),
        in_specs=[hbm] * len(operands),
        out_specs=(hbm,) * 11,
        scratch_shapes=[
            *[like(a) for a in operands],
            *[like(a) for a in results],
            like(pair_rep),
            dma((len(operands),)),
            dma((8,)),
            dma((len(results),)),
        ],
        compiler_params=pltpu.CompilerParams(**params),
    )(*operands)

    def swap(a):
        return jnp.transpose(a, (0, 2, 1))

    return (
        pair_grad,
        qg.T,
        swap(qpg),
        qfg,
        kg.T,
        vg.T,
        swap(kpg),
        swap(vpg),
        kfg,
        bw.T,
        hw.reshape(H),
    )


def solution(mesh, sizes=(4, 4, 2, 4, 2)):
    finer = Mesh(mesh.devices.reshape(sizes), ROW_COL)
    in_specs = (
        P(ROW, COL, None),
        P(),
        P(),
        P(None, ROW),
        P(None, COL),
        P(None, COL),
        P(None, None, ROW),
        P(None, None, COL),
        P(None, None, COL),
        P(),
        P(),
        P(),
        P(None, ROW),
        P(None, None, ROW),
        P(ROW, None, None),
    )
    out_specs = (
        P(ROW, COL, None),
        P(None, ROW_COL),
        P(None, None, ROW_COL),
        P(None, None, ROW_COL),
        P(None, COL_ROW),
        P(None, COL_ROW),
        P(None, None, COL_ROW),
        P(None, None, COL_ROW),
        P(None, None, COL_ROW),
        P(),
        P(),
    )
    return jax.shard_map(
        functools.partial(per_device, sizes),
        mesh=finer,
        in_specs=in_specs,
        out_specs=out_specs,
        check_vma=False,
    )
```

```python
import functools
import math

import jax
import jax.numpy as jnp
from jax import lax
from jax.experimental import pallas as pl
from jax.experimental.pallas import tpu as pltpu
from jax.sharding import Mesh
from jax.sharding import PartitionSpec as P

ROW = ("row_0", "row_1", "row_2")
COL = ("col_0", "col_1")
ROW_COL = ROW + COL
COL_ROW = COL + ROW

H, C, PQ, PV, CZ = 12, 16, 4, 8, 128
KD, KV, QF = 384, 512, 640
ROT_Q, ROT_K, SEL_Q, SEL_D, SEL_V, SEL_C = 0, 9, 18, 30, 36, 45


def frame_lines(values, count):
    diagonal = iota((count, 128), 0) == iota((count, 128), 1)
    return [
        jnp.sum(jnp.where(diagonal, v, 0.0), axis=0, keepdims=True)[:, :count] for v in values
    ]
LOGIT = math.sqrt(1.0 / 3.0)
POINT = math.sqrt(2.0 / (9.0 * PQ))
INNER = 1.0 / math.sqrt(C)

F32, BF = jnp.float32, jnp.bfloat16
HIGHEST = lax.Precision.HIGHEST
MESH = pl.DeviceIdType.MESH
VMEM_BYTES = 67043328


def dot(a, b, ca, cb, precision=None):
    return lax.dot_general(
        a, b, (((ca,), (cb,)), ((), ())), precision=precision, preferred_element_type=F32
    )


def split(a):
    hi = a.astype(BF)
    return hi, (a - hi.astype(F32)).astype(BF)


def dot3(a, b, ca, cb):
    (ah, al), (bh, bl) = a, b
    return dot(ah, bh, ca, cb) + dot(ah, bl, ca, cb) + dot(al, bh, ca, cb)


def split3(a):
    first = a.astype(BF)
    rest = a - first.astype(F32)
    second = rest.astype(BF)
    return first, second, (rest - second.astype(F32)).astype(BF)


def dot6(a, b):
    (a1, a2, a3), (b1, b2, b3) = split3(a), split3(b)
    left = jnp.concatenate([a1, a1, a1, a2, a2, a3], axis=0)
    return dot(left, jnp.concatenate([b1, b2, b3, b1, b2, b1], axis=0), 0, 0)


def three(a, axis):
    hi, lo = split(a)
    return jnp.concatenate([hi, hi, lo], axis=axis)


def three_rhs(b):
    hi, lo = split(b)
    return jnp.concatenate([hi, lo, hi], axis=0)


def iota(shape, dim):
    return lax.broadcasted_iota(jnp.int32, shape, dim)


def softplus(x):
    return jnp.maximum(x, 0.0) + jnp.log1p(jnp.exp(-jnp.abs(x)))


def tile_kernel(
    sizes,
    pair_hbm,
    *refs,
):
    inputs, refs = refs[:14], refs[14:]
    sums, refs = refs[:6], refs[6:]
    copies_in, refs = refs[:14], refs[14:]
    tile_body(sizes, pair_hbm, inputs, copies_in, *sums, *copies_in, *refs)


def tile_body(
    sizes,
    pair_hbm,
    inputs,
    copies_in,
    turn_hbm,
    kd_hbm,
    kv_hbm,
    query_hbm,
    small_hbm,
    sel_hbm,
    wt_ref,
    hw_ref,
    q_ref,
    k_ref,
    v_ref,
    qp_ref,
    kp_ref,
    vp_ref,
    rot_ref,
    trans_ref,
    count_ref,
    go_ref,
    gp_ref,
    gpair_ref,
    pair_v,
    turn_v,
    kd_out,
    kv_out,
    query_out,
    small_out,
    sel_out,
    turn_buf,
    wide_d,
    wide_v,
    s_ref,
    pair_t,
    ub_ref,
    x_ref,
    e_ref,
    p_ref,
    d_ref,
    q32,
    k32,
    g48,
    v48,
    vec,
    own_peak,
    own_dist,
    stat_own,
    stat_in,
    q_pack,
    g_pack,
    qa,
    qb,
    qv,
    qfeat,
    qt,
    qx,
    qy,
    qz,
    kd_refs,
    kv_refs,
    w_refs,
    in_sem,
    pair_sem,
    out_sem,
    stat_sems,
    qx_sems,
    qz_sems,
    kd_sems,
    kv_sems,
    w_sems,
):
    n0, n1, n2, m0, m1 = sizes
    cols_n = m0 * m1
    rows = q_ref.shape[0]
    cols = k_ref.shape[1]
    i0, i1, i2 = (lax.axis_index(a) for a in ROW)
    j0, j1 = (lax.axis_index(a) for a in COL)
    r = (i0 * n1 + i1) * n2 + i2
    c = j0 * m1 + j1

    def col_peer(d):
        p = lax.rem(c + d, cols_n)
        return {"col_0": p // m1, "col_1": lax.rem(p, m1)}

    groups = {
        "x": (m0 * n2, j0 * n2 + i2, lambda p: {"col_0": p // n2, "row_2": lax.rem(p, n2)}),
        "z": (m1 * n0, j1 * n0 + i0, lambda p: {"col_1": p // n0, "row_0": lax.rem(p, n0)}),
        "y": (n1, i1, lambda p: {"row_1": p}),
    }

    def group_peer(name, d):
        count, here, place = groups[name]
        return place(lax.rem(here + d, count))

    def send(src, dst, sems, n, device):
        copy = pltpu.make_async_remote_copy(
            src_ref=src,
            dst_ref=dst,
            send_sem=sems[0].at[n],
            recv_sem=sems[1].at[n],
            device_id=device,
            device_id_type=MESH,
        )
        copy.start()
        return copy

    parts = pair_sem.shape[0]
    step = rows // parts
    loads = [
        pltpu.make_async_copy(
            pair_hbm.at[pl.ds(b * step, step)], pair_v.at[pl.ds(b * step, step)], pair_sem.at[b]
        )
        for b in range(parts)
    ]
    smalls = [
        pltpu.make_async_copy(src, dst, in_sem.at[n])
        for n, (src, dst) in enumerate(zip(inputs, copies_in))
    ]
    for load in smalls:
        load.start()

    barrier = pltpu.get_barrier_semaphore()
    expected = 0
    for d in range(1, cols_n):
        pl.semaphore_signal(barrier, inc=1, device_id=col_peer(d), device_id_type=MESH)
        expected += 1
    for name in groups:
        for d in range(1, groups[name][0]):
            pl.semaphore_signal(
                barrier, inc=1, device_id=group_peer(name, d), device_id_type=MESH
            )
            expected += 1

    for load in loads:
        load.start()
    for load in smalls:
        load.wait()

    col_start = pl.multiple_of(c * cols, 128)
    row_start = r * rows
    row_base = pl.multiple_of((row_start // 128) * 128, 128)
    row_half = lax.rem(row_start, 128)

    def row_window(w):
        return jnp.where(row_half == 0, w[:, :rows], w[:, 128 - rows :])

    def row_rot(x, y):
        return row_window(rot_ref[x, pl.ds(y, 1), pl.ds(row_base, 128)])

    def col_rot(x, y):
        return rot_ref[x, pl.ds(y, 1), pl.ds(col_start, cols)]

    coef = 0.5 * LOGIT * POINT * softplus(hw_ref[...])

    zero_q = jnp.zeros((2, rows), F32)
    zero_k = jnp.zeros((2, cols), F32)
    q_t = q_ref[...].T * (LOGIT * INNER)
    k_all = k_ref[...]
    rr = [[row_rot(x, y) for y in range(3)] for x in range(3)]
    cr = [[col_rot(x, y) for y in range(3)] for x in range(3)]
    for x in range(3):
        t_row = row_window(trans_ref[pl.ds(x, 1), pl.ds(row_base, 128)])
        t_col = trans_ref[pl.ds(x, 1), pl.ds(col_start, cols)]
        qg = sum(rr[x][y] * qp_ref[y] for y in range(3)) + t_row
        kg = sum(cr[x][y] * kp_ref[y] for y in range(3)) + t_col
        vg = sum(cr[x][y] * vp_ref[y] for y in range(3)) + t_col
        for h in range(H):
            q32[32 * h + 16 + 4 * x : 32 * h + 20 + 4 * x, :] = qg[4 * h : 4 * h + 4]
            k32[32 * h + 16 + 4 * x : 32 * h + 20 + 4 * x, :] = kg[4 * h : 4 * h + 4]
            v48[48 * h + 16 + 8 * x : 48 * h + 24 + 8 * x, :] = vg[8 * h : 8 * h + 8]
    gp_t = [gp_ref[y].T for y in range(3)]
    for x in range(3):
        gg = sum(rr[x][y] * gp_t[y] for y in range(3))
        for h in range(H):
            g48[48 * h + 16 + 8 * x : 48 * h + 24 + 8 * x, :] = gg[8 * h : 8 * h + 8]
    go_t = go_ref[...].T
    for h in range(H):
        q32[32 * h : 32 * h + 16, :] = q_t[16 * h : 16 * h + 16]
        k32[32 * h : 32 * h + 16, :] = k_all[16 * h : 16 * h + 16]
        g48[48 * h : 48 * h + 16, :] = go_t[16 * h : 16 * h + 16]
        v48[48 * h : 48 * h + 16, :] = v_ref[16 * h : 16 * h + 16, :]
        g48[48 * h + 40 : 48 * h + 48, :] = jnp.zeros((8, rows), F32)
        v48[48 * h + 40 : 48 * h + 48, :] = jnp.zeros((8, cols), F32)
        qh = q32[32 * h + 16 : 32 * h + 28, :]
        kh = k32[32 * h + 16 : 32 * h + 28, :]
        q32[32 * h + 28 : 32 * h + 32, :] = jnp.concatenate(
            [jnp.sum(qh * qh, axis=0, keepdims=True), jnp.ones((1, rows), F32), zero_q], axis=0
        )
        k32[32 * h + 28 : 32 * h + 32, :] = jnp.concatenate(
            [jnp.ones((1, cols), F32), jnp.sum(kh * kh, axis=0, keepdims=True), zero_k], axis=0
        )

    w16 = jnp.concatenate([wt_ref[...].astype(F32), jnp.zeros((4, CZ), F32)], axis=0)
    w16b = w16.astype(BF)

    def stack(i):
        gpad = jnp.concatenate(
            [gpair_ref[:, i, :].astype(F32), jnp.zeros((4, CZ), F32)], axis=0
        ).astype(BF)
        return gpad

    e_ref[H:16] = jnp.zeros((16 - H, rows, cols), F32)
    p_ref[H:16] = jnp.zeros((16 - H, rows, cols), F32)
    point_row = iota((16, 1), 0) < 12
    for h in range(H):
        kb = k32[32 * h + 16 : 32 * h + 32, :]
        inner = dot6(q32[32 * h : 32 * h + 16, :], k32[32 * h : 32 * h + 16, :])
        dist = dot6(q32[32 * h + 16 : 32 * h + 32, :], jnp.where(point_row, -2.0 * kb, kb))
        d_ref[h] = dist
        e_ref[h] = inner - coef[:, h : h + 1] * dist
        p_ref[h] = dot(
            three(g48[48 * h : 48 * h + 48, :], 0), three_rhs(v48[48 * h : 48 * h + 48, :]), 0, 0
        )

    for b in range(parts):
        loads[b].wait()
        for ib in range(b * step // 8, (b + 1) * step // 8):
            proj = []
            for i in range(8 * ib, 8 * ib + 8):
                both = jnp.concatenate([w16b, stack(i)], axis=0)
                if i % 4 == 3:
                    proj.append(dot(both, pair_v[i], 1, 1))
                else:
                    pair_t[i] = pair_v[i].T
                    proj.append(dot(both, pair_t[i], 1, 0))
            s_ref[:, 8 * ib : 8 * ib + 8, :] = jnp.transpose(jnp.stack(proj), (1, 0, 2))

    valid = col_start + iota((1, cols), 1) < count_ref[0]
    lane = iota((rows, 128), 1)
    for h in range(H):
        prod = p_ref[h] + s_ref[16 + h]
        logits = e_ref[h] + LOGIT * s_ref[h]
        logits = jnp.where(valid, logits, -1000000000.0)
        peak = jnp.max(logits, axis=1, keepdims=True)
        e = jnp.exp(logits - peak)
        total = jnp.sum(e, axis=1, keepdims=True)
        upper = jnp.sum(e * prod, axis=1, keepdims=True)
        e_ref[h] = e
        p_ref[h] = prod
        vec[h * rows : (h + 1) * rows, :] = jnp.where(
            lane == 0, peak + jnp.log(total), jnp.where(lane == 1, upper / total, peak)
        )
    blocks = H * rows // 128
    own_peak[...] = jnp.zeros_like(own_peak)
    own_dist[...] = jnp.zeros_like(own_dist)
    for b in range(blocks):
        turned = vec[128 * b : 128 * b + 128, :].T
        stat_own[b : b + 1, :] = turned[0:1]
        stat_own[blocks + b : blocks + b + 1, :] = turned[1:2]
        own_peak[b : b + 1, :] = turned[2:3]

    pl.semaphore_wait(barrier, expected)

    stat_copies = [
        pltpu.make_async_remote_copy(
            src_ref=stat_own,
            dst_ref=stat_in.at[d - 1],
            send_sem=stat_sems[0].at[d - 1],
            recv_sem=stat_sems[1].at[d - 1],
            device_id=col_peer(d),
            device_id_type=MESH,
        )
        for d in sorted(range(1, cols_n), key=lambda d: d % m1 == 0)
    ]

    def send_stats(core):
        @pl.when(i2 == core)
        def _():
            for copy in stat_copies:
                copy.start()

    send_stats(0)

    for a in (6, 14, 22, 30):
        s_ref[a : a + 2] = jnp.zeros((2, rows, cols), F32)
    for h in range(H):
        own = slice(h * rows, (h + 1) * rows)
        if h == 4:
            send_stats(1)
        e = e_ref[h]
        es = split(e)
        ep = e * (p_ref[h] - vec[own, 1:2])
        ks = split(k32[32 * h : 32 * h + 32, :])
        qa[32 * h : 32 * h + 32, :] = dot3(ks, split(ep), 1, 1)
        qb[32 * h : 32 * h + 32, :] = dot3(ks, es, 1, 1)
        qv[24 * h : 24 * h + 24, :] = dot3(split(v48[48 * h : 48 * h + 48, :]), es, 1, 1)[16:40]
        s_ref[8 * (h % 2) + h // 2] = ep
        s_ref[16 + 8 * (h % 2) + h // 2] = e
        dist = d_ref[h]
        vec[own, :] = jnp.where(
            lane == 0,
            jnp.sum(ep * dist, axis=1, keepdims=True),
            jnp.sum(e * dist, axis=1, keepdims=True),
        )
    for b in range(blocks):
        turned = vec[128 * b : 128 * b + 128, :].T
        own_dist[b : b + 1, :] = turned[0:1]
        own_dist[8 + b : 9 + b, :] = turned[1:2]
    for ib in range(rows // 8):
        by_query = jnp.transpose(s_ref[:, 8 * ib : 8 * ib + 8, :], (1, 0, 2))
        for ii in range(8):
            both = dot(jnp.concatenate(split(by_query[ii]), axis=0), pair_v[8 * ib + ii], 1, 0)
            ub_ref[8 * ib + ii] = both[0:32] + both[32:64]
    for h in range(H):
        q_pack[32 * h : 32 * h + 32, :] = three(q32[32 * h : 32 * h + 32, :], 1)
        g_pack[48 * h : 48 * h + 48, :] = three(g48[48 * h : 48 * h + 48, :], 1)

    for copy in stat_copies:
        copy.wait()

    def padded(ref, part):
        rows_here = ref[part * blocks : part * blocks + blocks, :]
        return jnp.concatenate([rows_here, jnp.zeros((8 - blocks, 128), F32)], axis=0)

    stats = [
        (padded(ref, 0), padded(ref, 1))
        for ref in [stat_own] + [stat_in.at[d] for d in range(cols_n - 1)]
    ]
    peak = functools.reduce(jnp.maximum, [s[0] for s in stats])
    weights = [jnp.exp(s[0] - peak) for s in stats]
    total = functools.reduce(jnp.add, weights)
    delta = functools.reduce(jnp.add, [w * s[1] for w, s in zip(weights, stats)]) / total
    scale = jnp.exp(own_peak[...] - peak) / total
    shift = delta - stats[0][1]
    scale_t, delta_t = scale.T, delta.T

    class Small:
        def __init__(self, value):
            w_refs[0][...] = value
            self.level = 0

        def send(self, name):
            at = self.level
            self.copies = [
                send(
                    w_refs[2 * at],
                    w_refs[2 * at + 1].at[d - 1],
                    w_sems[2 * at : 2 * at + 2],
                    d - 1,
                    group_peer(name, d),
                )
                for d in range(1, groups[name][0])
            ]

        def add(self):
            for copy in self.copies:
                copy.wait()
            here, came = w_refs[2 * self.level], w_refs[2 * self.level + 1]
            total = here[...] + functools.reduce(
                jnp.add, [came[d] for d in range(came.shape[0])]
            )
            self.level += 1
            if self.level < 3:
                w_refs[2 * self.level][...] = total
            return total

    half = rows
    scale_h = jnp.concatenate([scale[:, :half], scale[:, half:]], axis=0)
    shift_h = jnp.concatenate([shift[:, :half], shift[:, half:]], axis=0)
    acc = jnp.zeros((16, CZ), F32)
    for i in range(rows):
        acc = acc + scale_h[:, i : i + 1] * (
            ub_ref[i, 0:16] - shift_h[:, i : i + 1] * ub_ref[i, 16:32]
        )
    moment = scale * (own_dist[0:8, :] - shift * own_dist[8:16, :])
    lane8, row8 = iota((8, 128), 1), iota((8, 128), 0)
    even = jnp.sum(jnp.where(lane8 < half, moment, 0.0), axis=1, keepdims=True)
    odd = jnp.sum(jnp.where(lane8 < half, 0.0, moment), axis=1, keepdims=True)
    spread = jnp.where(lane8 == 2 * row8, even, jnp.where(lane8 == 2 * row8 + 1, odd, 0.0))
    head_sum = jnp.sum(spread, axis=0, keepdims=True)
    small = Small(jnp.where(iota((16, 1), 0) == 6, head_sum, LOGIT * acc))
    small.send("x")

    kind = iota((32, 1), 0)
    is_vec = kind < 16

    class Staged:
        def __init__(self, refs, sems, out):
            self.feat, self.kt, self.k1, self.p1, self.k2, self.p2, self.k3 = refs
            self.sems = (sems[0:2], sems[2:4], sems[4:6])
            self.out = out

        def turn(self):
            share = self.kt.shape[2]
            per = 128 // (share * n2)
            for a in range(self.feat.shape[0] // 128):
                for b in range(cols // 128):
                    block = self.feat[128 * a : 128 * a + 128, 128 * b : 128 * b + 128].T
                    block = block.reshape(per, n2, share, 128)
                    for n in range(n2):
                        self.kt[n, b * per : (b + 1) * per, :, 128 * a : 128 * a + 128] = block[:, n]

        def send1(self):
            other = lax.rem(i2 + 1, n2)
            self.copies = [send(self.kt.at[other], self.k1, self.sems[0], 0, {"row_2": other})]

        def wait(self):
            for copy in self.copies:
                copy.wait()

        def send2(self):
            self.wait()
            for y in range(n1):
                for z in range(n0):
                    self.p1[y, z] = self.kt[i2, z * n1 + y] + self.k1[z * n1 + y]
            self.copies = []
            for d in range(1, n1):
                to = lax.rem(i1 + d, n1)
                self.copies.append(
                    send(self.p1.at[to], self.k2.at[d - 1], self.sems[1], d - 1, {"row_1": to})
                )

        def send3(self):
            self.wait()
            self.p2[...] = self.p1[i1] + functools.reduce(
                jnp.add, [self.k2[d] for d in range(n1 - 1)]
            )
            self.copies = []
            for d in range(1, n0):
                to = lax.rem(i0 + d, n0)
                self.copies.append(
                    send(self.p2.at[to], self.k3.at[d - 1], self.sems[2], d - 1, {"row_0": to})
                )

        def finish(self):
            self.wait()
            self.out[...] = self.p2[i0] + functools.reduce(
                jnp.add, [self.k3[d] for d in range(n0 - 1)]
            )

    side_d = Staged(kd_refs, kd_sems, kd_out)
    side_v = Staged(kv_refs, kv_sems, kv_out)

    side_d.feat[336:KD, :] = jnp.zeros((KD - 336, cols), F32)
    side_v.feat[480:KV, :] = jnp.zeros((KV - 480, cols), F32)
    for h in range(H):
        own = slice(h * rows, (h + 1) * rows)
        at = (slice(rows * (h % 2), rows * (h % 2) + rows), slice(h // 2, h // 2 + 1))
        attn = e_ref[h] * scale_t[at]
        dlog = attn * (p_ref[h] - delta_t[at])
        p_ref[h] = dlog
        e_ref[h] = attn
        two = 2.0 * coef[:, h : h + 1]
        kd = dot(q_pack[32 * h : 32 * h + 32, :], three_rhs(dlog), 1, 0)
        col_sum = kd[29:30]
        kd = jnp.where(is_vec, kd, two * (kd - k32[32 * h : 32 * h + 32, :] * col_sum))
        side_d.feat[16 * h : 16 * h + 16, :] = kd[0:16]
        for x in range(3):
            to = 192 + 48 * x + 4 * h
            side_d.feat[to : to + 4, :] = kd[16 + 4 * x : 20 + 4 * x]
    side_d.turn()
    side_d.send1()

    for h in range(H):
        own = slice(h * rows, (h + 1) * rows)
        ka = dot(g_pack[48 * h : 48 * h + 48, :], three_rhs(e_ref[h]), 1, 0)
        side_v.feat[16 * h : 16 * h + 16, :] = ka[0:16]
        for x in range(3):
            to = 192 + 96 * x + 8 * h
            side_v.feat[to : to + 8, :] = ka[16 + 8 * x : 24 + 8 * x]
    side_v.turn()
    side_v.send1()

    for h in range(H):
        at = (slice(h // 2, h // 2 + 1), slice(rows * (h % 2), rows * (h % 2) + rows))
        two = 2.0 * coef[:, h : h + 1]
        head = slice(32 * h, 32 * h + 32)
        qd = scale[at] * (qa[head, :] - shift[at] * qb[head, :])
        row_sum = qd[28:29]
        qd = jnp.where(is_vec, LOGIT * INNER * qd, two * (qd - q32[head, :] * row_sum))
        opt = scale[at] * qv[24 * h : 24 * h + 24, :]
        qfeat[16 * h : 16 * h + 16, :] = qd[0:16]
        for x in range(3):
            to = 192 + 48 * x + 4 * h
            qfeat[to : to + 4, :] = qd[16 + 4 * x : 20 + 4 * x]
            to = 336 + 96 * x + 8 * h
            qfeat[to : to + 8, :] = opt[8 * x : 8 * x + 8]
    qfeat[624:QF, :] = jnp.zeros((QF - 624, rows), F32)
    for a in range(QF // 128):
        qt[:, :, 128 * a : 128 * a + 128] = qfeat[128 * a : 128 * a + 128, :].T.reshape(
            qt.shape[0], qt.shape[1], 128
        )
    qx_copies = []
    for d in range(1, m0):
        to = lax.rem(j0 + d, m0)
        qx_copies.append(
            send(qt.at[pl.ds(to * m1, m1)], qx.at[d - 1], qx_sems, d - 1, {"col_0": to})
        )

    side_d.send2()

    side_v.send2()
    small.add()
    small.send("z")

    for ib in range(rows // 8):
        some = slice(8 * ib, 8 * ib + 8)
        x_ref[some, 0:16, :] = jnp.transpose(p_ref[:, some, :], (1, 0, 2)).astype(BF)
        x_ref[some, 16:32, :] = jnp.transpose(e_ref[:, some, :], (1, 0, 2)).astype(BF)
    for b in range(rows // 4):
        turn_v[b] = x_ref[4 * b : 4 * b + 4].reshape(128, cols).T
    turn_copy = pltpu.make_async_copy(turn_v, turn_hbm, out_sem.at[0])
    turn_copy.start()

    share = kd_out.shape[0]

    def frames(start):
        base = pl.multiple_of((start // 128) * 128, 128)
        sel = iota((share, 128), 1) == iota((share, 128), 0) + (start - base)

        def every_lane(row):
            one = jnp.sum(jnp.where(sel, row, 0.0), axis=1, keepdims=True)
            return jnp.broadcast_to(one, (share, 128))

        rot = [
            [every_lane(rot_ref[x, pl.ds(y, 1), pl.ds(base, 128)]) for y in range(3)]
            for x in range(3)
        ]
        return rot, [every_lane(trans_ref[pl.ds(x, 1), pl.ds(base, 128)]) for x in range(3)]

    rot, anchor = frames(r * rows + c * share)
    key_rot, _ = frames(c * cols + r * share)
    key_base = pl.multiple_of((r * share // 128) * 128, 128)
    key_at = pl.multiple_of(lax.rem(r * share, 128), 8)
    query_at = pl.multiple_of(c * share, 8)

    def hand_over(to, blocks, wide, at):
        for begin, block in blocks:
            wide[begin : begin + block.shape[0], :] = block
        for n in range(1, wide.shape[0] // 128):
            turn_buf[0 : wide.shape[1], :] = wide[128 * n : 128 * n + 128, :].T
            sel_out[to + n - 1] = turn_buf[pl.ds(at, share), :]

    constants = []
    for x in range(3):
        for y in range(3):
            sel_out[ROT_Q + 3 * x + y] = rot[x][y]
            sel_out[ROT_K + 3 * x + y] = key_rot[x][y]
    cotan = [gp_ref[y, pl.ds(query_at, share), :] for y in range(3)]
    sums = [jnp.sum(a, axis=1, keepdims=True) for a in cotan]
    for x in range(3):
        constants += [-anchor[x][:, 0:1] * sums[y] for y in range(3)]
        constants.append(-sum(rot[x][y][:, 0:1] * sums[y] for y in range(3)))
    for n, line in enumerate(frame_lines(constants, share)):
        sel_out[SEL_C + n // share, n % share : n % share + 1, 0:share] = line
    qfeat[...] = jnp.zeros_like(qfeat)
    wide_d[...] = jnp.zeros_like(wide_d)
    wide_v[...] = jnp.zeros_like(wide_v)
    for y in range(3):
        local, cotan_y = qp_ref[y], gp_ref[y].T
        blocks = [(192 + 48 * x, local) for x in range(3)]
        blocks += [(336 + 96 * x, cotan_y) for x in range(3)]
        hand_over(SEL_Q + 4 * y, blocks, qfeat, query_at)
        local = kp_ref[y, :, pl.ds(key_base, 128)]
        hand_over(SEL_D + 2 * y, [(192 + 48 * x, local) for x in range(3)], wide_d, key_at)
        local = vp_ref[y, :, pl.ds(key_base, 128)]
        hand_over(SEL_V + 3 * y, [(192 + 96 * x, local) for x in range(3)], wide_v, key_at)
    sel_copy = pltpu.make_async_copy(sel_out, sel_hbm, out_sem.at[5])
    sel_copy.start()

    for copy in qx_copies:
        copy.wait()
    qy[...] = qt[pl.ds(j0 * m1, m1)] + functools.reduce(jnp.add, [qx[d] for d in range(m0 - 1)])
    qz_copies = []
    for d in range(1, m1):
        to = lax.rem(j1 + d, m1)
        qz_copies.append(send(qy.at[to], qz.at[d - 1], qz_sems, d - 1, {"col_1": to}))
    side_d.send3()
    side_v.send3()
    small.add()
    small.send("y")
    side_d.finish()
    side_v.finish()
    for copy in qz_copies:
        copy.wait()
    query_out[...] = functools.reduce(jnp.add, [qz[d] for d in range(m1 - 1)], qy[j1])
    small_out[...] = small.add()
    outs = [
        pltpu.make_async_copy(query_out, query_hbm, out_sem.at[1]),
        pltpu.make_async_copy(kd_out, kd_hbm, out_sem.at[2]),
        pltpu.make_async_copy(kv_out, kv_hbm, out_sem.at[3]),
        pltpu.make_async_copy(small_out, small_hbm, out_sem.at[4]),
    ]
    for copy in outs:
        copy.start()
    for copy in outs + [turn_copy, sel_copy]:
        copy.wait()


def finish_kernel(*refs):
    inputs, refs = refs[:9], refs[9:]
    outs, refs = refs[:11], refs[11:]
    copies_in, refs = refs[:9], refs[9:]
    results, (pg_v, in_sem, pg_sem, out_sem) = refs[:10], refs[10:]
    turn_ref, wt_ref, gpair_ref = copies_in[:3]
    loads = [
        pltpu.make_async_copy(src, dst, in_sem.at[n])
        for n, (src, dst) in enumerate(zip(inputs, copies_in))
    ]
    for load in loads:
        load.start()
    for load in loads[:3]:
        load.wait()
    stores = []

    rows = pg_v.shape[0]
    zero4 = jnp.zeros((4, CZ), F32)
    w16s = jnp.concatenate([LOGIT * wt_ref[...].astype(F32), zero4], axis=0).astype(BF)
    zero32 = jnp.zeros((32, CZ), BF)

    def weights(i):
        gpad = jnp.concatenate([gpair_ref[:, i, :].astype(F32), zero4], axis=0).astype(BF)
        return jnp.concatenate([w16s, gpad], axis=0)

    parts = pg_sem.shape[0]
    step = rows // parts
    for b in range(rows // 4):
        for half in range(2):
            first, second = 4 * b + 2 * half, 4 * b + 2 * half + 1
            left = [zero32] * 4
            right = [zero32] * 4
            left[2 * half], right[2 * half + 1] = weights(first), weights(second)
            block = jnp.concatenate(
                [jnp.concatenate(left, axis=0), jnp.concatenate(right, axis=0)], axis=1
            )
            out = dot(turn_ref[b], block, 1, 0)
            pg_v[first] = out[:, :CZ].astype(BF)
            pg_v[second] = out[:, CZ:].astype(BF)
        if 4 * (b + 1) % step == 0:
            p = 4 * (b + 1) // step - 1
            store = pltpu.make_async_copy(
                pg_v.at[pl.ds(p * step, step)], outs[0].at[pl.ds(p * step, step)], pg_sem.at[p]
            )
            store.start()
            stores.append(store)

    for load in loads[3:]:
        load.wait()
    finish_body(*copies_in[3:], *results)
    for n, (src, dst) in enumerate(zip(results, outs[1:])):
        store = pltpu.make_async_copy(src, dst, out_sem.at[n])
        store.start()
        stores.append(store)
    for store in stores:
        store.wait()


def finish_body(
    kd_ref,
    kv_ref,
    query_ref,
    small_ref,
    sel_ref,
    hw_ref,
    qg_out,
    qpg_out,
    qfg_out,
    kg_out,
    vg_out,
    kpg_out,
    vpg_out,
    kfg_out,
    bw_out,
    hw_out,
):
    share = kd_ref.shape[0]

    def lanes(width, x, *segments):
        lane = iota((share, width), 1) + 128
        return functools.reduce(
            jnp.logical_or,
            [(lane >= b + w * x) & (lane < b + w * x + w) for b, w in segments],
        )

    def segment_sum(values, mask):
        kept = jnp.where(mask, values, 0.0)
        parts = [kept[:, 128 * n : 128 * n + 128] for n in range(kept.shape[1] // 128)]
        return functools.reduce(jnp.add, parts)

    def handed(at, count):
        return jnp.concatenate([sel_ref[at + n] for n in range(count)], axis=1)

    def put(out, lines):
        for n, line in enumerate(lines):
            out[n // 4, n % 4 : n % 4 + 1, :] = line

    query, key_d, key_v = query_ref[...], kd_ref[...], kv_ref[...]
    qg_out[...] = query[:, 0:192]
    kg_out[...] = key_d[:, 0:192]
    vg_out[...] = key_v[:, 0:192]
    turned = [
        (qpg_out, ROT_Q, [query[:, 192 + 48 * x : 240 + 48 * x] for x in range(3)]),
        (kpg_out, ROT_K, [key_d[:, 192 + 48 * x : 240 + 48 * x] for x in range(3)]),
        (vpg_out, ROT_K, [key_v[:, 192 + 96 * x : 288 + 96 * x] for x in range(3)]),
    ]

    query, key_d, key_v = query[:, 128:], key_d[:, 128:], key_v[:, 128:]
    frame, key_frame = [], []
    for x in range(3):
        both = lanes(512, x, (192, 48), (336, 96))
        mask_d, mask_v = lanes(256, x, (192, 48)), lanes(384, x, (192, 96))
        for y in range(4):
            if y < 3:
                one = segment_sum(query * handed(SEL_Q + 4 * y, 4), both)
                two = segment_sum(key_d * handed(SEL_D + 2 * y, 2), mask_d)
                three_ = segment_sum(key_v * handed(SEL_V + 3 * y, 3), mask_v)
            else:
                one = segment_sum(query, lanes(512, x, (192, 48)))
                two, three_ = segment_sum(key_d, mask_d), segment_sum(key_v, mask_v)
            frame.append(jnp.sum(one, axis=1, keepdims=True))
            key_frame.append(jnp.sum(two + three_, axis=1, keepdims=True))
    lines = frame_lines(frame, share)
    put(
        qfg_out,
        [
            line + sel_ref[SEL_C + n // share, n % share : n % share + 1, 0:share]
            for n, line in enumerate(lines)
        ],
    )
    put(kfg_out, frame_lines(key_frame, share))
    for out, at, parts in turned:
        width = parts[0].shape[1]
        for y in range(3):
            out[y] = sum(sel_ref[at + 3 * x + y, :, 0:width] * parts[x] for x in range(3))

    for h in range(H):
        bw_out[h : h + 1, :] = small_ref[8 * (h % 2) + h // 2 : 8 * (h % 2) + h // 2 + 1, :]
    raw = hw_ref[...]
    hw_out[...] = small_ref[6:7, 0:H] * (-0.5 * LOGIT * POINT) / (1.0 + jnp.exp(-raw))


def per_device(
    sizes,
    pair_rep,
    bias_weight,
    head_weight,
    queries,
    key_vectors,
    values,
    query_points,
    key_points,
    value_points,
    rotations,
    translations,
    residue_count,
    grad_output,
    grad_points,
    grad_pair,
):
    n0, n1, n2, m0, m1 = sizes
    cols_n = m0 * m1
    rows, cols = pair_rep.shape[:2]
    share, qshare = cols // (n0 * n1 * n2), rows // cols_n
    head_row = head_weight.reshape(1, H)
    grad_points_t = jnp.transpose(grad_points, (0, 2, 1))
    hbm = pl.BlockSpec(memory_space=pl.ANY)
    dma = pltpu.SemaphoreType.DMA
    params = dict(vmem_limit_bytes=VMEM_BYTES)

    def buf(*shape, dtype=F32):
        return pltpu.VMEM(shape, dtype)

    def like(array):
        space = pltpu.VMEM if array.size > 1 else pltpu.SMEM
        return space(array.shape, array.dtype)

    weight_t = bias_weight.T
    grad_pair_t = jnp.transpose(grad_pair, (1, 0, 2))
    operands = (
        weight_t,
        head_row,
        queries.T,
        key_vectors,
        values,
        query_points,
        key_points,
        value_points,
        rotations,
        translations,
        residue_count,
        grad_output.T,
        grad_points_t,
        grad_pair_t,
    )
    sums = (
        jax.ShapeDtypeStruct((rows // 4, cols, 128), BF),
        jax.ShapeDtypeStruct((share, KD), F32),
        jax.ShapeDtypeStruct((share, KV), F32),
        jax.ShapeDtypeStruct((qshare, QF), F32),
        jax.ShapeDtypeStruct((16, CZ), F32),
        jax.ShapeDtypeStruct((SEL_C + 2, share, 128), F32),
    )

    def staged(width):
        return (
            buf(width, cols),
            buf(n2, n0 * n1, share, width),
            buf(n0 * n1, share, width),
            buf(n1, n0, share, width),
            buf(n1 - 1, n0, share, width),
            buf(n0, share, width),
            buf(n0 - 1, share, width),
        )

    def pairs(*counts):
        return tuple(dma((n,)) for n in counts for _ in range(2))

    levels = (m0 * n2, m1 * n0, n1)
    turned, kd_sum, kv_sum, query_sum, small_sum, own_parts = pl.pallas_call(
        functools.partial(tile_kernel, sizes),
        name="tile",
        out_shape=sums,
        in_specs=[hbm] * (1 + len(operands)),
        out_specs=(hbm,) * 6,
        scratch_shapes=[
            *[like(a) for a in operands],
            like(pair_rep),
            *[like(a) for a in sums],
            buf(128, 128),
            buf(KD, 128),
            buf(KV, 128),
            buf(32, rows, cols),
            buf(rows, CZ, cols, dtype=BF),
            buf(rows, 32, CZ),
            buf(rows, 32, cols, dtype=BF),
            buf(16, rows, cols),
            buf(16, rows, cols),
            buf(H, rows, cols),
            buf(H * 32, rows),
            buf(H * 32, cols),
            buf(H * 48, rows),
            buf(H * 48, cols),
            buf(H * rows, 128),
            buf(8, 128),
            buf(16, 128),
            buf(2 * H * rows // 128, 128),
            buf(cols_n - 1, 2 * H * rows // 128, 128),
            buf(H * 32, 3 * rows, dtype=BF),
            buf(H * 48, 3 * rows, dtype=BF),
            buf(H * 32, rows),
            buf(H * 32, rows),
            buf(H * 24, rows),
            buf(QF, rows),
            buf(cols_n, qshare, QF),
            buf(m0 - 1, m1, qshare, QF),
            buf(m1, qshare, QF),
            buf(max(m1 - 1, 1), qshare, QF),
            staged(KD),
            staged(KV),
            tuple(b for n in levels for b in (buf(16, CZ), buf(n - 1, 16, CZ))),
            dma((len(operands),)),
            dma((2,)),
            dma((len(sums),)),
            pairs(cols_n - 1),
            pairs(m0 - 1),
            pairs(max(m1 - 1, 1)),
            pairs(1, n1 - 1, n0 - 1),
            pairs(1, n1 - 1, n0 - 1),
            pairs(*[n - 1 for n in levels]),
        ],
        compiler_params=pltpu.CompilerParams(collective_id=0, has_side_effects=True, **params),
    )(pair_rep, *operands)
    operands = (
        turned,
        weight_t,
        grad_pair_t,
        kd_sum,
        kv_sum,
        query_sum,
        small_sum,
        own_parts,
        head_row,
    )
    results = (
        jax.ShapeDtypeStruct((qshare, 192), F32),
        jax.ShapeDtypeStruct((3, qshare, 48), F32),
        jax.ShapeDtypeStruct((3, 4, qshare), F32),
        jax.ShapeDtypeStruct((share, 192), F32),
        jax.ShapeDtypeStruct((share, 192), F32),
        jax.ShapeDtypeStruct((3, share, 48), F32),
        jax.ShapeDtypeStruct((3, share, 96), F32),
        jax.ShapeDtypeStruct((3, 4, share), F32),
        jax.ShapeDtypeStruct((H, CZ), F32),
        jax.ShapeDtypeStruct((1, H), F32),
    )
    pair_grad, qg, qpg, qfg, kg, vg, kpg, vpg, kfg, bw, hw = pl.pallas_call(
        finish_kernel,
        name="finish",
        out_shape=(jax.ShapeDtypeStruct(pair_rep.shape, BF), *results),
        in_specs=[hbm] * len(operands),
        out_specs=(hbm,) * 11,
        scratch_shapes=[
            *[like(a) for a in operands],
            *[like(a) for a in results],
            like(pair_rep),
            dma((len(operands),)),
            dma((8,)),
            dma((len(results),)),
        ],
        compiler_params=pltpu.CompilerParams(**params),
    )(*operands)

    def swap(a):
        return jnp.transpose(a, (0, 2, 1))

    return (
        pair_grad,
        qg.T,
        swap(qpg),
        qfg,
        kg.T,
        vg.T,
        swap(kpg),
        swap(vpg),
        kfg,
        bw.T,
        hw.reshape(H),
    )


def solution(mesh, sizes=(4, 4, 2, 4, 2)):
    finer = Mesh(mesh.devices.reshape(sizes), ROW_COL)
    in_specs = (
        P(ROW, COL, None),
        P(),
        P(),
        P(None, ROW),
        P(None, COL),
        P(None, COL),
        P(None, None, ROW),
        P(None, None, COL),
        P(None, None, COL),
        P(),
        P(),
        P(),
        P(None, ROW),
        P(None, None, ROW),
        P(ROW, None, None),
    )
    out_specs = (
        P(ROW, COL, None),
        P(None, ROW_COL),
        P(None, None, ROW_COL),
        P(None, None, ROW_COL),
        P(None, COL_ROW),
        P(None, COL_ROW),
        P(None, None, COL_ROW),
        P(None, None, COL_ROW),
        P(None, None, COL_ROW),
        P(),
        P(),
    )
    return jax.shard_map(
        functools.partial(per_device, sizes),
        mesh=finer,
        in_specs=in_specs,
        out_specs=out_specs,
        check_vma=False,
    )
```
